256 devices in a mesh: scene: 2 (over z), view: 128 (over y, x, core).
Axes of the slice: x: 8, y: 8, z: 2, core: 2. Of those that a mesh axis runs over, the one named last changes fastest.
The devices are a block of a 8x8x16 slice.
Arguments:
- latents: bfloat16 [2048, 64, 512], P(('scene', 'view')), parts along dimension 0, may hold values from -48 to 48
- norm_gain: float32 [512], replicated, may hold values from 0.1 to 1.9
- norm_shift: float32 [512], replicated, may hold values from -3 to 3
- w_first: bfloat16 [512, 3, 3, 512], replicated, may hold values from -0.09375 to 0.09375
- bias_first: float32 [512], replicated, may hold values from -3 to 3
- w_second: bfloat16 [512, 3, 3, 512], replicated, may hold values from -0.09375 to 0.09375
- bias_second: float32 [512], replicated, may hold values from -3 to 3
Outputs:
- decoded: bfloat16 [4096, 128, 512], P(('scene', 'view')), parts along dimension 0
The draws below stay inside these ranges and needn't reach their ends.
There are 2 independent parts, one for each index of `scene`. The reference program is written for one: setup_inputs(seed, part) draws one part's arguments, and reference() takes and returns one part's arrays. A program takes and returns all parts, laid end to end along the dimension named above; an argument that names none is the same for every part. Nothing has to cross between parts.
All inputs are finite; a program needn't handle non-finite values.
Results may differ from the reference program's by a relative error of at most 0.0051.
Values may be sent and summed in bfloat16 or wider, within the bound.
A program may use at most 128 MiB of HBM per device.

```python
import jax
import jax.numpy as jnp
from jax import lax

C = 512
GROUPS = 32
ROWS_DEV = 8
H_LAT = 32
W_LAT = 64
SLABS = 4
VIEWS = 32


def draw_latents(key, part):
    total_rows = VIEWS * H_LAT
    block_count = total_rows // ROWS_DEV
    key_noise = jax.random.fold_in(key, 11)
    key_scale = jax.random.fold_in(key, 23)
    key_level = jax.random.fold_in(key, 37)
    key_sign = jax.random.fold_in(key, 41)
    key_jitter = jax.random.fold_in(key, 53)
    key_block_sign = jax.random.fold_in(key, 61)
    key_block_level = jax.random.fold_in(key, 67)
    key_block_noise = jax.random.fold_in(key, 71)
    noise = jnp.clip(jax.random.normal(key_noise, (total_rows, W_LAT, C), jnp.float32), -4.0, 4.0)
    place = jnp.arange(total_rows, dtype=jnp.float32) / (total_rows - 1)
    level = jax.random.uniform(key_level, (GROUPS,), jnp.float32, 0.5, 1.5)
    sign = jnp.where(jax.random.uniform(key_sign, (GROUPS,), jnp.float32) < 0.5, -1.0, 1.0)
    block_sign = jnp.where(jax.random.uniform(key_block_sign, (block_count, GROUPS), jnp.float32) < 0.5, -1.0, 1.0)
    chan_jitter = jax.random.uniform(key_jitter, (C,), jnp.float32, 0.7, 1.3)
    row_scale = 3.0 ** (place - 0.5)
    chan_scale = 2.0 ** (2.0 * jax.random.uniform(key_scale, (C,), jnp.float32) - 1.0)
    rise = 1.0 + 2.0 * place
    block_level = jax.random.uniform(key_block_level, (block_count, GROUPS), jnp.float32, 0.3, 1.7)
    block_noise = jax.random.uniform(key_block_noise, (block_count,), jnp.float32, 0.5, 1.5)
    common = 0.5
    block_group = common * (level * sign)[None, :] + block_sign * block_level
    block_shift = jnp.broadcast_to(block_group[:, :, None], (block_count, GROUPS, C // GROUPS)).reshape(block_count, C) * chan_jitter
    row_shift = jnp.repeat(block_shift, ROWS_DEV, axis=0)
    row_noise = jnp.repeat(block_noise, ROWS_DEV, axis=0)
    values = noise * (row_scale * row_noise)[:, None, None] * chan_scale + rise[:, None, None] * row_shift[:, None, :]
    values = jnp.clip(0.35 * values, -48.0, 48.0)
    return values.astype(jnp.bfloat16)


def normal_values(key, shape, spread, most, kind=jnp.bfloat16):
    entries = spread * jax.random.normal(key, shape, jnp.float32)
    return jnp.clip(entries, min=-most, max=most).astype(kind)


def setup_inputs(seed: int = 0, part: int = 0) -> dict:
    key_of = jax.random.split(jax.random.key(seed), 8)
    part_keys = jax.random.split(jax.random.fold_in(key_of[7], part), 8)
    latents = draw_latents(jax.random.fold_in(jax.random.fold_in(key_of[7], part), 71), part)
    norm_gain = jnp.clip(1.0 + 0.18 * jax.random.normal(key_of[1], (C,), jnp.float32), 0.1, 1.9)
    norm_shift = normal_values(key_of[2], (C,), 0.5, 3.0, jnp.float32)
    w_first = normal_values(key_of[3], (C, 3, 3, C), (9 * C) ** -0.5, 0.09375)
    bias_first = normal_values(key_of[4], (C,), 0.5, 3.0, jnp.float32)
    w_second = normal_values(key_of[5], (C, 3, 3, C), (9 * C) ** -0.5, 0.09375)
    bias_second = normal_values(key_of[6], (C,), 0.5, 3.0, jnp.float32)
    return dict(latents=latents, norm_gain=norm_gain, norm_shift=norm_shift, w_first=w_first, bias_first=bias_first, w_second=w_second, bias_second=bias_second)


epsilon = 1e-06

def convolve(inputs, filters):
    return lax.conv_general_dilated(inputs.astype(jnp.float32), filters.astype(jnp.float32), (1, 1), ((1, 1), (1, 1)), dimension_numbers=('NHWC', 'OHWI', 'NHWC'), precision=lax.Precision.HIGHEST)

def reference(latents, norm_gain, norm_shift, w_first, bias_first, w_second, bias_second):
    per_group = C // GROUPS
    values = latents.astype(jnp.float32).reshape(SLABS, VIEWS, ROWS_DEV, W_LAT, C)
    values = jnp.transpose(values, (1, 0, 2, 3, 4)).reshape(VIEWS, H_LAT, W_LAT, C)
    grouped = values.reshape(VIEWS, H_LAT, W_LAT, GROUPS, per_group)
    group_mean = lax.optimization_barrier(jnp.mean(grouped, axis=(0, 1, 2, 4), keepdims=True))
    group_var = lax.optimization_barrier(jnp.mean(jnp.square(grouped - group_mean), axis=(0, 1, 2, 4), keepdims=True))
    normed = ((grouped - group_mean) * lax.rsqrt(group_var + epsilon)).reshape(VIEWS, H_LAT, W_LAT, C)
    active = jax.nn.silu(normed * norm_gain + norm_shift).astype(jnp.bfloat16)
    mixed = (values + convolve(active, w_first) + bias_first).astype(jnp.bfloat16)
    doubled = jnp.repeat(jnp.repeat(mixed, 2, axis=1), 2, axis=2)
    decoded = (convolve(doubled, w_second) + bias_second).astype(jnp.bfloat16)
    decoded = decoded.reshape(VIEWS, SLABS, 2 * ROWS_DEV, 2 * W_LAT, C)
    decoded = jnp.transpose(decoded, (1, 0, 2, 3, 4))
    return decoded.reshape(VIEWS * 2 * H_LAT, 2 * W_LAT, C)
```

```python
import functools

import jax
import jax.numpy as jnp
from jax import lax
from jax.experimental import pallas as pl
from jax.experimental.pallas import tpu as pltpu
from jax.sharding import Mesh
from jax.sharding import PartitionSpec as P

GROUPS = 32
H_LAT = 32
AXES = ("view_0", "view_1", "view_2")
SCENE_VIEW = ("scene",) + AXES
EPSILON = 1e-06
F32 = jnp.float32
BF16 = jnp.bfloat16
MESH_ID = pl.DeviceIdType.MESH


def nt_dot(a, w):
    return lax.dot_general(a, w, (((1,), (1,)), ((), ())), preferred_element_type=F32)


def exchange_kernel(
    cols, latents, deep, stats,
    ybuf, xbuf, in_sem, ysend, yrecv, xsend, xrecv, hsend, hrecv,
):
    y = lax.axis_index("view_0")
    x = lax.axis_index("view_1")
    c = lax.axis_index("view_2")
    ny = lax.axis_size("view_0")
    nx = lax.axis_size("view_1")
    nc = lax.axis_size("view_2")
    rows = latents.shape[0]
    columns = latents.shape[1]
    halo = (deep.shape[0] - rows) // 2
    step = ny * (rows // cols) // H_LAT
    slot = x * nc + c
    members = nx * nc

    load = pltpu.make_async_copy(latents, deep.at[pl.ds(halo, rows)], in_sem)
    load.start()
    barrier = pltpu.get_barrier_semaphore()

    def y_peer(k):
        return lax.rem(y + k, ny)

    def x_peer(k):
        return lax.rem(slot + k, members)

    for k in range(1, ny):
        pl.semaphore_signal(barrier, inc=1, device_id={"view_0": y_peer(k)}, device_id_type=MESH_ID)
    for k in range(1, members):
        p = x_peer(k)
        pl.semaphore_signal(
            barrier, inc=1, device_id={"view_1": p // nc, "view_2": lax.rem(p, nc)}, device_id_type=MESH_ID
        )
    load.wait()

    total = jnp.zeros((8, columns), F32)
    squares = jnp.zeros((8, columns), F32)
    for i in range(0, rows, 64):
        v = deep[pl.ds(halo + i, 64), :].astype(F32)
        q = v * v
        for j in range(0, 64, 8):
            total = total + v[j : j + 8]
            squares = squares + q[j : j + 8]
    sub = lax.broadcasted_iota(jnp.int32, (8, columns), 0)
    both = jnp.where(
        sub == 0, jnp.sum(total, axis=0, keepdims=True), jnp.sum(squares, axis=0, keepdims=True)
    )
    lane = lax.broadcasted_iota(jnp.int32, (8, 128), 1)
    sub1 = lax.broadcasted_iota(jnp.int32, (8, 128), 0)
    packed = jnp.zeros((8, 128), F32)
    for t in range(columns // 128):
        tile = both[:, t * 128 : (t + 1) * 128]
        for d in (8, 4, 2, 1):
            tile = tile + pltpu.roll(tile, 128 - d, 1)
        s_part = pltpu.roll(tile, t, 1) if t else tile
        q_part = pltpu.roll(tile, t + 4, 1)
        packed = jnp.where((lax.rem(lane, 16) == t) & (sub1 == 0), s_part, packed)
        packed = jnp.where((lax.rem(lane, 16) == t + 4) & (sub1 == 1), q_part, packed)
    mine = jnp.sum(packed, axis=0, keepdims=True)
    ybuf[pl.ds(y, 1), :] = mine

    pl.semaphore_wait(barrier, ny - 1 + members - 1)

    def y_copy(k, row):
        return pltpu.make_async_remote_copy(
            src_ref=ybuf.at[pl.ds(row, 1)],
            dst_ref=ybuf.at[pl.ds(row, 1)],
            send_sem=ysend.at[k],
            recv_sem=yrecv.at[row],
            device_id={"view_0": y_peer(k)},
            device_id_type=MESH_ID,
        )

    def x_copy(k, row):
        p = x_peer(k)
        return pltpu.make_async_remote_copy(
            src_ref=xbuf.at[pl.ds(row, 1)],
            dst_ref=xbuf.at[pl.ds(row, 1)],
            send_sem=xsend.at[k],
            recv_sem=xrecv.at[row],
            device_id={"view_1": p // nc, "view_2": lax.rem(p, nc)},
            device_id_type=MESH_ID,
        )

    order_y = sorted(range(1, ny), key=lambda k: -min(k, ny - k))
    order_x = sorted(range(1, members), key=lambda k: -min(k, members - k))
    for k in order_y:
        y_copy(k, y).start()

    to_next = pltpu.make_async_remote_copy(
        src_ref=deep.at[pl.ds(rows, halo)],
        dst_ref=deep.at[pl.ds(0, halo)],
        send_sem=hsend.at[0],
        recv_sem=hrecv.at[0],
        device_id={"view_0": lax.rem(y + step, ny)},
        device_id_type=MESH_ID,
    )
    to_previous = pltpu.make_async_remote_copy(
        src_ref=deep.at[pl.ds(halo, halo)],
        dst_ref=deep.at[pl.ds(halo + rows, halo)],
        send_sem=hsend.at[1],
        recv_sem=hrecv.at[1],
        device_id={"view_0": lax.rem(y + ny - step, ny)},
        device_id_type=MESH_ID,
    )
    has_previous = y >= step
    has_next = y < ny - step

    @pl.when(has_next)
    def _():
        to_next.start()

    @pl.when(has_previous)
    def _():
        to_previous.start()

    for k in range(1, ny):
        y_copy(k, y_peer(k)).wait_recv()
    xbuf[pl.ds(slot, 1), :] = jnp.sum(ybuf[...], axis=0, keepdims=True)
    for k in order_x:
        x_copy(k, slot).start()
    for k in range(1, members):
        x_copy(k, x_peer(k)).wait_recv()
    stats[...] = jnp.broadcast_to(jnp.sum(xbuf[...], axis=0, keepdims=True), stats.shape)

    for k in range(1, ny):
        y_copy(k, y).wait_send()
    for k in range(1, members):
        x_copy(k, slot).wait_send()

    @pl.when(has_next)
    def _():
        to_next.wait_send()
        to_previous.wait_recv()

    @pl.when(has_previous)
    def _():
        to_previous.wait_send()
        to_next.wait_recv()


def shifted_down(v, first):
    row = lax.broadcasted_iota(jnp.int32, v.shape, 0)
    return jnp.where(row == 0, first, pltpu.roll(v, 1, 0))


def shifted_up(v, last):
    n = v.shape[0]
    row = lax.broadcasted_iota(jnp.int32, v.shape, 0)
    return jnp.where(row == n - 1, last, pltpu.roll(v, n - 1, 0))


def decode_kernel(
    entries, cols, deep, stats, gain, shift, bias1, bias2, w1, w2_hbm, out,
    w2, acat, m0, md, edge, keep_s, keep_x, z, obuf, w_sem, out_sem,
):
    channels = deep.shape[1]
    tall = deep.shape[0] // cols
    y_dev = lax.axis_index("view_0")
    ny = lax.axis_size("view_0")
    slab_rows = tall - 4
    step = ny * slab_rows // H_LAT
    has_previous = y_dev >= step
    has_next = y_dev < ny - step

    load = pltpu.make_async_copy(w2_hbm, w2, w_sem)
    load.start()

    st = stats[...]
    lane = lax.broadcasted_iota(jnp.int32, st.shape, 1)
    base = lane - lax.rem(lane, 16)
    means, rstds = [], []
    for t in range(channels // 128):
        s = jnp.take_along_axis(st, base + t, axis=1)
        q = jnp.take_along_axis(st, base + (t + 4), axis=1)
        mean = s / entries
        var = q / entries - mean * mean
        means.append(mean)
        rstds.append(lax.rsqrt(var + EPSILON))
    mean = jnp.concatenate(means, axis=1)[0:1]
    rstd = jnp.concatenate(rstds, axis=1)[0:1]
    scale = rstd * gain[...]
    offset = shift[...] - mean * scale
    half_scale = 0.5 * scale
    half_offset = 0.5 * offset

    for i in range(tall):
        h = deep[i * cols : (i + 1) * cols, :].astype(F32) * half_scale + half_offset
        a = h * jnp.tanh(h) + h
        if i < 2:
            a = jnp.where(has_previous, a, 0.0)
        if i >= tall - 2:
            a = jnp.where(has_next, a, 0.0)
        rows = slice(i * cols, (i + 1) * cols)
        acat[rows, 0:channels] = shifted_down(a, 0.0).astype(BF16)
        acat[rows, channels : 2 * channels] = a.astype(BF16)
        acat[rows, 2 * channels :] = shifted_up(a, 0.0).astype(BF16)

    mid = tall - 2
    half = mid // 2
    for part in range(2):
        m_rows = half * cols
        start = part * m_rows
        acc = None
        for r in range(3):
            for s in range(3):
                lhs = acat[start + r * cols : start + r * cols + m_rows, s * channels : (s + 1) * channels]
                term = nt_dot(lhs, w1[3 * r + s])
                acc = term if acc is None else acc + term
        for i in range(half):
            p = part * half + i
            v = acc[i * cols : (i + 1) * cols] + deep[(p + 1) * cols : (p + 2) * cols, :].astype(F32) + bias1[...]
            if p == 0:
                v = jnp.where(has_previous, v, 0.0)
            if p == mid - 1:
                v = jnp.where(has_next, v, 0.0)
            rows = slice(p * cols, (p + 1) * cols)
            m0[rows, :] = v.astype(BF16)
            md[rows, :] = shifted_down(v, 0.0).astype(BF16)
            edge[p : p + 1, :] = v[cols - 1 : cols]

    load.wait()

    def edge_rows(first, count):
        pad = jnp.zeros((16 - count, channels), F32)
        return jnp.concatenate([edge[first : first + count, :], pad], axis=0).astype(BF16)

    zero16 = jnp.zeros((16, channels), BF16)
    corners = slab_rows + 1
    cut = (corners + 1) // 2
    for lo, hi in ((0, cut), (cut, corners)):
        n = hi - lo
        nb = min(hi, slab_rows) - lo
        ss = sb = bs = bb = None

        def block(buf, first, count):
            return buf[first * cols : (first + count) * cols, :]

        def with_edge(buf, first, count, e):
            return jnp.concatenate([block(buf, first, count), e], axis=0)

        bb = nt_dot(block(m0, lo + 1, nb), w2[4])
        bs = nt_dot(with_edge(md, lo + 1, nb, edge_rows(lo + 1, nb)), w2[3])
        bs = bs + nt_dot(with_edge(m0, lo + 1, nb, zero16), w2[5])
        sb = nt_dot(block(m0, lo, n), w2[1]) + nt_dot(block(m0, lo + 1, n), w2[7])
        ss = nt_dot(with_edge(md, lo, n, edge_rows(lo, n)), w2[0])
        ss = ss + nt_dot(with_edge(m0, lo, n, zero16), w2[2])
        ss = ss + nt_dot(with_edge(md, lo + 1, n, edge_rows(lo + 1, n)), w2[6])
        ss = ss + nt_dot(with_edge(m0, lo + 1, n, zero16), w2[8])

        for i in range(lo, hi):
            k = i - lo
            s_main = ss[k * cols : (k + 1) * cols]
            s_edge = ss[n * cols + k : n * cols + k + 1]
            c_main = sb[k * cols : (k + 1) * cols] + bias2[...]
            for yy in (2 * i - 1, 2 * i):
                if not 0 <= yy < 2 * slab_rows:
                    continue
                b = yy // 2
                if b < lo:
                    u = s_main + keep_s[0:cols, :]
                    u_edge = s_edge + keep_x[0:1, :]
                    w = c_main + keep_s[cols : 2 * cols, :]
                else:
                    kb = b - lo
                    u = s_main + bs[kb * cols : (kb + 1) * cols]
                    u_edge = s_edge + bs[nb * cols + kb : nb * cols + kb + 1]
                    w = c_main + bb[kb * cols : (kb + 1) * cols]
                zi = yy % 2
                even = u + w
                odd = shifted_up(u, u_edge) + w
                for t in range(channels // 128):
                    lanes = slice(t * 128, (t + 1) * 128)
                    z[zi, t, pl.ds(0, cols, stride=2), :] = even[:, lanes]
                    z[zi, t, pl.ds(1, cols, stride=2), :] = odd[:, lanes]
                    obuf[yy, :, lanes] = z[zi, t].astype(BF16)
        if hi < corners:
            kb = nb - 1
            keep_s[0:cols, :] = bs[kb * cols : (kb + 1) * cols]
            keep_s[cols : 2 * cols, :] = bb[kb * cols : (kb + 1) * cols]
            keep_x[0:1, :] = bs[nb * cols + kb : nb * cols + kb + 1]
        y_lo = max(2 * lo - 1, 0)
        y_hi = min(2 * hi - 1, 2 * slab_rows)
        pltpu.make_async_copy(
            obuf.at[pl.ds(y_lo, y_hi - y_lo)], out.at[pl.ds(y_lo, y_hi - y_lo)], out_sem.at[0 if lo == 0 else 1]
        ).start()
    for n, (lo, hi) in enumerate(((0, cut), (cut, corners))):
        y_lo = max(2 * lo - 1, 0)
        y_hi = min(2 * hi - 1, 2 * slab_rows)
        pltpu.make_async_copy(
            obuf.at[pl.ds(y_lo, y_hi - y_lo)], out.at[pl.ds(y_lo, y_hi - y_lo)], out_sem.at[n]
        ).wait()


def exchange(flat, cols, ny, members):
    rows, channels = flat.shape
    vspec = pl.BlockSpec(memory_space=pltpu.VMEM)
    return pl.pallas_call(
        functools.partial(exchange_kernel, cols),
        out_shape=(
            pltpu.VMEM((rows + 4 * cols, channels), BF16),
            pltpu.VMEM((8, 128), F32),
        ),
        in_specs=[pl.BlockSpec(memory_space=pltpu.HBM)],
        out_specs=(vspec,) * 2,
        scratch_shapes=[
            pltpu.VMEM((ny, 128), F32),
            pltpu.VMEM((members, 128), F32),
            pltpu.SemaphoreType.DMA,
            pltpu.SemaphoreType.DMA((ny,)),
            pltpu.SemaphoreType.DMA((ny,)),
            pltpu.SemaphoreType.DMA((members,)),
            pltpu.SemaphoreType.DMA((members,)),
            pltpu.SemaphoreType.DMA((2,)),
            pltpu.SemaphoreType.DMA((2,)),
        ],
        compiler_params=pltpu.CompilerParams(
            collective_id=0, has_side_effects=True, vmem_limit_bytes=16 * 2**20
        ),
        cost_estimate=pl.CostEstimate(flops=2 * 10**9, bytes_accessed=2 * 10**6, transcendentals=0),
        name="exchange",
    )(pltpu.with_memory_space_constraint(flat, pltpu.HBM))


def decode(deep, stats, gain, shift, bias1, bias2, w1, w2, cols, entries):
    tall_rows, channels = deep.shape
    tall = tall_rows // cols
    slab_rows = tall - 4
    vspec = pl.BlockSpec(memory_space=pltpu.VMEM)
    return pl.pallas_call(
        functools.partial(decode_kernel, entries, cols),
        out_shape=jax.ShapeDtypeStruct((2 * slab_rows, 2 * cols, channels), BF16),
        in_specs=[vspec] * 7 + [pl.BlockSpec(memory_space=pltpu.HBM)],
        out_specs=pl.BlockSpec(memory_space=pl.ANY),
        scratch_shapes=[
            pltpu.VMEM(w2.shape, BF16),
            pltpu.VMEM((tall_rows, 3 * channels), BF16),
            pltpu.VMEM(((tall - 2) * cols, channels), BF16),
            pltpu.VMEM(((tall - 2) * cols, channels), BF16),
            pltpu.VMEM((24, channels), F32),
            pltpu.VMEM((2 * cols, channels), F32),
            pltpu.VMEM((8, channels), F32),
            pltpu.VMEM((2, channels // 128, 2 * cols, 128), F32),
            pltpu.VMEM((2 * slab_rows, 2 * cols, channels), BF16),
            pltpu.SemaphoreType.DMA,
            pltpu.SemaphoreType.DMA((2,)),
        ],
        compiler_params=pltpu.CompilerParams(vmem_limit_bytes=40 * 2**20),
        cost_estimate=pl.CostEstimate(flops=6 * 10**9, bytes_accessed=14 * 10**6, transcendentals=0),
        name="decode",
    )(deep, stats, gain, shift, bias1, bias2, w1, pltpu.with_memory_space_constraint(w2, pltpu.HBM))


def per_device(latents, norm_gain, norm_shift, w_first, bias_first, w_second, bias_second):
    slab_rows, cols, channels = latents.shape
    ny = lax.axis_size("view_0")
    members = lax.axis_size("view_1") * lax.axis_size("view_2")
    entries = float(slab_rows * cols * (channels // GROUPS) * ny * members)
    w1 = jnp.transpose(w_first, (1, 2, 0, 3)).reshape(9, channels, channels)
    w2 = jnp.transpose(w_second, (1, 2, 0, 3)).reshape(9, channels, channels)
    flat = latents.reshape(slab_rows * cols, channels)
    deep, stats = exchange(flat, cols, ny, members)
    row = lambda v: v.reshape(1, channels)
    return decode(
        deep, stats, row(norm_gain), row(norm_shift), row(bias_first), row(bias_second), w1, w2, cols, entries
    )


def solution(mesh):
    torus = Mesh(mesh.devices.reshape(mesh.shape["scene"], 8, 8, 2), SCENE_VIEW)
    in_specs = (P(SCENE_VIEW, None, None), P(), P(), P(), P(), P(), P())
    out_specs = P(SCENE_VIEW, None, None)
    return jax.shard_map(per_device, mesh=torus, in_specs=in_specs, out_specs=out_specs, check_vma=False)
```

```python
import functools

import jax
import jax.numpy as jnp
from jax import lax
from jax.experimental import pallas as pl
from jax.experimental.pallas import tpu as pltpu
from jax.sharding import Mesh
from jax.sharding import PartitionSpec as P

GROUPS = 32
H_LAT = 32
AXES = ("view_0", "view_1", "view_2")
SCENE_VIEW = ("scene",) + AXES
EPSILON = 1e-06
F32 = jnp.float32
BF16 = jnp.bfloat16
MESH_ID = pl.DeviceIdType.MESH


def nt_dot(a, w):
    return lax.dot_general(a, w, (((1,), (1,)), ((), ())), preferred_element_type=F32)


def exchange_kernel(
    cols, latents, w1, w2, deep, stats, w1v, w2v,
    ybuf, xbuf, rootbuf, restbuf,
    in_sem, w_sem, ysend, yrecv, xsend, xrecv, dsend, rsend, rrecv, msend, mrecv, hsend, hrecv,
):
    y = lax.axis_index("view_0")
    x = lax.axis_index("view_1")
    c = lax.axis_index("view_2")
    ny = lax.axis_size("view_0")
    nx = lax.axis_size("view_1")
    nc = lax.axis_size("view_2")
    rows = latents.shape[0]
    columns = latents.shape[1]
    halo = (deep.shape[0] - rows) // 2
    step = ny * (rows // cols) // H_LAT
    slot = x * nc + c
    members = nx * nc
    everyone = ny * members

    is_root = (y == 0) & (slot == 0)
    not_root = jnp.logical_not(is_root)
    is_deputy = (y == 1) & (slot == 0)
    first_row = (y == 0) & not_root
    is_mate = (y == 0) & (slot == 1)

    load = pltpu.make_async_copy(latents, deep.at[pl.ds(halo, rows)], in_sem)
    load.start()
    ybuf[...] = jnp.zeros_like(ybuf)

    def y_peer(k):
        return lax.rem(y + k, ny)

    def x_peer(k):
        return lax.rem(slot + k, members)

    def member(row, p):
        return {"view_0": row, "view_1": p // nc, "view_2": lax.rem(p, nc)}

    barrier = pltpu.get_barrier_semaphore()

    def greet(device):
        pl.semaphore_signal(barrier, inc=1, device_id=device, device_id_type=MESH_ID)

    @pl.when(not_root)
    def _():
        greet(member(0, 0))
        for k in range(1, ny):
            p = y_peer(k)

            @pl.when((p != 0) | (slot != 0))
            def _():
                greet(member(p, slot))

        for k in range(1, members):
            p = x_peer(k)

            @pl.when((y != 0) | (p != 0))
            def _():
                greet(member(y, p))

    @pl.when(first_row)
    def _():
        greet(member(1, 0))

    load.wait()
    weights = [pltpu.make_async_copy(w1, w1v, w_sem.at[0]), pltpu.make_async_copy(w2, w2v, w_sem.at[1])]

    total = jnp.zeros((8, columns), F32)
    squares = jnp.zeros((8, columns), F32)
    for i in range(0, rows, 64):
        v = deep[pl.ds(halo + i, 64), :].astype(F32)
        q = v * v
        for j in range(0, 64, 8):
            total = total + v[j : j + 8]
            squares = squares + q[j : j + 8]
    sub = lax.broadcasted_iota(jnp.int32, (8, columns), 0)
    both = jnp.where(
        sub == 0, jnp.sum(total, axis=0, keepdims=True), jnp.sum(squares, axis=0, keepdims=True)
    )
    lane = lax.broadcasted_iota(jnp.int32, (8, 128), 1)
    sub1 = lax.broadcasted_iota(jnp.int32, (8, 128), 0)
    packed = jnp.zeros((8, 128), F32)
    for t in range(columns // 128):
        tile = both[:, t * 128 : (t + 1) * 128]
        for d in (8, 4, 2, 1):
            tile = tile + pltpu.roll(tile, 128 - d, 1)
        s_part = pltpu.roll(tile, t, 1) if t else tile
        q_part = pltpu.roll(tile, t + 4, 1)
        packed = jnp.where((lax.rem(lane, 16) == t) & (sub1 == 0), s_part, packed)
        packed = jnp.where((lax.rem(lane, 16) == t + 4) & (sub1 == 1), q_part, packed)
    mine = jnp.sum(packed, axis=0, keepdims=True)

    def remote(src, dst, send, recv, device):
        return pltpu.make_async_remote_copy(
            src_ref=src, dst_ref=dst, send_sem=send, recv_sem=recv, device_id=device, device_id_type=MESH_ID
        )

    def y_copy(k, row):
        line = ybuf.at[pl.ds(row, 1)]
        return remote(line, line, ysend.at[k], yrecv.at[row], member(y_peer(k), slot))

    def x_copy(k, row):
        line = xbuf.at[pl.ds(row, 1)]
        return remote(line, line, xsend.at[k], xrecv.at[row], member(y, x_peer(k)))

    def deputy_copy(p):
        line = xbuf.at[pl.ds(0, 1)]
        return remote(line, line, dsend.at[p], xrecv.at[0], member(0, p))

    def root_copy(p):
        return remote(rootbuf, rootbuf, rsend.at[p], rrecv, member(p // members, lax.rem(p, members)))

    mate_copy = remote(restbuf, restbuf, msend, mrecv, member(0, 0))
    to_next = remote(
        deep.at[pl.ds(rows, halo)], deep.at[pl.ds(0, halo)], hsend.at[0], hrecv.at[0],
        member(lax.rem(y + step, ny), slot),
    )
    to_previous = remote(
        deep.at[pl.ds(halo, halo)], deep.at[pl.ds(halo + rows, halo)], hsend.at[1], hrecv.at[1],
        member(lax.rem(y + ny - step, ny), slot),
    )
    has_previous = y >= step
    has_next = y < ny - step
    meets_root = (y == step) & (slot == 0)

    @pl.when(is_root)
    def _():
        rootbuf[...] = mine
        pl.semaphore_wait(barrier, everyone - 1)
        half = nx // 2
        near = sorted(range(1, members), key=lambda p: -min(p // nc, nx - p // nc))
        for p in near:
            root_copy(p).start()
        lax.fori_loop(members, everyone, lambda p, _: (root_copy(p).start(), 0)[1], 0)
        to_next.start()
        for copy in weights:
            copy.start()
        to_previous.wait_recv()
        mate_copy.wait_recv()
        stats[...] = jnp.broadcast_to(mine + restbuf[...], stats.shape)
        lax.fori_loop(1, everyone, lambda p, _: (root_copy(p).wait_send(), 0)[1], 0)
        to_next.wait_send()
        for copy in weights:
            copy.wait()

    @pl.when(not_root)
    def _():
        for copy in weights:
            copy.start()
        ybuf[pl.ds(y, 1), :] = mine
        lost = jnp.where(slot == 0, 1, 0) + jnp.where(y == 0, 1, 0)
        extra = jnp.where(is_deputy, members - 1, 0)
        pl.semaphore_wait(barrier, ny - 1 + members - 1 - lost + extra)

        for k in sorted(range(1, ny), key=lambda k: -min(k, ny - k)):

            @pl.when((y_peer(k) != 0) | (slot != 0))
            def _():
                y_copy(k, y).start()

        @pl.when(has_next)
        def _():
            to_next.start()

        @pl.when(has_previous & jnp.logical_not(meets_root))
        def _():
            to_previous.start()

        for k in range(1, ny):

            @pl.when((y_peer(k) != 0) | (slot != 0))
            def _():
                y_copy(k, y_peer(k)).wait_recv()

        xbuf[pl.ds(slot, 1), :] = jnp.sum(ybuf[...], axis=0, keepdims=True)
        for k in sorted(range(1, members), key=lambda k: -min(k, members - k)):

            @pl.when((y != 0) | (x_peer(k) != 0))
            def _():
                x_copy(k, slot).start()

        @pl.when(is_deputy)
        def _():
            for p in range(1, members):
                deputy_copy(p).start()

        for k in range(1, members):
            x_copy(k, x_peer(k)).wait_recv()
        rest = jnp.sum(xbuf[...], axis=0, keepdims=True)

        for copy in weights:
            copy.wait()
        for k in range(1, ny):

            @pl.when((y_peer(k) != 0) | (slot != 0))
            def _():
                y_copy(k, y).wait_send()

        for k in range(1, members):

            @pl.when((y != 0) | (x_peer(k) != 0))
            def _():
                x_copy(k, slot).wait_send()

        @pl.when(is_deputy)
        def _():
            for p in range(1, members):
                deputy_copy(p).wait_send()

        @pl.when(has_next)
        def _():
            to_next.wait_send()
            to_previous.wait_recv()

        @pl.when(has_previous & jnp.logical_not(meets_root))
        def _():
            to_previous.wait_send()
            to_next.wait_recv()

        restbuf[...] = rest
        root_copy(0).wait_recv()
        stats[...] = jnp.broadcast_to(rest + rootbuf[...], stats.shape)

        @pl.when(is_mate)
        def _():
            mate_copy.start()
            mate_copy.wait_send()

        @pl.when(meets_root)
        def _():
            to_previous.start()
            to_next.wait_recv()
            to_previous.wait_send()


def shifted_down(v, first):
    row = lax.broadcasted_iota(jnp.int32, v.shape, 0)
    return jnp.where(row == 0, first, pltpu.roll(v, 1, 0))


def shifted_up(v, last):
    n = v.shape[0]
    row = lax.broadcasted_iota(jnp.int32, v.shape, 0)
    return jnp.where(row == n - 1, last, pltpu.roll(v, n - 1, 0))


def decode_kernel(
    entries, cols, deep, stats, gain, shift, bias1, bias2, w1, w2, out,
    acat, m0, md, edge, keep_s, keep_x, z, obuf, out_sem,
):
    channels = deep.shape[1]
    tall = deep.shape[0] // cols
    y_dev = lax.axis_index("view_0")
    ny = lax.axis_size("view_0")
    slab_rows = tall - 4
    step = ny * slab_rows // H_LAT
    has_previous = y_dev >= step
    has_next = y_dev < ny - step

    st = stats[...]
    lane = lax.broadcasted_iota(jnp.int32, st.shape, 1)
    base = lane - lax.rem(lane, 16)
    means, rstds = [], []
    for t in range(channels // 128):
        s = jnp.take_along_axis(st, base + t, axis=1)
        q = jnp.take_along_axis(st, base + (t + 4), axis=1)
        mean = s / entries
        var = q / entries - mean * mean
        means.append(mean)
        rstds.append(lax.rsqrt(var + EPSILON))
    mean = jnp.concatenate(means, axis=1)[0:1]
    rstd = jnp.concatenate(rstds, axis=1)[0:1]
    scale = rstd * gain[...]
    offset = shift[...] - mean * scale
    half_scale = 0.5 * scale
    half_offset = 0.5 * offset

    for i in range(tall):
        h = deep[i * cols : (i + 1) * cols, :].astype(F32) * half_scale + half_offset
        a = h * jnp.tanh(h) + h
        if i < 2:
            a = jnp.where(has_previous, a, 0.0)
        if i >= tall - 2:
            a = jnp.where(has_next, a, 0.0)
        rows = slice(i * cols, (i + 1) * cols)
        acat[rows, 0:channels] = shifted_down(a, 0.0).astype(BF16)
        acat[rows, channels : 2 * channels] = a.astype(BF16)
        acat[rows, 2 * channels :] = shifted_up(a, 0.0).astype(BF16)

    mid = tall - 2
    half = mid // 2
    for part in range(2):
        m_rows = half * cols
        start = part * m_rows
        acc = None
        for r in range(3):
            for s in range(3):
                lhs = acat[start + r * cols : start + r * cols + m_rows, s * channels : (s + 1) * channels]
                term = nt_dot(lhs, w1[3 * r + s])
                acc = term if acc is None else acc + term
        for i in range(half):
            p = part * half + i
            v = acc[i * cols : (i + 1) * cols] + deep[(p + 1) * cols : (p + 2) * cols, :].astype(F32) + bias1[...]
            if p == 0:
                v = jnp.where(has_previous, v, 0.0)
            if p == mid - 1:
                v = jnp.where(has_next, v, 0.0)
            rows = slice(p * cols, (p + 1) * cols)
            m0[rows, :] = v.astype(BF16)
            md[rows, :] = shifted_down(v, 0.0).astype(BF16)
            edge[p : p + 1, :] = v[cols - 1 : cols]

    def edge_rows(first, count):
        pad = jnp.zeros((16 - count, channels), F32)
        return jnp.concatenate([edge[first : first + count, :], pad], axis=0).astype(BF16)

    zero16 = jnp.zeros((16, channels), BF16)
    corners = slab_rows + 1
    cut = (corners + 1) // 2
    for lo, hi in ((0, cut), (cut, corners)):
        n = hi - lo
        nb = min(hi, slab_rows) - lo
        ss = sb = bs = bb = None

        def block(buf, first, count):
            return buf[first * cols : (first + count) * cols, :]

        def with_edge(buf, first, count, e):
            return jnp.concatenate([block(buf, first, count), e], axis=0)

        bb = nt_dot(block(m0, lo + 1, nb), w2[4])
        bs = nt_dot(with_edge(md, lo + 1, nb, edge_rows(lo + 1, nb)), w2[3])
        bs = bs + nt_dot(with_edge(m0, lo + 1, nb, zero16), w2[5])
        sb = nt_dot(block(m0, lo, n), w2[1]) + nt_dot(block(m0, lo + 1, n), w2[7])
        ss = nt_dot(with_edge(md, lo, n, edge_rows(lo, n)), w2[0])
        ss = ss + nt_dot(with_edge(m0, lo, n, zero16), w2[2])
        ss = ss + nt_dot(with_edge(md, lo + 1, n, edge_rows(lo + 1, n)), w2[6])
        ss = ss + nt_dot(with_edge(m0, lo + 1, n, zero16), w2[8])

        for i in range(lo, hi):
            k = i - lo
            s_main = ss[k * cols : (k + 1) * cols]
            s_edge = ss[n * cols + k : n * cols + k + 1]
            c_main = sb[k * cols : (k + 1) * cols] + bias2[...]
            for yy in (2 * i - 1, 2 * i):
                if not 0 <= yy < 2 * slab_rows:
                    continue
                b = yy // 2
                if b < lo:
                    u = s_main + keep_s[0:cols, :]
                    u_edge = s_edge + keep_x[0:1, :]
                    w = c_main + keep_s[cols : 2 * cols, :]
                else:
                    kb = b - lo
                    u = s_main + bs[kb * cols : (kb + 1) * cols]
                    u_edge = s_edge + bs[nb * cols + kb : nb * cols + kb + 1]
                    w = c_main + bb[kb * cols : (kb + 1) * cols]
                zi = yy % 2
                even = u + w
                odd = shifted_up(u, u_edge) + w
                for t in range(channels // 128):
                    lanes = slice(t * 128, (t + 1) * 128)
                    z[zi, t, pl.ds(0, cols, stride=2), :] = even[:, lanes]
                    z[zi, t, pl.ds(1, cols, stride=2), :] = odd[:, lanes]
                    obuf[yy, :, lanes] = z[zi, t].astype(BF16)
        if hi < corners:
            kb = nb - 1
            keep_s[0:cols, :] = bs[kb * cols : (kb + 1) * cols]
            keep_s[cols : 2 * cols, :] = bb[kb * cols : (kb + 1) * cols]
            keep_x[0:1, :] = bs[nb * cols + kb : nb * cols + kb + 1]
        y_lo = max(2 * lo - 1, 0)
        y_hi = min(2 * hi - 1, 2 * slab_rows)
        pltpu.make_async_copy(
            obuf.at[pl.ds(y_lo, y_hi - y_lo)], out.at[pl.ds(y_lo, y_hi - y_lo)], out_sem.at[0 if lo == 0 else 1]
        ).start()
    for n, (lo, hi) in enumerate(((0, cut), (cut, corners))):
        y_lo = max(2 * lo - 1, 0)
        y_hi = min(2 * hi - 1, 2 * slab_rows)
        pltpu.make_async_copy(
            obuf.at[pl.ds(y_lo, y_hi - y_lo)], out.at[pl.ds(y_lo, y_hi - y_lo)], out_sem.at[n]
        ).wait()


def in_hbm(array):
    return pltpu.with_memory_space_constraint(array, pltpu.HBM)


def exchange(flat, w1, w2, cols, ny, members):
    rows, channels = flat.shape
    hbm = pl.BlockSpec(memory_space=pltpu.HBM)
    vmem = pl.BlockSpec(memory_space=pltpu.VMEM)
    dma = pltpu.SemaphoreType.DMA
    return pl.pallas_call(
        functools.partial(exchange_kernel, cols),
        out_shape=(
            pltpu.VMEM((rows + 4 * cols, channels), BF16),
            pltpu.VMEM((8, 128), F32),
            pltpu.VMEM(w1.shape, BF16),
            pltpu.VMEM(w2.shape, BF16),
        ),
        in_specs=[hbm] * 3,
        out_specs=(vmem,) * 4,
        scratch_shapes=[
            pltpu.VMEM((ny, 128), F32),
            pltpu.VMEM((members, 128), F32),
            pltpu.VMEM((1, 128), F32),
            pltpu.VMEM((1, 128), F32),
            dma,
            dma((2,)),
            dma((ny,)),
            dma((ny,)),
            dma((members,)),
            dma((members,)),
            dma((members,)),
            dma((ny * members,)),
            dma,
            dma,
            dma,
            dma((2,)),
            dma((2,)),
        ],
        compiler_params=pltpu.CompilerParams(
            collective_id=0, has_side_effects=True, vmem_limit_bytes=16 * 2**20
        ),
        cost_estimate=pl.CostEstimate(flops=2 * 10**9, bytes_accessed=2 * 10**6, transcendentals=0),
        name="exchange",
    )(in_hbm(flat), in_hbm(w1), in_hbm(w2))


def decode(deep, stats, gain, shift, bias1, bias2, w1, w2, cols, entries):
    tall_rows, channels = deep.shape
    tall = tall_rows // cols
    slab_rows = tall - 4
    vspec = pl.BlockSpec(memory_space=pltpu.VMEM)
    return pl.pallas_call(
        functools.partial(decode_kernel, entries, cols),
        out_shape=jax.ShapeDtypeStruct((2 * slab_rows, 2 * cols, channels), BF16),
        in_specs=[vspec] * 8,
        out_specs=pl.BlockSpec(memory_space=pl.ANY),
        scratch_shapes=[
            pltpu.VMEM((tall_rows, 3 * channels), BF16),
            pltpu.VMEM(((tall - 2) * cols, channels), BF16),
            pltpu.VMEM(((tall - 2) * cols, channels), BF16),
            pltpu.VMEM((24, channels), F32),
            pltpu.VMEM((2 * cols, channels), F32),
            pltpu.VMEM((8, channels), F32),
            pltpu.VMEM((2, channels // 128, 2 * cols, 128), F32),
            pltpu.VMEM((2 * slab_rows, 2 * cols, channels), BF16),
            pltpu.SemaphoreType.DMA((2,)),
        ],
        compiler_params=pltpu.CompilerParams(vmem_limit_bytes=40 * 2**20),
        cost_estimate=pl.CostEstimate(flops=6 * 10**9, bytes_accessed=14 * 10**6, transcendentals=0),
        name="decode",
    )(deep, stats, gain, shift, bias1, bias2, w1, w2)


def per_device(latents, norm_gain, norm_shift, w_first, bias_first, w_second, bias_second):
    slab_rows, cols, channels = latents.shape
    ny = lax.axis_size("view_0")
    members = lax.axis_size("view_1") * lax.axis_size("view_2")
    entries = float(slab_rows * cols * (channels // GROUPS) * ny * members)
    w1 = jnp.transpose(w_first, (1, 2, 0, 3)).reshape(9, channels, channels)
    w2 = jnp.transpose(w_second, (1, 2, 0, 3)).reshape(9, channels, channels)
    flat = latents.reshape(slab_rows * cols, channels)
    deep, stats, w1, w2 = exchange(flat, w1, w2, cols, ny, members)
    row = lambda v: v.reshape(1, channels)
    return decode(
        deep, stats, row(norm_gain), row(norm_shift), row(bias_first), row(bias_second), w1, w2, cols, entries
    )


def solution(mesh):
    torus = Mesh(mesh.devices.reshape(mesh.shape["scene"], 8, 8, 2), SCENE_VIEW)
    in_specs = (P(SCENE_VIEW, None, None), P(), P(), P(), P(), P(), P())
    out_specs = P(SCENE_VIEW, None, None)
    return jax.shard_map(per_device, mesh=torus, in_specs=in_specs, out_specs=out_specs, check_vma=False)
```

```python
import functools

import jax
import jax.numpy as jnp
from jax import lax
from jax.experimental import pallas as pl
from jax.experimental.pallas import tpu as pltpu
from jax.sharding import Mesh
from jax.sharding import PartitionSpec as P

GROUPS = 32
H_LAT = 32
AXES = ("view_0", "view_1", "view_2")
SCENE_VIEW = ("scene",) + AXES
EPSILON = 1e-06
F32 = jnp.float32
BF16 = jnp.bfloat16
MESH_ID = pl.DeviceIdType.MESH


def nt_dot(a, w):
    return lax.dot_general(a, w, (((1,), (1,)), ((), ())), preferred_element_type=F32)


def exchange_kernel(
    cols, latents, w1, w2, deep, stats, w1v, w2v,
    gather, total,
    in_sem, w_sem, gsend, grecv, rowsend, colsend, trecv, hsend, hrecv, ready,
):
    y = lax.axis_index("view_0")
    x = lax.axis_index("view_1")
    c = lax.axis_index("view_2")
    ny = lax.axis_size("view_0")
    nx = lax.axis_size("view_1")
    nc = lax.axis_size("view_2")
    rows = latents.shape[0]
    columns = latents.shape[1]
    halo = (deep.shape[0] - rows) // 2
    step = ny * (rows // cols) // H_LAT
    slot = x * nc + c
    members = nx * nc
    everyone = ny * members
    hub = 1
    me = y * members + slot
    is_hub = me == hub
    not_hub = jnp.logical_not(is_hub)
    has_previous = y >= step
    has_next = y < ny - step

    load = pltpu.make_async_copy(latents, deep.at[pl.ds(halo, rows)], in_sem)
    load.start()
    weights = [pltpu.make_async_copy(w1, w1v, w_sem.at[0]), pltpu.make_async_copy(w2, w2v, w_sem.at[1])]

    def member(row, p):
        return {"view_0": row, "view_1": p // nc, "view_2": lax.rem(p, nc)}

    barrier = pltpu.get_barrier_semaphore()

    def greet(device):
        pl.semaphore_signal(barrier, inc=1, device_id=device, device_id_type=MESH_ID)

    @pl.when(is_hub)
    def _():
        def body(p, carry):
            q = lax.rem(hub + p, everyone)
            greet(member(q // members, lax.rem(q, members)))
            return carry

        lax.fori_loop(1, everyone, body, 0)

    @pl.when(has_previous)
    def _():
        greet(member(lax.rem(y + ny - step, ny), slot))

    load.wait()
    for copy in weights:
        copy.start()

    sums = jnp.zeros((8, columns), F32)
    squares = jnp.zeros((8, columns), F32)
    for i in range(0, rows, 64):
        v = deep[pl.ds(halo + i, 64), :].astype(F32)
        q = v * v
        for j in range(0, 64, 8):
            sums = sums + v[j : j + 8]
            squares = squares + q[j : j + 8]
    sub = lax.broadcasted_iota(jnp.int32, (8, columns), 0)
    both = jnp.where(
        sub == 0, jnp.sum(sums, axis=0, keepdims=True), jnp.sum(squares, axis=0, keepdims=True)
    )
    lane = lax.broadcasted_iota(jnp.int32, (8, 128), 1)
    sub1 = lax.broadcasted_iota(jnp.int32, (8, 128), 0)
    packed = jnp.zeros((8, 128), F32)
    for t in range(columns // 128):
        tile = both[:, t * 128 : (t + 1) * 128]
        for d in (8, 4, 2, 1):
            tile = tile + pltpu.roll(tile, 128 - d, 1)
        s_part = pltpu.roll(tile, t, 1) if t else tile
        q_part = pltpu.roll(tile, t + 4, 1)
        packed = jnp.where((lax.rem(lane, 16) == t) & (sub1 == 0), s_part, packed)
        packed = jnp.where((lax.rem(lane, 16) == t + 4) & (sub1 == 1), q_part, packed)
    gather[pl.ds(me, 1), :] = jnp.sum(packed, axis=0, keepdims=True)

    pl.semaphore_wait(barrier, jnp.where(is_hub, 0, 1) + jnp.where(has_next, 1, 0))

    def remote(src, dst, send, recv, device):
        return pltpu.make_async_remote_copy(
            src_ref=src, dst_ref=dst, send_sem=send, recv_sem=recv, device_id=device, device_id_type=MESH_ID
        )

    def to_row(p):
        return remote(total, total, rowsend.at[p], trecv, member(0, p))

    def to_column(k):
        return remote(total, total, colsend.at[k], trecv, member(k, slot))

    line = gather.at[pl.ds(me, 1)]
    to_hub = remote(line, line, gsend, grecv, member(0, hub))
    following = member(lax.rem(y + step, ny), slot)
    to_next = remote(
        deep.at[pl.ds(rows, halo)], deep.at[pl.ds(0, halo)], hsend.at[0], hrecv.at[0], following
    )
    to_previous = remote(
        deep.at[pl.ds(halo, halo)], deep.at[pl.ds(halo + rows, halo)], hsend.at[1], hrecv.at[1],
        member(lax.rem(y + ny - step, ny), slot),
    )

    @pl.when(not_hub)
    def _():
        to_hub.start()

    @pl.when(has_next)
    def _():
        pl.semaphore_signal(ready, inc=1, device_id=following, device_id_type=MESH_ID)
        to_next.start()

    @pl.when(has_previous)
    def _():
        pl.semaphore_wait(ready, 1)
        to_previous.start()

    @pl.when(not_hub)
    def _():
        to_hub.wait_send()

    far_first = sorted(
        (p for p in range(members) if p != hub), key=lambda p: -min(p // nc, nx - p // nc)
    )

    @pl.when(is_hub)
    def _():
        arrivals = gather.at[pl.ds(1, everyone - 1)]
        pltpu.make_async_copy(arrivals, arrivals, grecv).wait()
        total[...] = jnp.sum(gather[...], axis=0, keepdims=True)
        for p in far_first:
            to_row(p).start()

    @pl.when(not_hub)
    def _():
        to_row(0).wait_recv()

    @pl.when(y == 0)
    def _():
        for k in range(1, ny):
            to_column(k).start()

    stats[...] = jnp.broadcast_to(total[...], stats.shape)

    for copy in weights:
        copy.wait()

    @pl.when(has_next)
    def _():
        to_next.wait_send()
        to_previous.wait_recv()

    @pl.when(has_previous)
    def _():
        to_previous.wait_send()
        to_next.wait_recv()

    @pl.when(is_hub)
    def _():
        for p in far_first:
            to_row(p).wait_send()

    @pl.when(y == 0)
    def _():
        for k in range(1, ny):
            to_column(k).wait_send()


def shifted_down(v, first):
    row = lax.broadcasted_iota(jnp.int32, v.shape, 0)
    return jnp.where(row == 0, first, pltpu.roll(v, 1, 0))


def shifted_up(v, last):
    n = v.shape[0]
    row = lax.broadcasted_iota(jnp.int32, v.shape, 0)
    return jnp.where(row == n - 1, last, pltpu.roll(v, n - 1, 0))


def decode_kernel(
    entries, cols, deep, stats, gain, shift, bias1, bias2, w1, w2, out,
    acat, m0, md, edge, keep_s, keep_x, z, obuf, out_sem,
):
    channels = deep.shape[1]
    tall = deep.shape[0] // cols
    y_dev = lax.axis_index("view_0")
    ny = lax.axis_size("view_0")
    slab_rows = tall - 4
    step = ny * slab_rows // H_LAT
    has_previous = y_dev >= step
    has_next = y_dev < ny - step

    st = stats[...]
    lane = lax.broadcasted_iota(jnp.int32, st.shape, 1)
    base = lane - lax.rem(lane, 16)
    means, rstds = [], []
    for t in range(channels // 128):
        s = jnp.take_along_axis(st, base + t, axis=1)
        q = jnp.take_along_axis(st, base + (t + 4), axis=1)
        mean = s / entries
        var = q / entries - mean * mean
        means.append(mean)
        rstds.append(lax.rsqrt(var + EPSILON))
    mean = jnp.concatenate(means, axis=1)[0:1]
    rstd = jnp.concatenate(rstds, axis=1)[0:1]
    scale = rstd * gain[...]
    offset = shift[...] - mean * scale
    half_scale = 0.5 * scale
    half_offset = 0.5 * offset

    for i in range(tall):
        h = deep[i * cols : (i + 1) * cols, :].astype(F32) * half_scale + half_offset
        a = h * jnp.tanh(h) + h
        if i < 2:
            a = jnp.where(has_previous, a, 0.0)
        if i >= tall - 2:
            a = jnp.where(has_next, a, 0.0)
        rows = slice(i * cols, (i + 1) * cols)
        acat[rows, 0:channels] = shifted_down(a, 0.0).astype(BF16)
        acat[rows, channels : 2 * channels] = a.astype(BF16)
        acat[rows, 2 * channels :] = shifted_up(a, 0.0).astype(BF16)

    mid = tall - 2
    half = mid // 2
    for part in range(2):
        m_rows = half * cols
        start = part * m_rows
        acc = None
        for r in range(3):
            for s in range(3):
                lhs = acat[start + r * cols : start + r * cols + m_rows, s * channels : (s + 1) * channels]
                term = nt_dot(lhs, w1[3 * r + s])
                acc = term if acc is None else acc + term
        for i in range(half):
            p = part * half + i
            v = acc[i * cols : (i + 1) * cols] + deep[(p + 1) * cols : (p + 2) * cols, :].astype(F32) + bias1[...]
            if p == 0:
                v = jnp.where(has_previous, v, 0.0)
            if p == mid - 1:
                v = jnp.where(has_next, v, 0.0)
            rows = slice(p * cols, (p + 1) * cols)
            m0[rows, :] = v.astype(BF16)
            md[rows, :] = shifted_down(v, 0.0).astype(BF16)
            edge[p : p + 1, :] = v[cols - 1 : cols]

    def edge_rows(first, count):
        pad = jnp.zeros((16 - count, channels), F32)
        return jnp.concatenate([edge[first : first + count, :], pad], axis=0).astype(BF16)

    zero16 = jnp.zeros((16, channels), BF16)
    corners = slab_rows + 1
    cut = (corners + 1) // 2
    for lo, hi in ((0, cut), (cut, corners)):
        n = hi - lo
        nb = min(hi, slab_rows) - lo
        ss = sb = bs = bb = None

        def block(buf, first, count):
            return buf[first * cols : (first + count) * cols, :]

        def with_edge(buf, first, count, e):
            return jnp.concatenate([block(buf, first, count), e], axis=0)

        bb = nt_dot(block(m0, lo + 1, nb), w2[4])
        bs = nt_dot(with_edge(md, lo + 1, nb, edge_rows(lo + 1, nb)), w2[3])
        bs = bs + nt_dot(with_edge(m0, lo + 1, nb, zero16), w2[5])
        sb = nt_dot(block(m0, lo, n), w2[1]) + nt_dot(block(m0, lo + 1, n), w2[7])
        ss = nt_dot(with_edge(md, lo, n, edge_rows(lo, n)), w2[0])
        ss = ss + nt_dot(with_edge(m0, lo, n, zero16), w2[2])
        ss = ss + nt_dot(with_edge(md, lo + 1, n, edge_rows(lo + 1, n)), w2[6])
        ss = ss + nt_dot(with_edge(m0, lo + 1, n, zero16), w2[8])

        for i in range(lo, hi):
            k = i - lo
            s_main = ss[k * cols : (k + 1) * cols]
            s_edge = ss[n * cols + k : n * cols + k + 1]
            c_main = sb[k * cols : (k + 1) * cols] + bias2[...]
            for yy in (2 * i - 1, 2 * i):
                if not 0 <= yy < 2 * slab_rows:
                    continue
                b = yy // 2
                if b < lo:
                    u = s_main + keep_s[0:cols, :]
                    u_edge = s_edge + keep_x[0:1, :]
                    w = c_main + keep_s[cols : 2 * cols, :]
                else:
                    kb = b - lo
                    u = s_main + bs[kb * cols : (kb + 1) * cols]
                    u_edge = s_edge + bs[nb * cols + kb : nb * cols + kb + 1]
                    w = c_main + bb[kb * cols : (kb + 1) * cols]
                zi = yy % 2
                even = u + w
                odd = shifted_up(u, u_edge) + w
                for t in range(channels // 128):
                    lanes = slice(t * 128, (t + 1) * 128)
                    z[zi, t, pl.ds(0, cols, stride=2), :] = even[:, lanes]
                    z[zi, t, pl.ds(1, cols, stride=2), :] = odd[:, lanes]
                    obuf[yy, :, lanes] = z[zi, t].astype(BF16)
        if hi < corners:
            kb = nb - 1
            keep_s[0:cols, :] = bs[kb * cols : (kb + 1) * cols]
            keep_s[cols : 2 * cols, :] = bb[kb * cols : (kb + 1) * cols]
            keep_x[0:1, :] = bs[nb * cols + kb : nb * cols + kb + 1]
        y_lo = max(2 * lo - 1, 0)
        y_hi = min(2 * hi - 1, 2 * slab_rows)
        pltpu.make_async_copy(
            obuf.at[pl.ds(y_lo, y_hi - y_lo)], out.at[pl.ds(y_lo, y_hi - y_lo)], out_sem.at[0 if lo == 0 else 1]
        ).start()
    for n, (lo, hi) in enumerate(((0, cut), (cut, corners))):
        y_lo = max(2 * lo - 1, 0)
        y_hi = min(2 * hi - 1, 2 * slab_rows)
        pltpu.make_async_copy(
            obuf.at[pl.ds(y_lo, y_hi - y_lo)], out.at[pl.ds(y_lo, y_hi - y_lo)], out_sem.at[n]
        ).wait()


def in_hbm(array):
    return pltpu.with_memory_space_constraint(array, pltpu.HBM)


def exchange(flat, w1, w2, cols, ny, members):
    rows, channels = flat.shape
    hbm = pl.BlockSpec(memory_space=pltpu.HBM)
    vmem = pl.BlockSpec(memory_space=pltpu.VMEM)
    dma = pltpu.SemaphoreType.DMA
    return pl.pallas_call(
        functools.partial(exchange_kernel, cols),
        out_shape=(
            pltpu.VMEM((rows + 4 * cols, channels), BF16),
            pltpu.VMEM((8, 128), F32),
            pltpu.VMEM(w1.shape, BF16),
            pltpu.VMEM(w2.shape, BF16),
        ),
        in_specs=[hbm] * 3,
        out_specs=(vmem,) * 4,
        scratch_shapes=[
            pltpu.VMEM((ny * members, 128), F32),
            pltpu.VMEM((1, 128), F32),
            dma,
            dma((2,)),
            dma,
            dma,
            dma((members,)),
            dma((ny,)),
            dma,
            dma((2,)),
            dma((2,)),
            pltpu.SemaphoreType.REGULAR,
        ],
        compiler_params=pltpu.CompilerParams(
            collective_id=0, has_side_effects=True, vmem_limit_bytes=16 * 2**20
        ),
        cost_estimate=pl.CostEstimate(flops=2 * 10**9, bytes_accessed=2 * 10**6, transcendentals=0),
        name="exchange",
    )(in_hbm(flat), in_hbm(w1), in_hbm(w2))


def decode(deep, stats, gain, shift, bias1, bias2, w1, w2, cols, entries):
    tall_rows, channels = deep.shape
    tall = tall_rows // cols
    slab_rows = tall - 4
    vspec = pl.BlockSpec(memory_space=pltpu.VMEM)
    return pl.pallas_call(
        functools.partial(decode_kernel, entries, cols),
        out_shape=jax.ShapeDtypeStruct((2 * slab_rows, 2 * cols, channels), BF16),
        in_specs=[vspec] * 8,
        out_specs=pl.BlockSpec(memory_space=pl.ANY),
        scratch_shapes=[
            pltpu.VMEM((tall_rows, 3 * channels), BF16),
            pltpu.VMEM(((tall - 2) * cols, channels), BF16),
            pltpu.VMEM(((tall - 2) * cols, channels), BF16),
            pltpu.VMEM((24, channels), F32),
            pltpu.VMEM((2 * cols, channels), F32),
            pltpu.VMEM((8, channels), F32),
            pltpu.VMEM((2, channels // 128, 2 * cols, 128), F32),
            pltpu.VMEM((2 * slab_rows, 2 * cols, channels), BF16),
            pltpu.SemaphoreType.DMA((2,)),
        ],
        compiler_params=pltpu.CompilerParams(vmem_limit_bytes=40 * 2**20),
        cost_estimate=pl.CostEstimate(flops=6 * 10**9, bytes_accessed=14 * 10**6, transcendentals=0),
        name="decode",
    )(deep, stats, gain, shift, bias1, bias2, w1, w2)


def per_device(latents, norm_gain, norm_shift, w_first, bias_first, w_second, bias_second):
    slab_rows, cols, channels = latents.shape
    ny = lax.axis_size("view_0")
    members = lax.axis_size("view_1") * lax.axis_size("view_2")
    entries = float(slab_rows * cols * (channels // GROUPS) * ny * members)
    w1 = jnp.transpose(w_first, (1, 2, 0, 3)).reshape(9, channels, channels)
    w2 = jnp.transpose(w_second, (1, 2, 0, 3)).reshape(9, channels, channels)
    flat = latents.reshape(slab_rows * cols, channels)
    deep, stats, w1, w2 = exchange(flat, w1, w2, cols, ny, members)
    row = lambda v: v.reshape(1, channels)
    return decode(
        deep, stats, row(norm_gain), row(norm_shift), row(bias_first), row(bias_second), w1, w2, cols, entries
    )


def solution(mesh):
    torus = Mesh(mesh.devices.reshape(mesh.shape["scene"], 8, 8, 2), SCENE_VIEW)
    in_specs = (P(SCENE_VIEW, None, None), P(), P(), P(), P(), P(), P())
    out_specs = P(SCENE_VIEW, None, None)
    return jax.shard_map(per_device, mesh=torus, in_specs=in_specs, out_specs=out_specs, check_vma=False)
```

```python
import functools

import jax
import jax.numpy as jnp
from jax import lax
from jax.experimental import pallas as pl
from jax.experimental.pallas import tpu as pltpu
from jax.sharding import Mesh
from jax.sharding import PartitionSpec as P

GROUPS = 32
H_LAT = 32
AXES = ("view_0", "view_1", "view_2")
SCENE_VIEW = ("scene",) + AXES
EPSILON = 1e-06
F32 = jnp.float32
BF16 = jnp.bfloat16
MESH_ID = pl.DeviceIdType.MESH


MIX_CHUNKS = ((0, 5), (5, 10))
UP_CHUNKS = ((0, 5), (5, 9))


def dot(a, w):
    return lax.dot_general(a, w, (((1,), (1,)), ((), ())), preferred_element_type=F32)


def exchange_kernel(
    cols, latents, w1, w2, deep, stats, w1v, w2v,
    gather, raw, rest, total,
    in_sem, w_sem, gsend, grecv, rawsend, rawrecv, rowsend, colsend, trecv, hsend, hrecv, ready,
):
    y = lax.axis_index("view_0")
    x = lax.axis_index("view_1")
    c = lax.axis_index("view_2")
    ny = lax.axis_size("view_0")
    nx = lax.axis_size("view_1")
    nc = lax.axis_size("view_2")
    rows = latents.shape[0]
    columns = latents.shape[1]
    halo = (deep.shape[0] - rows) // 2
    step = ny * (rows // cols) // H_LAT
    slot = x * nc + c
    members = nx * nc
    everyone = ny * members
    hub = 1
    me = y * members + slot
    is_hub = me == hub
    not_hub = jnp.logical_not(is_hub)
    is_root = me == 0
    fed_by_root = (y == 0) & (c == 0) & (x != 0)
    fed_by_hub = (y == 0) & (c != 0) & (x != 0)
    has_previous = y >= step
    has_next = y < ny - step

    load = pltpu.make_async_copy(latents, deep.at[pl.ds(halo, rows)], in_sem)
    load.start()
    weights = [pltpu.make_async_copy(w1, w1v, w_sem.at[0]), pltpu.make_async_copy(w2, w2v, w_sem.at[1])]

    def member(row, p):
        return {"view_0": row, "view_1": p // nc, "view_2": lax.rem(p, nc)}

    barrier = pltpu.get_barrier_semaphore()

    def greet(device):
        pl.semaphore_signal(barrier, inc=1, device_id=device, device_id_type=MESH_ID)

    @pl.when(is_hub)
    def _():
        def body(p, carry):
            q = lax.rem(hub + p, everyone)
            greet(member(q // members, lax.rem(q, members)))
            return carry

        lax.fori_loop(1, everyone, body, 0)

    @pl.when(has_previous)
    def _():
        greet(member(lax.rem(y + ny - step, ny), slot))

    @pl.when(fed_by_root)
    def _():
        greet(member(0, 0))

    load.wait()
    for copy in weights:
        copy.start()

    sums = jnp.zeros((8, columns), F32)
    squares = jnp.zeros((8, columns), F32)
    for i in range(0, rows, 64):
        v = deep[pl.ds(halo + i, 64), :].astype(F32)
        q = v * v
        for j in range(0, 64, 8):
            sums = sums + v[j : j + 8]
            squares = squares + q[j : j + 8]
    sub = lax.broadcasted_iota(jnp.int32, (8, columns), 0)
    both = jnp.where(
        sub == 0, jnp.sum(sums, axis=0, keepdims=True), jnp.sum(squares, axis=0, keepdims=True)
    )
    lane = lax.broadcasted_iota(jnp.int32, (8, 128), 1)
    sub1 = lax.broadcasted_iota(jnp.int32, (8, 128), 0)
    packed = jnp.zeros((8, 128), F32)
    for t in range(columns // 128):
        tile = both[:, t * 128 : (t + 1) * 128]
        for d in (8, 4, 2, 1):
            tile = tile + pltpu.roll(tile, 128 - d, 1)
        s_part = pltpu.roll(tile, t, 1) if t else tile
        q_part = pltpu.roll(tile, t + 4, 1)
        packed = jnp.where((lax.rem(lane, 16) == t) & (sub1 == 0), s_part, packed)
        packed = jnp.where((lax.rem(lane, 16) == t + 4) & (sub1 == 1), q_part, packed)
    mine = jnp.sum(packed, axis=0, keepdims=True)
    gather[pl.ds(me, 1), :] = mine

    pl.semaphore_wait(barrier, jnp.where(is_hub, 0, 1) + jnp.where(has_next, 1, 0) + jnp.where(is_root, nx - 1, 0))

    def remote(src, dst, send, recv, device):
        return pltpu.make_async_remote_copy(
            src_ref=src, dst_ref=dst, send_sem=send, recv_sem=recv, device_id=device, device_id_type=MESH_ID
        )

    def to_row(buf, p):
        return remote(buf, buf, rowsend.at[p], trecv, member(0, p))

    def raw_to(p):
        return remote(raw, raw, rawsend.at[p], rawrecv, member(0, p))

    def to_column(k):
        return remote(total, total, colsend.at[k], trecv, member(k, slot))

    line = gather.at[pl.ds(me, 1)]
    to_hub = remote(line, line, gsend, grecv, member(0, hub))
    far = sorted(range(1, nx), key=lambda k: -min(k, nx - k))
    fed = [k * nc for k in far]
    sent_total = [k * nc + 1 for k in far]
    following = member(lax.rem(y + step, ny), slot)
    to_next = remote(
        deep.at[pl.ds(rows, halo)], deep.at[pl.ds(0, halo)], hsend.at[0], hrecv.at[0], following
    )
    to_previous = remote(
        deep.at[pl.ds(halo, halo)], deep.at[pl.ds(halo + rows, halo)], hsend.at[1], hrecv.at[1],
        member(lax.rem(y + ny - step, ny), slot),
    )

    @pl.when(is_root)
    def _():
        raw[...] = mine
        raw_to(hub).start()
        for p in fed:
            raw_to(p).start()

    @pl.when(not_hub & jnp.logical_not(is_root))
    def _():
        to_hub.start()

    @pl.when(has_next)
    def _():
        pl.semaphore_signal(ready, inc=1, device_id=following, device_id_type=MESH_ID)
        to_next.start()

    @pl.when(has_previous)
    def _():
        pl.semaphore_wait(ready, 1)
        to_previous.start()

    @pl.when(not_hub & jnp.logical_not(is_root))
    def _():
        to_hub.wait_send()

    @pl.when(is_hub)
    def _():
        arrivals = gather.at[pl.ds(hub + 1, everyone - hub - 1)]
        pltpu.make_async_copy(arrivals, arrivals, grecv).wait()
        row = lax.broadcasted_iota(jnp.int32, gather.shape, 0)
        rest[...] = jnp.sum(jnp.where(row == 0, 0.0, gather[...]), axis=0, keepdims=True)
        for p in fed:
            to_row(rest, p).start()
        raw_to(hub).wait_recv()
        total[...] = rest[...] + raw[...]
        for p in sent_total:
            to_row(total, p).start()
        to_row(rest, 0).start()

    @pl.when(is_root | fed_by_root)
    def _():
        to_row(rest, 0).wait_recv()

        @pl.when(fed_by_root)
        def _():
            raw_to(hub).wait_recv()

        total[...] = rest[...] + raw[...]

    @pl.when(fed_by_hub | (y != 0))
    def _():
        to_row(total, 0).wait_recv()

    @pl.when(y == 0)
    def _():
        for k in range(1, ny):
            to_column(k).start()

    stats[...] = jnp.broadcast_to(total[...], stats.shape)

    for copy in weights:
        copy.wait()

    @pl.when(has_next)
    def _():
        to_next.wait_send()
        to_previous.wait_recv()

    @pl.when(has_previous)
    def _():
        to_previous.wait_send()
        to_next.wait_recv()

    @pl.when(is_hub)
    def _():
        for p in fed:
            to_row(rest, p).wait_send()
        for p in sent_total:
            to_row(total, p).wait_send()
        to_row(rest, 0).wait_send()

    @pl.when(is_root)
    def _():
        for p in [hub] + fed:
            raw_to(p).wait_send()

    @pl.when(y == 0)
    def _():
        for k in range(1, ny):
            to_column(k).wait_send()


def shifted_down(v, first):
    row = lax.broadcasted_iota(jnp.int32, v.shape, 0)
    return jnp.where(row == 0, first, pltpu.roll(v, 1, 0))


def shifted_up(v, last):
    n = v.shape[0]
    row = lax.broadcasted_iota(jnp.int32, v.shape, 0)
    return jnp.where(row == n - 1, last, pltpu.roll(v, n - 1, 0))


def decode_kernel(
    entries, cols, deep, stats, gain, shift, bias1, bias2, w1, w2, out,
    acat, m0, md, edge, keep_s, keep_x, z, obuf, out_sem,
):
    channels = deep.shape[1]
    tall = deep.shape[0] // cols
    y_dev = lax.axis_index("view_0")
    ny = lax.axis_size("view_0")
    slab_rows = tall - 4
    step = ny * slab_rows // H_LAT
    has_previous = y_dev >= step
    has_next = y_dev < ny - step

    st = stats[...]
    lane = lax.broadcasted_iota(jnp.int32, st.shape, 1)
    base = lane - lax.rem(lane, 16)
    means, rstds = [], []
    for t in range(channels // 128):
        s = jnp.take_along_axis(st, base + t, axis=1)
        q = jnp.take_along_axis(st, base + (t + 4), axis=1)
        mean = s / entries
        var = q / entries - mean * mean
        means.append(mean)
        rstds.append(lax.rsqrt(var + EPSILON))
    mean = jnp.concatenate(means, axis=1)[0:1]
    rstd = jnp.concatenate(rstds, axis=1)[0:1]
    scale = rstd * gain[...]
    offset = shift[...] - mean * scale
    half_scale = 0.5 * scale
    half_offset = 0.5 * offset

    def activate(i):
        h = deep[i * cols : (i + 1) * cols, :].astype(F32) * half_scale + half_offset
        a = h * jnp.tanh(h) + h
        if i < 2:
            a = jnp.where(has_previous, a, 0.0)
        if i >= tall - 2:
            a = jnp.where(has_next, a, 0.0)
        rows = slice(i * cols, (i + 1) * cols)
        acat[rows, 0:channels] = shifted_down(a, 0.0).astype(BF16)
        acat[rows, channels : 2 * channels] = a.astype(BF16)
        acat[rows, 2 * channels :] = shifted_up(a, 0.0).astype(BF16)

    mid = tall - 2

    def mix(lo, hi):
        acc = None
        for r in range(3):
            for s in range(3):
                lhs = acat[(lo + r) * cols : (hi + r) * cols, s * channels : (s + 1) * channels]
                term = dot(lhs, w1[3 * r + s])
                acc = term if acc is None else acc + term
        for p in range(lo, hi):
            i = p - lo
            v = acc[i * cols : (i + 1) * cols] + deep[(p + 1) * cols : (p + 2) * cols, :].astype(F32) + bias1[...]
            if p == 0:
                v = jnp.where(has_previous, v, 0.0)
            if p == mid - 1:
                v = jnp.where(has_next, v, 0.0)
            rows = slice(p * cols, (p + 1) * cols)
            m0[rows, :] = v.astype(BF16)
            md[rows, :] = shifted_down(v, 0.0).astype(BF16)
            edge[p : p + 1, :] = v[cols - 1 : cols]

    def edge_rows(first, count):
        pad = jnp.zeros((16 - count, channels), F32)
        return jnp.concatenate([edge[first : first + count, :], pad], axis=0).astype(BF16)

    zero16 = jnp.zeros((16, channels), BF16)
    corners = slab_rows + 1

    def block(buf, first, count):
        return buf[first * cols : (first + count) * cols, :]

    def with_edge(buf, first, count, e):
        return jnp.concatenate([block(buf, first, count), e], axis=0)

    def send_rows(y_lo, y_hi, sem):
        copy = pltpu.make_async_copy(
            obuf.at[pl.ds(y_lo, y_hi - y_lo)], out.at[pl.ds(y_lo, y_hi - y_lo)], out_sem.at[sem]
        )
        copy.start()
        return copy

    def upsample(lo, hi):
        n = hi - lo
        nb = min(hi, slab_rows) - lo
        bb = dot(block(m0, lo + 1, nb), w2[4])
        bs = dot(with_edge(md, lo + 1, nb, edge_rows(lo + 1, nb)), w2[3])
        bs = bs + dot(with_edge(m0, lo + 1, nb, zero16), w2[5])
        sb = dot(block(m0, lo, n), w2[1]) + dot(block(m0, lo + 1, n), w2[7])
        ss = dot(with_edge(md, lo, n, edge_rows(lo, n)), w2[0])
        ss = ss + dot(with_edge(m0, lo, n, zero16), w2[2])
        ss = ss + dot(with_edge(md, lo + 1, n, edge_rows(lo + 1, n)), w2[6])
        ss = ss + dot(with_edge(m0, lo + 1, n, zero16), w2[8])

        return n, nb, bb, bs, sb, ss

    def combine(lo, hi, n_out, n, nb, bb, bs, sb, ss):
        sent = []
        for i in range(lo, hi):
            k = i - lo
            s_main = ss[k * cols : (k + 1) * cols]
            s_edge = ss[n * cols + k : n * cols + k + 1]
            c_main = sb[k * cols : (k + 1) * cols] + bias2[...]
            for yy in (2 * i - 1, 2 * i):
                if not 0 <= yy < 2 * slab_rows:
                    continue
                b = yy // 2
                if b < lo:
                    u = s_main + keep_s[0:cols, :]
                    u_edge = s_edge + keep_x[0:1, :]
                    w = c_main + keep_s[cols : 2 * cols, :]
                else:
                    kb = b - lo
                    u = s_main + bs[kb * cols : (kb + 1) * cols]
                    u_edge = s_edge + bs[nb * cols + kb : nb * cols + kb + 1]
                    w = c_main + bb[kb * cols : (kb + 1) * cols]
                zi = yy % 4
                even = u + w
                odd = shifted_up(u, u_edge) + w
                for t in range(channels // 128):
                    lanes = slice(t * 128, (t + 1) * 128)
                    z[zi, t, pl.ds(0, cols, stride=2), :] = even[:, lanes]
                    z[zi, t, pl.ds(1, cols, stride=2), :] = odd[:, lanes]
                    obuf[yy, :, lanes] = z[zi, t].astype(BF16)
            if hi == corners:
                sent.append(send_rows(max(2 * i - 1, 0), min(2 * i + 1, 2 * slab_rows), n_out + k))
        if hi < corners:
            kb = nb - 1
            keep_s[0:cols, :] = bs[kb * cols : (kb + 1) * cols]
            keep_s[cols : 2 * cols, :] = bb[kb * cols : (kb + 1) * cols]
            keep_x[0:1, :] = bs[nb * cols + kb : nb * cols + kb + 1]
        return sent

    done = 0
    mix_chunks = MIX_CHUNKS
    for lo, hi in mix_chunks:
        for i in range(done, hi + 2):
            activate(i)
        done = hi + 2
        mix(lo, hi)
    copies = []
    (a_lo, a_hi), (b_lo, b_hi) = UP_CHUNKS
    first = upsample(a_lo, a_hi)
    second = upsample(b_lo, b_hi)
    combine(a_lo, a_hi, 0, *first)
    copies.append([send_rows(max(2 * a_lo - 1, 0), 2 * a_hi - 1, 0)])
    copies.append(combine(b_lo, b_hi, 1, *second))
    for group in copies:
        for copy in group:
            copy.wait()


def in_hbm(array):
    return pltpu.with_memory_space_constraint(array, pltpu.HBM)


def exchange(flat, w1, w2, cols, ny, members):
    rows, channels = flat.shape
    hbm = pl.BlockSpec(memory_space=pltpu.HBM)
    vmem = pl.BlockSpec(memory_space=pltpu.VMEM)
    dma = pltpu.SemaphoreType.DMA
    return pl.pallas_call(
        functools.partial(exchange_kernel, cols),
        out_shape=(
            pltpu.VMEM((rows + 4 * cols, channels), BF16),
            pltpu.VMEM((8, 128), F32),
            pltpu.VMEM(w1.shape, BF16),
            pltpu.VMEM(w2.shape, BF16),
        ),
        in_specs=[hbm] * 3,
        out_specs=(vmem,) * 4,
        scratch_shapes=[
            pltpu.VMEM((ny * members, 128), F32),
            pltpu.VMEM((1, 128), F32),
            pltpu.VMEM((1, 128), F32),
            pltpu.VMEM((1, 128), F32),
            dma,
            dma((2,)),
            dma,
            dma,
            dma((members,)),
            dma,
            dma((members,)),
            dma((ny,)),
            dma,
            dma((2,)),
            dma((2,)),
            pltpu.SemaphoreType.REGULAR,
        ],
        compiler_params=pltpu.CompilerParams(
            collective_id=0, has_side_effects=True, vmem_limit_bytes=16 * 2**20
        ),
        cost_estimate=pl.CostEstimate(flops=2 * 10**9, bytes_accessed=2 * 10**6, transcendentals=0),
        name="exchange",
    )(in_hbm(flat), in_hbm(w1), in_hbm(w2))


def decode(deep, stats, gain, shift, bias1, bias2, w1, w2, cols, entries):
    tall_rows, channels = deep.shape
    tall = tall_rows // cols
    slab_rows = tall - 4
    vspec = pl.BlockSpec(memory_space=pltpu.VMEM)
    return pl.pallas_call(
        functools.partial(decode_kernel, entries, cols),
        out_shape=jax.ShapeDtypeStruct((2 * slab_rows, 2 * cols, channels), BF16),
        in_specs=[vspec] * 8,
        out_specs=pl.BlockSpec(memory_space=pl.ANY),
        scratch_shapes=[
            pltpu.VMEM((tall_rows, 3 * channels), BF16),
            pltpu.VMEM(((tall - 2) * cols, channels), BF16),
            pltpu.VMEM(((tall - 2) * cols, channels), BF16),
            pltpu.VMEM((24, channels), F32),
            pltpu.VMEM((2 * cols, channels), F32),
            pltpu.VMEM((8, channels), F32),
            pltpu.VMEM((4, channels // 128, 2 * cols, 128), F32),
            pltpu.VMEM((2 * slab_rows, 2 * cols, channels), BF16),
            pltpu.SemaphoreType.DMA((16,)),
        ],
        compiler_params=pltpu.CompilerParams(vmem_limit_bytes=40 * 2**20),
        cost_estimate=pl.CostEstimate(flops=6 * 10**9, bytes_accessed=14 * 10**6, transcendentals=0),
        name="decode",
    )(deep, stats, gain, shift, bias1, bias2, w1, w2)


def per_device(latents, norm_gain, norm_shift, w_first, bias_first, w_second, bias_second):
    slab_rows, cols, channels = latents.shape
    ny = lax.axis_size("view_0")
    members = lax.axis_size("view_1") * lax.axis_size("view_2")
    entries = float(slab_rows * cols * (channels // GROUPS) * ny * members)
    w1 = jnp.transpose(w_first, (1, 2, 0, 3)).reshape(9, channels, channels)
    w2 = jnp.transpose(w_second, (1, 2, 0, 3)).reshape(9, channels, channels)
    flat = latents.reshape(slab_rows * cols, channels)
    deep, stats, w1, w2 = exchange(flat, w1, w2, cols, ny, members)
    row = lambda v: v.reshape(1, channels)
    return decode(
        deep, stats, row(norm_gain), row(norm_shift), row(bias_first), row(bias_second), w1, w2, cols, entries
    )


def solution(mesh):
    torus = Mesh(mesh.devices.reshape(mesh.shape["scene"], 8, 8, 2), SCENE_VIEW)
    in_specs = (P(SCENE_VIEW, None, None), P(), P(), P(), P(), P(), P())
    out_specs = P(SCENE_VIEW, None, None)
    return jax.shard_map(per_device, mesh=torus, in_specs=in_specs, out_specs=out_specs, check_vma=False)
```

```python
import functools

import jax
import jax.numpy as jnp
from jax import lax
from jax.experimental import pallas as pl
from jax.experimental.pallas import tpu as pltpu
from jax.sharding import Mesh
from jax.sharding import PartitionSpec as P

GROUPS = 32
H_LAT = 32
AXES = ("view_0", "view_1", "view_2")
SCENE_VIEW = ("scene",) + AXES
EPSILON = 1e-06
F32 = jnp.float32
BF16 = jnp.bfloat16
MESH_ID = pl.DeviceIdType.MESH


MIX_CHUNKS = ((0, 5), (5, 10))
UP_CHUNKS = ((0, 5), (5, 9))


def dot(a, w):
    return lax.dot_general(a, w, (((1,), (1,)), ((), ())), preferred_element_type=F32)


def exchange_kernel(
    entries, cols, latents, w1, w2, gain, shift, deep, acat, w1v, w2v,
    gain_v, shift_v, gather, raw, rest, total,
    in_sem, w_sem, gsend, grecv, rawsend, rawrecv, rowsend, colsend, trecv, hsend, hrecv, ready,
):
    y = lax.axis_index("view_0")
    x = lax.axis_index("view_1")
    c = lax.axis_index("view_2")
    ny = lax.axis_size("view_0")
    nx = lax.axis_size("view_1")
    nc = lax.axis_size("view_2")
    rows = latents.shape[0]
    columns = latents.shape[1]
    halo = (deep.shape[0] - rows) // 2
    step = ny * (rows // cols) // H_LAT
    slot = x * nc + c
    members = nx * nc
    everyone = ny * members
    hub = 1
    me = y * members + slot
    is_hub = me == hub
    not_hub = jnp.logical_not(is_hub)
    is_root = me == 0
    fed_by_root = (y == 0) & (c == 0) & (x != 0)
    fed_by_hub = (y == 0) & (c != 0) & (x != 0)
    has_previous = y >= step
    has_next = y < ny - step

    load = pltpu.make_async_copy(latents, deep.at[pl.ds(halo, rows)], in_sem)
    load.start()
    affine = [
        pltpu.make_async_copy(gain, gain_v, w_sem.at[2]),
        pltpu.make_async_copy(shift, shift_v, w_sem.at[3]),
    ]
    weights = [pltpu.make_async_copy(w1, w1v, w_sem.at[0]), pltpu.make_async_copy(w2, w2v, w_sem.at[1])]

    def member(row, p):
        return {"view_0": row, "view_1": p // nc, "view_2": lax.rem(p, nc)}

    barrier = pltpu.get_barrier_semaphore()

    def greet(device):
        pl.semaphore_signal(barrier, inc=1, device_id=device, device_id_type=MESH_ID)

    @pl.when(is_hub)
    def _():
        def body(p, carry):
            q = lax.rem(hub + p, everyone)
            greet(member(q // members, lax.rem(q, members)))
            return carry

        lax.fori_loop(1, everyone, body, 0)

    @pl.when(has_previous)
    def _():
        greet(member(lax.rem(y + ny - step, ny), slot))

    @pl.when(fed_by_root)
    def _():
        greet(member(0, 0))

    load.wait()
    for copy in affine + weights:
        copy.start()

    sums = jnp.zeros((8, columns), F32)
    squares = jnp.zeros((8, columns), F32)
    for i in range(0, rows, 64):
        v = deep[pl.ds(halo + i, 64), :].astype(F32)
        q = v * v
        for j in range(0, 64, 8):
            sums = sums + v[j : j + 8]
            squares = squares + q[j : j + 8]
    sub = lax.broadcasted_iota(jnp.int32, (8, columns), 0)
    both = jnp.where(
        sub == 0, jnp.sum(sums, axis=0, keepdims=True), jnp.sum(squares, axis=0, keepdims=True)
    )
    lane = lax.broadcasted_iota(jnp.int32, (8, 128), 1)
    sub1 = lax.broadcasted_iota(jnp.int32, (8, 128), 0)
    packed = jnp.zeros((8, 128), F32)
    for t in range(columns // 128):
        tile = both[:, t * 128 : (t + 1) * 128]
        for d in (8, 4, 2, 1):
            tile = tile + pltpu.roll(tile, 128 - d, 1)
        s_part = pltpu.roll(tile, t, 1) if t else tile
        q_part = pltpu.roll(tile, t + 4, 1)
        packed = jnp.where((lax.rem(lane, 16) == t) & (sub1 == 0), s_part, packed)
        packed = jnp.where((lax.rem(lane, 16) == t + 4) & (sub1 == 1), q_part, packed)
    mine = jnp.sum(packed, axis=0, keepdims=True)
    gather[pl.ds(me, 1), :] = mine

    pl.semaphore_wait(barrier, jnp.where(is_hub, 0, 1) + jnp.where(has_next, 1, 0) + jnp.where(is_root, nx - 1, 0))

    def remote(src, dst, send, recv, device):
        return pltpu.make_async_remote_copy(
            src_ref=src, dst_ref=dst, send_sem=send, recv_sem=recv, device_id=device, device_id_type=MESH_ID
        )

    def to_row(buf, p):
        return remote(buf, buf, rowsend.at[p], trecv, member(0, p))

    def raw_to(p):
        return remote(raw, raw, rawsend.at[p], rawrecv, member(0, p))

    def to_column(k):
        return remote(total, total, colsend.at[k], trecv, member(k, slot))

    line = gather.at[pl.ds(me, 1)]
    to_hub = remote(line, line, gsend, grecv, member(0, hub))
    far = sorted(range(1, nx), key=lambda k: -min(k, nx - k))
    fed = [k * nc for k in far]
    sent_total = [k * nc + 1 for k in far]
    following = member(lax.rem(y + step, ny), slot)
    to_next = remote(
        deep.at[pl.ds(rows, halo)], deep.at[pl.ds(0, halo)], hsend.at[0], hrecv.at[0], following
    )
    to_previous = remote(
        deep.at[pl.ds(halo, halo)], deep.at[pl.ds(halo + rows, halo)], hsend.at[1], hrecv.at[1],
        member(lax.rem(y + ny - step, ny), slot),
    )

    @pl.when(is_root)
    def _():
        raw[...] = mine
        raw_to(hub).start()
        for p in fed:
            raw_to(p).start()

    @pl.when(not_hub & jnp.logical_not(is_root))
    def _():
        to_hub.start()

    @pl.when(has_next)
    def _():
        pl.semaphore_signal(ready, inc=1, device_id=following, device_id_type=MESH_ID)
        to_next.start()

    @pl.when(has_previous)
    def _():
        pl.semaphore_wait(ready, 1)
        to_previous.start()

    @pl.when(not_hub & jnp.logical_not(is_root))
    def _():
        to_hub.wait_send()

    @pl.when(is_hub)
    def _():
        arrivals = gather.at[pl.ds(hub + 1, everyone - hub - 1)]
        pltpu.make_async_copy(arrivals, arrivals, grecv).wait()
        row = lax.broadcasted_iota(jnp.int32, gather.shape, 0)
        rest[...] = jnp.sum(jnp.where(row == 0, 0.0, gather[...]), axis=0, keepdims=True)
        for p in fed:
            to_row(rest, p).start()
        raw_to(hub).wait_recv()
        total[...] = rest[...] + raw[...]
        for p in sent_total:
            to_row(total, p).start()
        to_row(rest, 0).start()

    @pl.when(is_root | fed_by_root)
    def _():
        to_row(rest, 0).wait_recv()

        @pl.when(fed_by_root)
        def _():
            raw_to(hub).wait_recv()

        total[...] = rest[...] + raw[...]

    @pl.when(fed_by_hub | (y != 0))
    def _():
        to_row(total, 0).wait_recv()

    @pl.when(y == 0)
    def _():
        for k in range(1, ny):
            to_column(k).start()

    @pl.when(has_next)
    def _():
        to_previous.wait_recv()

    @pl.when(has_previous)
    def _():
        to_next.wait_recv()

    for copy in affine:
        copy.wait()
    st = jnp.broadcast_to(total[...], (8, 128))
    base = lane - lax.rem(lane, 16)
    means, rstds = [], []
    for t in range(columns // 128):
        s = jnp.take_along_axis(st, base + t, axis=1)
        q = jnp.take_along_axis(st, base + (t + 4), axis=1)
        mean = s / entries
        var = q / entries - mean * mean
        means.append(mean)
        rstds.append(lax.rsqrt(var + EPSILON))
    mean = jnp.concatenate(means, axis=1)[0:1]
    rstd = jnp.concatenate(rstds, axis=1)[0:1]
    scale = rstd * gain_v[...]
    offset = shift_v[...] - mean * scale
    half_scale = 0.5 * scale
    half_offset = 0.5 * offset

    tall = deep.shape[0] // cols

    def activate(i):
        h = deep[i * cols : (i + 1) * cols, :].astype(F32) * half_scale + half_offset
        a = h * jnp.tanh(h) + h
        if i < 2:
            a = jnp.where(has_previous, a, 0.0)
        if i >= tall - 2:
            a = jnp.where(has_next, a, 0.0)
        rows = slice(i * cols, (i + 1) * cols)
        acat[rows, 0:columns] = shifted_down(a, 0.0).astype(BF16)
        acat[rows, columns : 2 * columns] = a.astype(BF16)
        acat[rows, 2 * columns :] = shifted_up(a, 0.0).astype(BF16)

    for i in range(tall):
        activate(i)

    for copy in weights:
        copy.wait()

    @pl.when(has_next)
    def _():
        to_next.wait_send()

    @pl.when(has_previous)
    def _():
        to_previous.wait_send()

    @pl.when(is_hub)
    def _():
        for p in fed:
            to_row(rest, p).wait_send()
        for p in sent_total:
            to_row(total, p).wait_send()
        to_row(rest, 0).wait_send()

    @pl.when(is_root)
    def _():
        for p in [hub] + fed:
            raw_to(p).wait_send()

    @pl.when(y == 0)
    def _():
        for k in range(1, ny):
            to_column(k).wait_send()


def shifted_down(v, first):
    row = lax.broadcasted_iota(jnp.int32, v.shape, 0)
    return jnp.where(row == 0, first, pltpu.roll(v, 1, 0))


def shifted_up(v, last):
    n = v.shape[0]
    row = lax.broadcasted_iota(jnp.int32, v.shape, 0)
    return jnp.where(row == n - 1, last, pltpu.roll(v, n - 1, 0))


def decode_kernel(
    cols, deep, acat, bias1, bias2, w1, w2, out,
    m0, md, edge, keep_s, keep_x, z, obuf, out_sem,
):
    channels = deep.shape[1]
    tall = deep.shape[0] // cols
    y_dev = lax.axis_index("view_0")
    ny = lax.axis_size("view_0")
    slab_rows = tall - 4
    step = ny * slab_rows // H_LAT
    has_previous = y_dev >= step
    has_next = y_dev < ny - step

    mid = tall - 2

    def mix(lo, hi):
        acc = None
        for r in range(3):
            for s in range(3):
                lhs = acat[(lo + r) * cols : (hi + r) * cols, s * channels : (s + 1) * channels]
                term = dot(lhs, w1[3 * r + s])
                acc = term if acc is None else acc + term
        for p in range(lo, hi):
            i = p - lo
            v = acc[i * cols : (i + 1) * cols] + deep[(p + 1) * cols : (p + 2) * cols, :].astype(F32) + bias1[...]
            if p == 0:
                v = jnp.where(has_previous, v, 0.0)
            if p == mid - 1:
                v = jnp.where(has_next, v, 0.0)
            rows = slice(p * cols, (p + 1) * cols)
            m0[rows, :] = v.astype(BF16)
            md[rows, :] = shifted_down(v, 0.0).astype(BF16)
            edge[p : p + 1, :] = v[cols - 1 : cols]

    def edge_rows(first, count):
        pad = jnp.zeros((16 - count, channels), F32)
        return jnp.concatenate([edge[first : first + count, :], pad], axis=0).astype(BF16)

    zero16 = jnp.zeros((16, channels), BF16)
    corners = slab_rows + 1

    def block(buf, first, count):
        return buf[first * cols : (first + count) * cols, :]

    def with_edge(buf, first, count, e):
        return jnp.concatenate([block(buf, first, count), e], axis=0)

    def send_rows(y_lo, y_hi, sem):
        copy = pltpu.make_async_copy(
            obuf.at[pl.ds(y_lo, y_hi - y_lo)], out.at[pl.ds(y_lo, y_hi - y_lo)], out_sem.at[sem]
        )
        copy.start()
        return copy

    def upsample(lo, hi):
        n = hi - lo
        nb = min(hi, slab_rows) - lo
        bb = dot(block(m0, lo + 1, nb), w2[4])
        bs = dot(with_edge(md, lo + 1, nb, edge_rows(lo + 1, nb)), w2[3])
        bs = bs + dot(with_edge(m0, lo + 1, nb, zero16), w2[5])
        sb = dot(block(m0, lo, n), w2[1]) + dot(block(m0, lo + 1, n), w2[7])
        ss = dot(with_edge(md, lo, n, edge_rows(lo, n)), w2[0])
        ss = ss + dot(with_edge(m0, lo, n, zero16), w2[2])
        ss = ss + dot(with_edge(md, lo + 1, n, edge_rows(lo + 1, n)), w2[6])
        ss = ss + dot(with_edge(m0, lo + 1, n, zero16), w2[8])

        return n, nb, bb, bs, sb, ss

    def combine(lo, hi, n_out, n, nb, bb, bs, sb, ss):
        sent = []
        for i in range(lo, hi):
            k = i - lo
            s_main = ss[k * cols : (k + 1) * cols]
            s_edge = ss[n * cols + k : n * cols + k + 1]
            c_main = sb[k * cols : (k + 1) * cols] + bias2[...]
            for yy in (2 * i - 1, 2 * i):
                if not 0 <= yy < 2 * slab_rows:
                    continue
                b = yy // 2
                if b < lo:
                    u = s_main + keep_s[0:cols, :]
                    u_edge = s_edge + keep_x[0:1, :]
                    w = c_main + keep_s[cols : 2 * cols, :]
                else:
                    kb = b - lo
                    u = s_main + bs[kb * cols : (kb + 1) * cols]
                    u_edge = s_edge + bs[nb * cols + kb : nb * cols + kb + 1]
                    w = c_main + bb[kb * cols : (kb + 1) * cols]
                zi = yy % 4
                even = u + w
                odd = shifted_up(u, u_edge) + w
                for t in range(channels // 128):
                    lanes = slice(t * 128, (t + 1) * 128)
                    z[zi, t, pl.ds(0, cols, stride=2), :] = even[:, lanes]
                    z[zi, t, pl.ds(1, cols, stride=2), :] = odd[:, lanes]
                    obuf[yy, :, lanes] = z[zi, t].astype(BF16)
            if hi == corners:
                sent.append(send_rows(max(2 * i - 1, 0), min(2 * i + 1, 2 * slab_rows), n_out + k))
        if hi < corners:
            kb = nb - 1
            keep_s[0:cols, :] = bs[kb * cols : (kb + 1) * cols]
            keep_s[cols : 2 * cols, :] = bb[kb * cols : (kb + 1) * cols]
            keep_x[0:1, :] = bs[nb * cols + kb : nb * cols + kb + 1]
        return sent

    mix_chunks = MIX_CHUNKS
    for lo, hi in mix_chunks:
        mix(lo, hi)
    copies = []
    (a_lo, a_hi), (b_lo, b_hi) = UP_CHUNKS
    first = upsample(a_lo, a_hi)
    second = upsample(b_lo, b_hi)
    combine(a_lo, a_hi, 0, *first)
    copies.append([send_rows(max(2 * a_lo - 1, 0), 2 * a_hi - 1, 0)])
    copies.append(combine(b_lo, b_hi, 1, *second))
    for group in copies:
        for copy in group:
            copy.wait()


def in_hbm(array):
    return pltpu.with_memory_space_constraint(array, pltpu.HBM)


def exchange(flat, w1, w2, gain, shift, cols, ny, members, entries):
    rows, channels = flat.shape
    hbm = pl.BlockSpec(memory_space=pltpu.HBM)
    vmem = pl.BlockSpec(memory_space=pltpu.VMEM)
    dma = pltpu.SemaphoreType.DMA
    return pl.pallas_call(
        functools.partial(exchange_kernel, entries, cols),
        out_shape=(
            pltpu.VMEM((rows + 4 * cols, channels), BF16),
            pltpu.VMEM((rows + 4 * cols, 3 * channels), BF16),
            pltpu.VMEM(w1.shape, BF16),
            pltpu.VMEM(w2.shape, BF16),
        ),
        in_specs=[hbm] * 5,
        out_specs=(vmem,) * 4,
        scratch_shapes=[
            pltpu.VMEM((1, channels), F32),
            pltpu.VMEM((1, channels), F32),
            pltpu.VMEM((ny * members, 128), F32),
            pltpu.VMEM((1, 128), F32),
            pltpu.VMEM((1, 128), F32),
            pltpu.VMEM((1, 128), F32),
            dma,
            dma((4,)),
            dma,
            dma,
            dma((members,)),
            dma,
            dma((members,)),
            dma((ny,)),
            dma,
            dma((2,)),
            dma((2,)),
            pltpu.SemaphoreType.REGULAR,
        ],
        compiler_params=pltpu.CompilerParams(
            collective_id=0, has_side_effects=True, vmem_limit_bytes=16 * 2**20
        ),
        cost_estimate=pl.CostEstimate(flops=2 * 10**9, bytes_accessed=2 * 10**6, transcendentals=0),
        name="exchange",
    )(in_hbm(flat), in_hbm(w1), in_hbm(w2), in_hbm(gain), in_hbm(shift))


def decode(deep, acat, bias1, bias2, w1, w2, cols):
    tall_rows, channels = deep.shape
    tall = tall_rows // cols
    slab_rows = tall - 4
    vspec = pl.BlockSpec(memory_space=pltpu.VMEM)
    return pl.pallas_call(
        functools.partial(decode_kernel, cols),
        out_shape=jax.ShapeDtypeStruct((2 * slab_rows, 2 * cols, channels), BF16),
        in_specs=[vspec] * 6,
        out_specs=pl.BlockSpec(memory_space=pl.ANY),
        scratch_shapes=[
            pltpu.VMEM(((tall - 2) * cols, channels), BF16),
            pltpu.VMEM(((tall - 2) * cols, channels), BF16),
            pltpu.VMEM((24, channels), F32),
            pltpu.VMEM((2 * cols, channels), F32),
            pltpu.VMEM((8, channels), F32),
            pltpu.VMEM((4, channels // 128, 2 * cols, 128), F32),
            pltpu.VMEM((2 * slab_rows, 2 * cols, channels), BF16),
            pltpu.SemaphoreType.DMA((16,)),
        ],
        compiler_params=pltpu.CompilerParams(vmem_limit_bytes=40 * 2**20),
        cost_estimate=pl.CostEstimate(flops=6 * 10**9, bytes_accessed=14 * 10**6, transcendentals=0),
        name="decode",
    )(deep, acat, bias1, bias2, w1, w2)


def per_device(latents, norm_gain, norm_shift, w_first, bias_first, w_second, bias_second):
    slab_rows, cols, channels = latents.shape
    ny = lax.axis_size("view_0")
    members = lax.axis_size("view_1") * lax.axis_size("view_2")
    entries = float(slab_rows * cols * (channels // GROUPS) * ny * members)
    w1 = jnp.transpose(w_first, (1, 2, 0, 3)).reshape(9, channels, channels)
    w2 = jnp.transpose(w_second, (1, 2, 0, 3)).reshape(9, channels, channels)
    flat = latents.reshape(slab_rows * cols, channels)
    row = lambda v: v.reshape(1, channels)
    deep, acat, w1, w2 = exchange(
        flat, w1, w2, row(norm_gain), row(norm_shift), cols, ny, members, entries
    )
    return decode(deep, acat, row(bias_first), row(bias_second), w1, w2, cols)


def solution(mesh):
    torus = Mesh(mesh.devices.reshape(mesh.shape["scene"], 8, 8, 2), SCENE_VIEW)
    in_specs = (P(SCENE_VIEW, None, None), P(), P(), P(), P(), P(), P())
    out_specs = P(SCENE_VIEW, None, None)
    return jax.shard_map(per_device, mesh=torus, in_specs=in_specs, out_specs=out_specs, check_vma=False)
```

```python
import functools

import jax
import jax.numpy as jnp
from jax import lax
from jax.experimental import pallas as pl
from jax.experimental.pallas import tpu as pltpu
from jax.sharding import Mesh
from jax.sharding import PartitionSpec as P

GROUPS = 32
H_LAT = 32
AXES = ("view_0", "view_1", "view_2")
SCENE_VIEW = ("scene",) + AXES
EPSILON = 1e-06
F32 = jnp.float32
BF16 = jnp.bfloat16
MESH_ID = pl.DeviceIdType.MESH


MIX_CHUNKS = ((0, 5), (5, 10))
UP_CHUNKS = ((0, 5), (5, 9))


def dot(a, w):
    return lax.dot_general(a, w, (((1,), (1,)), ((), ())), preferred_element_type=F32)


def exchange_kernel(
    entries, cols, latents, w1_hbm, w2, gain, shift, bias1_hbm, m0, md, edge, w2v,
    deep, acat, w1, gain_v, shift_v, bias1, gather, raw, rest, total,
    in_sem, w_sem, gsend, grecv, rawsend, rawrecv, rowsend, colsend, trecv, hsend, hrecv, ready,
):
    y = lax.axis_index("view_0")
    x = lax.axis_index("view_1")
    c = lax.axis_index("view_2")
    ny = lax.axis_size("view_0")
    nx = lax.axis_size("view_1")
    nc = lax.axis_size("view_2")
    rows = latents.shape[0]
    columns = latents.shape[1]
    halo = (deep.shape[0] - rows) // 2
    step = ny * (rows // cols) // H_LAT
    slot = x * nc + c
    members = nx * nc
    everyone = ny * members
    hub = 1
    me = y * members + slot
    is_hub = me == hub
    not_hub = jnp.logical_not(is_hub)
    is_root = me == 0
    fed_by_root = (y == 0) & (c == 0) & (x != 0)
    fed_by_hub = (y == 0) & (c != 0) & (x != 0)
    has_previous = y >= step
    has_next = y < ny - step

    load = pltpu.make_async_copy(latents, deep.at[pl.ds(halo, rows)], in_sem)
    load.start()
    affine = [
        pltpu.make_async_copy(gain, gain_v, w_sem.at[2]),
        pltpu.make_async_copy(shift, shift_v, w_sem.at[3]),
        pltpu.make_async_copy(bias1_hbm, bias1, w_sem.at[4]),
    ]
    weights = [pltpu.make_async_copy(w1_hbm, w1, w_sem.at[0]), pltpu.make_async_copy(w2, w2v, w_sem.at[1])]

    def member(row, p):
        return {"view_0": row, "view_1": p // nc, "view_2": lax.rem(p, nc)}

    barrier = pltpu.get_barrier_semaphore()

    def greet(device):
        pl.semaphore_signal(barrier, inc=1, device_id=device, device_id_type=MESH_ID)

    @pl.when(is_hub)
    def _():
        def body(p, carry):
            q = lax.rem(hub + p, everyone)
            greet(member(q // members, lax.rem(q, members)))
            return carry

        lax.fori_loop(1, everyone, body, 0)

    @pl.when(has_previous)
    def _():
        greet(member(lax.rem(y + ny - step, ny), slot))

    @pl.when(fed_by_root)
    def _():
        greet(member(0, 0))

    load.wait()
    for copy in affine + weights:
        copy.start()

    sums = jnp.zeros((8, columns), F32)
    squares = jnp.zeros((8, columns), F32)
    for i in range(0, rows, 64):
        v = deep[pl.ds(halo + i, 64), :].astype(F32)
        q = v * v
        for j in range(0, 64, 8):
            sums = sums + v[j : j + 8]
            squares = squares + q[j : j + 8]
    sub = lax.broadcasted_iota(jnp.int32, (8, columns), 0)
    both = jnp.where(
        sub == 0, jnp.sum(sums, axis=0, keepdims=True), jnp.sum(squares, axis=0, keepdims=True)
    )
    lane = lax.broadcasted_iota(jnp.int32, (8, 128), 1)
    sub1 = lax.broadcasted_iota(jnp.int32, (8, 128), 0)
    packed = jnp.zeros((8, 128), F32)
    for t in range(columns // 128):
        tile = both[:, t * 128 : (t + 1) * 128]
        for d in (8, 4, 2, 1):
            tile = tile + pltpu.roll(tile, 128 - d, 1)
        s_part = pltpu.roll(tile, t, 1) if t else tile
        q_part = pltpu.roll(tile, t + 4, 1)
        packed = jnp.where((lax.rem(lane, 16) == t) & (sub1 == 0), s_part, packed)
        packed = jnp.where((lax.rem(lane, 16) == t + 4) & (sub1 == 1), q_part, packed)
    mine = jnp.sum(packed, axis=0, keepdims=True)
    gather[pl.ds(me, 1), :] = mine

    pl.semaphore_wait(barrier, jnp.where(is_hub, 0, 1) + jnp.where(has_next, 1, 0) + jnp.where(is_root, nx - 1, 0))

    def remote(src, dst, send, recv, device):
        return pltpu.make_async_remote_copy(
            src_ref=src, dst_ref=dst, send_sem=send, recv_sem=recv, device_id=device, device_id_type=MESH_ID
        )

    def to_row(buf, p):
        return remote(buf, buf, rowsend.at[p], trecv, member(0, p))

    def to_second(p):
        return remote(total, total, rowsend.at[members + p], trecv, member(1, p))

    def raw_to(p):
        return remote(raw, raw, rawsend.at[p], rawrecv, member(0, p))

    def to_column(k):
        return remote(total, total, colsend.at[k], trecv, member(k, slot))

    line = gather.at[pl.ds(me, 1)]
    to_hub = remote(line, line, gsend, grecv, member(0, hub))
    far = sorted(range(1, nx), key=lambda k: -min(k, nx - k))
    fed = [k * nc for k in far]
    sent_total = [k * nc + 1 for k in far]
    second = [k * nc + q for k in far + [0] for q in range(nc)]
    following = member(lax.rem(y + step, ny), slot)
    to_next = remote(
        deep.at[pl.ds(rows, halo)], deep.at[pl.ds(0, halo)], hsend.at[0], hrecv.at[0], following
    )
    to_previous = remote(
        deep.at[pl.ds(halo, halo)], deep.at[pl.ds(halo + rows, halo)], hsend.at[1], hrecv.at[1],
        member(lax.rem(y + ny - step, ny), slot),
    )

    @pl.when(is_root)
    def _():
        raw[...] = mine
        raw_to(hub).start()
        for p in fed:
            raw_to(p).start()

    @pl.when(not_hub & jnp.logical_not(is_root))
    def _():
        to_hub.start()

    @pl.when(has_next)
    def _():
        pl.semaphore_signal(ready, inc=1, device_id=following, device_id_type=MESH_ID)
        to_next.start()

    @pl.when(has_previous)
    def _():
        pl.semaphore_wait(ready, 1)
        to_previous.start()

    @pl.when(not_hub & jnp.logical_not(is_root))
    def _():
        to_hub.wait_send()

    @pl.when(is_hub)
    def _():
        arrivals = gather.at[pl.ds(hub + 1, everyone - hub - 1)]
        pltpu.make_async_copy(arrivals, arrivals, grecv).wait()
        row = lax.broadcasted_iota(jnp.int32, gather.shape, 0)
        rest[...] = jnp.sum(jnp.where(row == 0, 0.0, gather[...]), axis=0, keepdims=True)
        for p in fed:
            to_row(rest, p).start()
        raw_to(hub).wait_recv()
        total[...] = rest[...] + raw[...]
        for p in sent_total:
            to_row(total, p).start()
        to_row(rest, 0).start()
        for p in second:
            to_second(p).start()

    @pl.when(is_root | fed_by_root)
    def _():
        to_row(rest, 0).wait_recv()

        @pl.when(fed_by_root)
        def _():
            raw_to(hub).wait_recv()

        total[...] = rest[...] + raw[...]

    @pl.when(fed_by_hub | (y != 0))
    def _():
        to_row(total, 0).wait_recv()

    @pl.when(y == 0)
    def _():
        for k in range(2, ny):
            to_column(k).start()

    @pl.when(has_next)
    def _():
        to_previous.wait_recv()

    @pl.when(has_previous)
    def _():
        to_next.wait_recv()

    for copy in affine:
        copy.wait()
    st = jnp.broadcast_to(total[...], (8, 128))
    base = lane - lax.rem(lane, 16)
    means, rstds = [], []
    for t in range(columns // 128):
        s = jnp.take_along_axis(st, base + t, axis=1)
        q = jnp.take_along_axis(st, base + (t + 4), axis=1)
        mean = s / entries
        var = q / entries - mean * mean
        means.append(mean)
        rstds.append(lax.rsqrt(var + EPSILON))
    mean = jnp.concatenate(means, axis=1)[0:1]
    rstd = jnp.concatenate(rstds, axis=1)[0:1]
    scale = rstd * gain_v[...]
    offset = shift_v[...] - mean * scale
    half_scale = 0.5 * scale
    half_offset = 0.5 * offset

    tall = deep.shape[0] // cols

    def activate(i):
        h = deep[i * cols : (i + 1) * cols, :].astype(F32) * half_scale + half_offset
        a = h * jnp.tanh(h) + h
        if i < 2:
            a = jnp.where(has_previous, a, 0.0)
        if i >= tall - 2:
            a = jnp.where(has_next, a, 0.0)
        rows = slice(i * cols, (i + 1) * cols)
        acat[rows, 0:columns] = shifted_down(a, 0.0).astype(BF16)
        acat[rows, columns : 2 * columns] = a.astype(BF16)
        acat[rows, 2 * columns :] = shifted_up(a, 0.0).astype(BF16)

    mid = tall - 2

    def mix(lo, hi):
        acc = None
        for r in range(3):
            for s in range(3):
                lhs = acat[(lo + r) * cols : (hi + r) * cols, s * columns : (s + 1) * columns]
                term = dot(lhs, w1[3 * r + s])
                acc = term if acc is None else acc + term
        for p in range(lo, hi):
            i = p - lo
            v = acc[i * cols : (i + 1) * cols] + deep[(p + 1) * cols : (p + 2) * cols, :].astype(F32) + bias1[...]
            if p == 0:
                v = jnp.where(has_previous, v, 0.0)
            if p == mid - 1:
                v = jnp.where(has_next, v, 0.0)
            rows = slice(p * cols, (p + 1) * cols)
            m0[rows, :] = v.astype(BF16)
            md[rows, :] = shifted_down(v, 0.0).astype(BF16)
            edge[p : p + 1, :] = v[cols - 1 : cols]

    weights[0].wait()
    done = 0
    for lo, hi in MIX_CHUNKS:
        for i in range(done, hi + 2):
            activate(i)
        done = hi + 2
        mix(lo, hi)

    weights[1].wait()

    @pl.when(has_next)
    def _():
        to_next.wait_send()

    @pl.when(has_previous)
    def _():
        to_previous.wait_send()

    @pl.when(is_hub)
    def _():
        for p in fed:
            to_row(rest, p).wait_send()
        for p in sent_total:
            to_row(total, p).wait_send()
        to_row(rest, 0).wait_send()
        for p in second:
            to_second(p).wait_send()

    @pl.when(is_root)
    def _():
        for p in [hub] + fed:
            raw_to(p).wait_send()

    @pl.when(y == 0)
    def _():
        for k in range(2, ny):
            to_column(k).wait_send()


def shifted_down(v, first):
    row = lax.broadcasted_iota(jnp.int32, v.shape, 0)
    return jnp.where(row == 0, first, pltpu.roll(v, 1, 0))


def shifted_up(v, last):
    n = v.shape[0]
    row = lax.broadcasted_iota(jnp.int32, v.shape, 0)
    return jnp.where(row == n - 1, last, pltpu.roll(v, n - 1, 0))


def upsample_kernel(
    cols, m0, md, edge, bias2, w2, out,
    keep_s, keep_x, z, obuf, out_sem,
):
    channels = m0.shape[1]
    slab_rows = m0.shape[0] // cols - 2

    def edge_rows(first, count):
        pad = jnp.zeros((16 - count, channels), F32)
        return jnp.concatenate([edge[first : first + count, :], pad], axis=0).astype(BF16)

    zero16 = jnp.zeros((16, channels), BF16)
    corners = slab_rows + 1

    def block(buf, first, count):
        return buf[first * cols : (first + count) * cols, :]

    def with_edge(buf, first, count, e):
        return jnp.concatenate([block(buf, first, count), e], axis=0)

    def send_rows(y_lo, y_hi, sem):
        copy = pltpu.make_async_copy(
            obuf.at[pl.ds(y_lo, y_hi - y_lo)], out.at[pl.ds(y_lo, y_hi - y_lo)], out_sem.at[sem]
        )
        copy.start()
        return copy

    def upsample(lo, hi):
        n = hi - lo
        nb = min(hi, slab_rows) - lo
        bb = dot(block(m0, lo + 1, nb), w2[4])
        bs = dot(with_edge(md, lo + 1, nb, edge_rows(lo + 1, nb)), w2[3])
        bs = bs + dot(with_edge(m0, lo + 1, nb, zero16), w2[5])
        sb = dot(block(m0, lo, n), w2[1]) + dot(block(m0, lo + 1, n), w2[7])
        ss = dot(with_edge(md, lo, n, edge_rows(lo, n)), w2[0])
        ss = ss + dot(with_edge(m0, lo, n, zero16), w2[2])
        ss = ss + dot(with_edge(md, lo + 1, n, edge_rows(lo + 1, n)), w2[6])
        ss = ss + dot(with_edge(m0, lo + 1, n, zero16), w2[8])

        return n, nb, bb, bs, sb, ss

    def combine(lo, hi, n_out, n, nb, bb, bs, sb, ss):
        sent = []
        for i in range(lo, hi):
            k = i - lo
            s_main = ss[k * cols : (k + 1) * cols]
            s_edge = ss[n * cols + k : n * cols + k + 1]
            c_main = sb[k * cols : (k + 1) * cols] + bias2[...]
            for yy in (2 * i - 1, 2 * i):
                if not 0 <= yy < 2 * slab_rows:
                    continue
                b = yy // 2
                if b < lo:
                    u = s_main + keep_s[0:cols, :]
                    u_edge = s_edge + keep_x[0:1, :]
                    w = c_main + keep_s[cols : 2 * cols, :]
                else:
                    kb = b - lo
                    u = s_main + bs[kb * cols : (kb + 1) * cols]
                    u_edge = s_edge + bs[nb * cols + kb : nb * cols + kb + 1]
                    w = c_main + bb[kb * cols : (kb + 1) * cols]
                zi = yy % 4
                even = u + w
                odd = shifted_up(u, u_edge) + w
                for t in range(channels // 128):
                    lanes = slice(t * 128, (t + 1) * 128)
                    z[zi, t, pl.ds(0, cols, stride=2), :] = even[:, lanes]
                    z[zi, t, pl.ds(1, cols, stride=2), :] = odd[:, lanes]
                    obuf[yy, :, lanes] = z[zi, t].astype(BF16)
            if hi == corners:
                sent.append(send_rows(max(2 * i - 1, 0), min(2 * i + 1, 2 * slab_rows), n_out + k))
        if hi < corners:
            kb = nb - 1
            keep_s[0:cols, :] = bs[kb * cols : (kb + 1) * cols]
            keep_s[cols : 2 * cols, :] = bb[kb * cols : (kb + 1) * cols]
            keep_x[0:1, :] = bs[nb * cols + kb : nb * cols + kb + 1]
        return sent

    copies = []
    (a_lo, a_hi), (b_lo, b_hi) = UP_CHUNKS
    first = upsample(a_lo, a_hi)
    second = upsample(b_lo, b_hi)
    combine(a_lo, a_hi, 0, *first)
    copies.append([send_rows(max(2 * a_lo - 1, 0), 2 * a_hi - 1, 0)])
    copies.append(combine(b_lo, b_hi, 1, *second))
    for group in copies:
        for copy in group:
            copy.wait()


def in_hbm(array):
    return pltpu.with_memory_space_constraint(array, pltpu.HBM)


def exchange(flat, w1, w2, gain, shift, bias1, cols, ny, members, entries):
    rows, channels = flat.shape
    hbm = pl.BlockSpec(memory_space=pltpu.HBM)
    vmem = pl.BlockSpec(memory_space=pltpu.VMEM)
    dma = pltpu.SemaphoreType.DMA
    return pl.pallas_call(
        functools.partial(exchange_kernel, entries, cols),
        out_shape=(
            pltpu.VMEM((rows + 2 * cols, channels), BF16),
            pltpu.VMEM((rows + 2 * cols, channels), BF16),
            pltpu.VMEM((24, channels), F32),
            pltpu.VMEM(w2.shape, BF16),
        ),
        in_specs=[hbm] * 6,
        out_specs=(vmem,) * 4,
        scratch_shapes=[
            pltpu.VMEM((rows + 4 * cols, channels), BF16),
            pltpu.VMEM((rows + 4 * cols, 3 * channels), BF16),
            pltpu.VMEM(w1.shape, BF16),
            pltpu.VMEM((1, channels), F32),
            pltpu.VMEM((1, channels), F32),
            pltpu.VMEM((1, channels), F32),
            pltpu.VMEM((ny * members, 128), F32),
            pltpu.VMEM((1, 128), F32),
            pltpu.VMEM((1, 128), F32),
            pltpu.VMEM((1, 128), F32),
            dma,
            dma((5,)),
            dma,
            dma,
            dma((members,)),
            dma,
            dma((2 * members,)),
            dma((ny,)),
            dma,
            dma((2,)),
            dma((2,)),
            pltpu.SemaphoreType.REGULAR,
        ],
        compiler_params=pltpu.CompilerParams(
            collective_id=0, has_side_effects=True, vmem_limit_bytes=24 * 2**20
        ),
        cost_estimate=pl.CostEstimate(flops=3 * 10**9, bytes_accessed=10 * 10**6, transcendentals=0),
        name="exchange",
    )(in_hbm(flat), in_hbm(w1), in_hbm(w2), in_hbm(gain), in_hbm(shift), in_hbm(bias1))


def upsample(m0, md, edge, bias2, w2, cols):
    tall_rows, channels = m0.shape
    slab_rows = tall_rows // cols - 2
    vmem = pl.BlockSpec(memory_space=pltpu.VMEM)
    return pl.pallas_call(
        functools.partial(upsample_kernel, cols),
        out_shape=jax.ShapeDtypeStruct((2 * slab_rows, 2 * cols, channels), BF16),
        in_specs=[vmem] * 5,
        out_specs=pl.BlockSpec(memory_space=pl.ANY),
        scratch_shapes=[
            pltpu.VMEM((2 * cols, channels), F32),
            pltpu.VMEM((8, channels), F32),
            pltpu.VMEM((4, channels // 128, 2 * cols, 128), F32),
            pltpu.VMEM((2 * slab_rows, 2 * cols, channels), BF16),
            pltpu.SemaphoreType.DMA((16,)),
        ],
        compiler_params=pltpu.CompilerParams(vmem_limit_bytes=32 * 2**20),
        cost_estimate=pl.CostEstimate(flops=3 * 10**9, bytes_accessed=4 * 10**6, transcendentals=0),
        name="upsample",
    )(m0, md, edge, bias2, w2)


def per_device(latents, norm_gain, norm_shift, w_first, bias_first, w_second, bias_second):
    slab_rows, cols, channels = latents.shape
    ny = lax.axis_size("view_0")
    members = lax.axis_size("view_1") * lax.axis_size("view_2")
    entries = float(slab_rows * cols * (channels // GROUPS) * ny * members)
    w1 = jnp.transpose(w_first, (1, 2, 0, 3)).reshape(9, channels, channels)
    w2 = jnp.transpose(w_second, (1, 2, 0, 3)).reshape(9, channels, channels)
    flat = latents.reshape(slab_rows * cols, channels)
    row = lambda v: v.reshape(1, channels)
    m0, md, edge, w2 = exchange(
        flat, w1, w2, row(norm_gain), row(norm_shift), row(bias_first), cols, ny, members, entries
    )
    return upsample(m0, md, edge, row(bias_second), w2, cols)


def solution(mesh):
    torus = Mesh(mesh.devices.reshape(mesh.shape["scene"], 8, 8, 2), SCENE_VIEW)
    in_specs = (P(SCENE_VIEW, None, None), P(), P(), P(), P(), P(), P())
    out_specs = P(SCENE_VIEW, None, None)
    return jax.shard_map(per_device, mesh=torus, in_specs=in_specs, out_specs=out_specs, check_vma=False)
```

```python
import functools

import jax
import jax.numpy as jnp
from jax import lax
from jax.experimental import pallas as pl
from jax.experimental.pallas import tpu as pltpu
from jax.sharding import Mesh
from jax.sharding import PartitionSpec as P

GROUPS = 32
H_LAT = 32
AXES = ("view_0", "view_1", "view_2")
SCENE_VIEW = ("scene",) + AXES
EPSILON = 1e-06
F32 = jnp.float32
BF16 = jnp.bfloat16
MESH_ID = pl.DeviceIdType.MESH


MIX_CHUNKS = ((0, 5), (5, 10))
UP_CHUNKS = ((0, 5), (5, 9))


def dot(a, w):
    return lax.dot_general(a, w, (((1,), (0,)), ((), ())), preferred_element_type=F32)


def exchange_kernel(
    entries, cols, latents, w1_hbm, w2, gain, shift, bias1_hbm, m0, md, edge, w2v,
    deep, acat, w1_raw, w2_raw, w1, gain_v, shift_v, bias1, gather, raw, rest, total,
    in_sem, w_sem, gsend, grecv, rawsend, rawrecv, rowsend, colsend, trecv, hsend, hrecv, ready,
):
    y = lax.axis_index("view_0")
    x = lax.axis_index("view_1")
    c = lax.axis_index("view_2")
    ny = lax.axis_size("view_0")
    nx = lax.axis_size("view_1")
    nc = lax.axis_size("view_2")
    rows = latents.shape[0]
    columns = latents.shape[1]
    halo = (deep.shape[0] - rows) // 2
    step = ny * (rows // cols) // H_LAT
    slot = x * nc + c
    members = nx * nc
    everyone = ny * members
    hub = 1
    me = y * members + slot
    is_hub = me == hub
    not_hub = jnp.logical_not(is_hub)
    is_root = me == 0
    fed_by_root = (y == 0) & (c == 0) & (x != 0)
    fed_by_hub = (y == 0) & (c != 0) & (x != 0)
    has_previous = y >= step
    has_next = y < ny - step

    load = pltpu.make_async_copy(latents, deep.at[pl.ds(halo, rows)], in_sem)
    load.start()
    affine = [
        pltpu.make_async_copy(gain, gain_v, w_sem.at[2]),
        pltpu.make_async_copy(shift, shift_v, w_sem.at[3]),
        pltpu.make_async_copy(bias1_hbm, bias1, w_sem.at[4]),
    ]
    weights = [
        pltpu.make_async_copy(w1_hbm, w1_raw, w_sem.at[0]),
        pltpu.make_async_copy(w2, w2_raw, w_sem.at[1]),
    ]

    def turn_weights():
        for copy, source, target in zip(weights, (w1_raw, w2_raw), (w1, w2v)):
            copy.wait()

            def body(t, carry):
                target[t] = source[t].T
                return carry

            lax.fori_loop(0, source.shape[0], body, 0)


    def member(row, p):
        return {"view_0": row, "view_1": p // nc, "view_2": lax.rem(p, nc)}

    barrier = pltpu.get_barrier_semaphore()

    def greet(device):
        pl.semaphore_signal(barrier, inc=1, device_id=device, device_id_type=MESH_ID)

    @pl.when(is_hub)
    def _():
        def body(p, carry):
            q = lax.rem(hub + p, everyone)
            greet(member(q // members, lax.rem(q, members)))
            return carry

        lax.fori_loop(1, everyone, body, 0)

    @pl.when(has_previous)
    def _():
        greet(member(lax.rem(y + ny - step, ny), slot))

    @pl.when(fed_by_root)
    def _():
        greet(member(0, 0))

    load.wait()
    for copy in affine + weights:
        copy.start()

    sums = jnp.zeros((8, columns), F32)
    squares = jnp.zeros((8, columns), F32)
    for i in range(0, rows, 64):
        v = deep[pl.ds(halo + i, 64), :].astype(F32)
        q = v * v
        for j in range(0, 64, 8):
            sums = sums + v[j : j + 8]
            squares = squares + q[j : j + 8]
    sub = lax.broadcasted_iota(jnp.int32, (8, columns), 0)
    both = jnp.where(
        sub == 0, jnp.sum(sums, axis=0, keepdims=True), jnp.sum(squares, axis=0, keepdims=True)
    )
    lane = lax.broadcasted_iota(jnp.int32, (8, 128), 1)
    sub1 = lax.broadcasted_iota(jnp.int32, (8, 128), 0)
    packed = jnp.zeros((8, 128), F32)
    for t in range(columns // 128):
        tile = both[:, t * 128 : (t + 1) * 128]
        for d in (8, 4, 2, 1):
            tile = tile + pltpu.roll(tile, 128 - d, 1)
        s_part = pltpu.roll(tile, t, 1) if t else tile
        q_part = pltpu.roll(tile, t + 4, 1)
        packed = jnp.where((lax.rem(lane, 16) == t) & (sub1 == 0), s_part, packed)
        packed = jnp.where((lax.rem(lane, 16) == t + 4) & (sub1 == 1), q_part, packed)
    mine = jnp.sum(packed, axis=0, keepdims=True)
    gather[pl.ds(me, 1), :] = mine

    pl.semaphore_wait(barrier, jnp.where(is_hub, 0, 1) + jnp.where(has_next, 1, 0) + jnp.where(is_root, nx - 1, 0))

    def remote(src, dst, send, recv, device):
        return pltpu.make_async_remote_copy(
            src_ref=src, dst_ref=dst, send_sem=send, recv_sem=recv, device_id=device, device_id_type=MESH_ID
        )

    def to_row(buf, p):
        return remote(buf, buf, rowsend.at[p], trecv, member(0, p))

    def to_second(p):
        return remote(total, total, rowsend.at[members + p], trecv, member(1, p))

    def raw_to(p):
        return remote(raw, raw, rawsend.at[p], rawrecv, member(0, p))

    def to_column(k):
        return remote(total, total, colsend.at[k], trecv, member(k, slot))

    line = gather.at[pl.ds(me, 1)]
    to_hub = remote(line, line, gsend, grecv, member(0, hub))
    far = sorted(range(1, nx), key=lambda k: -min(k, nx - k))
    fed = [k * nc for k in far]
    sent_total = [k * nc + 1 for k in far]
    second = [k * nc for k in far + [0]]
    following = member(lax.rem(y + step, ny), slot)
    to_next = remote(
        deep.at[pl.ds(rows, halo)], deep.at[pl.ds(0, halo)], hsend.at[0], hrecv.at[0], following
    )
    to_previous = remote(
        deep.at[pl.ds(halo, halo)], deep.at[pl.ds(halo + rows, halo)], hsend.at[1], hrecv.at[1],
        member(lax.rem(y + ny - step, ny), slot),
    )

    @pl.when(is_root)
    def _():
        raw[...] = mine
        raw_to(hub).start()
        for p in fed:
            raw_to(p).start()

    @pl.when(not_hub & jnp.logical_not(is_root))
    def _():
        to_hub.start()

    @pl.when(has_next)
    def _():
        pl.semaphore_signal(ready, inc=1, device_id=following, device_id_type=MESH_ID)
        to_next.start()

    @pl.when(jnp.logical_not(is_root))
    def _():
        turn_weights()

    @pl.when(has_previous)
    def _():
        pl.semaphore_wait(ready, 1)
        to_previous.start()

    @pl.when(not_hub & jnp.logical_not(is_root))
    def _():
        to_hub.wait_send()

    @pl.when(is_hub)
    def _():
        arrivals = gather.at[pl.ds(hub + 1, everyone - hub - 1)]
        pltpu.make_async_copy(arrivals, arrivals, grecv).wait()
        row = lax.broadcasted_iota(jnp.int32, gather.shape, 0)
        rest[...] = jnp.sum(jnp.where(row == 0, 0.0, gather[...]), axis=0, keepdims=True)
        for p in fed:
            to_row(rest, p).start()
        raw_to(hub).wait_recv()
        total[...] = rest[...] + raw[...]
        for p in sent_total:
            to_row(total, p).start()
        to_row(rest, 0).start()
        for p in second:
            to_second(p).start()

    @pl.when(is_root | fed_by_root)
    def _():
        to_row(rest, 0).wait_recv()

        @pl.when(fed_by_root)
        def _():
            raw_to(hub).wait_recv()

        total[...] = rest[...] + raw[...]

    @pl.when(fed_by_hub | (y != 0))
    def _():
        to_row(total, 0).wait_recv()

    @pl.when(y == 0)
    def _():
        for k in range(2, ny):
            to_column(k).start()

        @pl.when(c != 0)
        def _():
            to_column(1).start()

    @pl.when(is_root)
    def _():
        turn_weights()

    @pl.when(has_next)
    def _():
        to_previous.wait_recv()

    @pl.when(has_previous)
    def _():
        to_next.wait_recv()

    for copy in affine:
        copy.wait()
    st = jnp.broadcast_to(total[...], (8, 128))
    base = lane - lax.rem(lane, 16)
    means, rstds = [], []
    for t in range(columns // 128):
        s = jnp.take_along_axis(st, base + t, axis=1)
        q = jnp.take_along_axis(st, base + (t + 4), axis=1)
        mean = s / entries
        var = q / entries - mean * mean
        means.append(mean)
        rstds.append(lax.rsqrt(var + EPSILON))
    mean = jnp.concatenate(means, axis=1)[0:1]
    rstd = jnp.concatenate(rstds, axis=1)[0:1]
    scale = rstd * gain_v[...]
    offset = shift_v[...] - mean * scale
    half_scale = 0.5 * scale
    half_offset = 0.5 * offset

    tall = deep.shape[0] // cols

    def activate(i):
        h = deep[i * cols : (i + 1) * cols, :].astype(F32) * half_scale + half_offset
        a = h * jnp.tanh(h) + h
        if i < 2:
            a = jnp.where(has_previous, a, 0.0)
        if i >= tall - 2:
            a = jnp.where(has_next, a, 0.0)
        rows = slice(i * cols, (i + 1) * cols)
        acat[rows, 0:columns] = shifted_down(a, 0.0).astype(BF16)
        acat[rows, columns : 2 * columns] = a.astype(BF16)
        acat[rows, 2 * columns :] = shifted_up(a, 0.0).astype(BF16)

    mid = tall - 2

    def mix(lo, hi):
        acc = None
        for r in range(3):
            for s in range(3):
                lhs = acat[(lo + r) * cols : (hi + r) * cols, s * columns : (s + 1) * columns]
                term = dot(lhs, w1[3 * r + s])
                acc = term if acc is None else acc + term
        for p in range(lo, hi):
            i = p - lo
            v = acc[i * cols : (i + 1) * cols] + deep[(p + 1) * cols : (p + 2) * cols, :].astype(F32) + bias1[...]
            if p == 0:
                v = jnp.where(has_previous, v, 0.0)
            if p == mid - 1:
                v = jnp.where(has_next, v, 0.0)
            rows = slice(p * cols, (p + 1) * cols)
            m0[rows, :] = v.astype(BF16)
            md[rows, :] = shifted_down(v, 0.0).astype(BF16)
            edge[p : p + 1, :] = v[cols - 1 : cols]

    done = 0
    for lo, hi in MIX_CHUNKS:
        for i in range(done, hi + 2):
            activate(i)
        done = hi + 2
        mix(lo, hi)

    @pl.when(has_next)
    def _():
        to_next.wait_send()

    @pl.when(has_previous)
    def _():
        to_previous.wait_send()

    @pl.when(is_hub)
    def _():
        for p in fed:
            to_row(rest, p).wait_send()
        for p in sent_total:
            to_row(total, p).wait_send()
        to_row(rest, 0).wait_send()
        for p in second:
            to_second(p).wait_send()

    @pl.when(is_root)
    def _():
        for p in [hub] + fed:
            raw_to(p).wait_send()

    @pl.when(y == 0)
    def _():
        for k in range(2, ny):
            to_column(k).wait_send()

        @pl.when(c != 0)
        def _():
            to_column(1).wait_send()


def shifted_down(v, first):
    row = lax.broadcasted_iota(jnp.int32, v.shape, 0)
    return jnp.where(row == 0, first, pltpu.roll(v, 1, 0))


def shifted_up(v, last):
    n = v.shape[0]
    row = lax.broadcasted_iota(jnp.int32, v.shape, 0)
    return jnp.where(row == n - 1, last, pltpu.roll(v, n - 1, 0))


def upsample_kernel(
    cols, m0, md, edge, bias2, w2, out,
    keep_s, keep_x, z, obuf, out_sem,
):
    channels = m0.shape[1]
    slab_rows = m0.shape[0] // cols - 2

    def edge_rows(first, count):
        pad = jnp.zeros((16 - count, channels), F32)
        return jnp.concatenate([edge[first : first + count, :], pad], axis=0).astype(BF16)

    zero16 = jnp.zeros((16, channels), BF16)
    corners = slab_rows + 1

    def block(buf, first, count):
        return buf[first * cols : (first + count) * cols, :]

    def with_edge(buf, first, count, e):
        return jnp.concatenate([block(buf, first, count), e], axis=0)

    def send_rows(y_lo, y_hi, sem):
        copy = pltpu.make_async_copy(
            obuf.at[pl.ds(y_lo, y_hi - y_lo)], out.at[pl.ds(y_lo, y_hi - y_lo)], out_sem.at[sem]
        )
        copy.start()
        return copy

    def upsample(lo, hi):
        n = hi - lo
        nb = min(hi, slab_rows) - lo
        bb = dot(block(m0, lo + 1, nb), w2[4])
        bs = dot(with_edge(md, lo + 1, nb, edge_rows(lo + 1, nb)), w2[3])
        bs = bs + dot(with_edge(m0, lo + 1, nb, zero16), w2[5])
        sb = dot(block(m0, lo, n), w2[1]) + dot(block(m0, lo + 1, n), w2[7])
        ss = dot(with_edge(md, lo, n, edge_rows(lo, n)), w2[0])
        ss = ss + dot(with_edge(m0, lo, n, zero16), w2[2])
        ss = ss + dot(with_edge(md, lo + 1, n, edge_rows(lo + 1, n)), w2[6])
        ss = ss + dot(with_edge(m0, lo + 1, n, zero16), w2[8])

        return n, nb, bb, bs, sb, ss

    def combine(lo, hi, n_out, n, nb, bb, bs, sb, ss):
        sent = []
        for i in range(lo, hi):
            k = i - lo
            s_main = ss[k * cols : (k + 1) * cols]
            s_edge = ss[n * cols + k : n * cols + k + 1]
            c_main = sb[k * cols : (k + 1) * cols] + bias2[...]
            for yy in (2 * i - 1, 2 * i):
                if not 0 <= yy < 2 * slab_rows:
                    continue
                b = yy // 2
                if b < lo:
                    u = s_main + keep_s[0:cols, :]
                    u_edge = s_edge + keep_x[0:1, :]
                    w = c_main + keep_s[cols : 2 * cols, :]
                else:
                    kb = b - lo
                    u = s_main + bs[kb * cols : (kb + 1) * cols]
                    u_edge = s_edge + bs[nb * cols + kb : nb * cols + kb + 1]
                    w = c_main + bb[kb * cols : (kb + 1) * cols]
                zi = yy % 4
                even = u + w
                odd = shifted_up(u, u_edge) + w
                for t in range(channels // 128):
                    lanes = slice(t * 128, (t + 1) * 128)
                    z[zi, t, pl.ds(0, cols, stride=2), :] = even[:, lanes]
                    z[zi, t, pl.ds(1, cols, stride=2), :] = odd[:, lanes]
                    obuf[yy, :, lanes] = z[zi, t].astype(BF16)
            if hi == corners:
                sent.append(send_rows(max(2 * i - 1, 0), min(2 * i + 1, 2 * slab_rows), n_out + k))
        if hi < corners:
            kb = nb - 1
            keep_s[0:cols, :] = bs[kb * cols : (kb + 1) * cols]
            keep_s[cols : 2 * cols, :] = bb[kb * cols : (kb + 1) * cols]
            keep_x[0:1, :] = bs[nb * cols + kb : nb * cols + kb + 1]
        return sent

    copies = []
    (a_lo, a_hi), (b_lo, b_hi) = UP_CHUNKS
    first = upsample(a_lo, a_hi)
    second = upsample(b_lo, b_hi)
    combine(a_lo, a_hi, 0, *first)
    copies.append([send_rows(max(2 * a_lo - 1, 0), 2 * a_hi - 1, 0)])
    copies.append(combine(b_lo, b_hi, 1, *second))
    for group in copies:
        for copy in group:
            copy.wait()


def in_hbm(array):
    return pltpu.with_memory_space_constraint(array, pltpu.HBM)


def exchange(flat, w1, w2, gain, shift, bias1, cols, ny, members, entries):
    rows, channels = flat.shape
    hbm = pl.BlockSpec(memory_space=pltpu.HBM)
    vmem = pl.BlockSpec(memory_space=pltpu.VMEM)
    dma = pltpu.SemaphoreType.DMA
    return pl.pallas_call(
        functools.partial(exchange_kernel, entries, cols),
        out_shape=(
            pltpu.VMEM((rows + 2 * cols, channels), BF16),
            pltpu.VMEM((rows + 2 * cols, channels), BF16),
            pltpu.VMEM((24, channels), F32),
            pltpu.VMEM(w2.shape, BF16),
        ),
        in_specs=[hbm] * 6,
        out_specs=(vmem,) * 4,
        scratch_shapes=[
            pltpu.VMEM((rows + 4 * cols, channels), BF16),
            pltpu.VMEM((rows + 4 * cols, 3 * channels), BF16),
            pltpu.VMEM(w1.shape, BF16),
            pltpu.VMEM(w2.shape, BF16),
            pltpu.VMEM(w1.shape, BF16),
            pltpu.VMEM((1, channels), F32),
            pltpu.VMEM((1, channels), F32),
            pltpu.VMEM((1, channels), F32),
            pltpu.VMEM((ny * members, 128), F32),
            pltpu.VMEM((1, 128), F32),
            pltpu.VMEM((1, 128), F32),
            pltpu.VMEM((1, 128), F32),
            dma,
            dma((5,)),
            dma,
            dma,
            dma((members,)),
            dma,
            dma((2 * members,)),
            dma((ny,)),
            dma,
            dma((2,)),
            dma((2,)),
            pltpu.SemaphoreType.REGULAR,
        ],
        compiler_params=pltpu.CompilerParams(
            collective_id=0, has_side_effects=True, vmem_limit_bytes=36 * 2**20
        ),
        cost_estimate=pl.CostEstimate(flops=3 * 10**9, bytes_accessed=10 * 10**6, transcendentals=0),
        name="exchange",
    )(in_hbm(flat), in_hbm(w1), in_hbm(w2), in_hbm(gain), in_hbm(shift), in_hbm(bias1))


def upsample(m0, md, edge, bias2, w2, cols):
    tall_rows, channels = m0.shape
    slab_rows = tall_rows // cols - 2
    vmem = pl.BlockSpec(memory_space=pltpu.VMEM)
    return pl.pallas_call(
        functools.partial(upsample_kernel, cols),
        out_shape=jax.ShapeDtypeStruct((2 * slab_rows, 2 * cols, channels), BF16),
        in_specs=[vmem] * 5,
        out_specs=pl.BlockSpec(memory_space=pl.ANY),
        scratch_shapes=[
            pltpu.VMEM((2 * cols, channels), F32),
            pltpu.VMEM((8, channels), F32),
            pltpu.VMEM((4, channels // 128, 2 * cols, 128), F32),
            pltpu.VMEM((2 * slab_rows, 2 * cols, channels), BF16),
            pltpu.SemaphoreType.DMA((16,)),
        ],
        compiler_params=pltpu.CompilerParams(vmem_limit_bytes=32 * 2**20),
        cost_estimate=pl.CostEstimate(flops=3 * 10**9, bytes_accessed=4 * 10**6, transcendentals=0),
        name="upsample",
    )(m0, md, edge, bias2, w2)


def per_device(latents, norm_gain, norm_shift, w_first, bias_first, w_second, bias_second):
    slab_rows, cols, channels = latents.shape
    ny = lax.axis_size("view_0")
    members = lax.axis_size("view_1") * lax.axis_size("view_2")
    entries = float(slab_rows * cols * (channels // GROUPS) * ny * members)
    w1 = jnp.transpose(w_first, (1, 2, 0, 3)).reshape(9, channels, channels)
    w2 = jnp.transpose(w_second, (1, 2, 0, 3)).reshape(9, channels, channels)
    flat = latents.reshape(slab_rows * cols, channels)
    row = lambda v: v.reshape(1, channels)
    m0, md, edge, w2 = exchange(
        flat, w1, w2, row(norm_gain), row(norm_shift), row(bias_first), cols, ny, members, entries
    )
    return upsample(m0, md, edge, row(bias_second), w2, cols)


def solution(mesh):
    torus = Mesh(mesh.devices.reshape(mesh.shape["scene"], 8, 8, 2), SCENE_VIEW)
    in_specs = (P(SCENE_VIEW, None, None), P(), P(), P(), P(), P(), P())
    out_specs = P(SCENE_VIEW, None, None)
    return jax.shard_map(per_device, mesh=torus, in_specs=in_specs, out_specs=out_specs, check_vma=False)
```

```python
import functools

import jax
import jax.numpy as jnp
from jax import lax
from jax.experimental import pallas as pl
from jax.experimental.pallas import tpu as pltpu
from jax.sharding import Mesh
from jax.sharding import PartitionSpec as P

GROUPS = 32
H_LAT = 32
AXES = ("view_0", "view_1", "view_2")
SCENE_VIEW = ("scene",) + AXES
EPSILON = 1e-06
F32 = jnp.float32
BF16 = jnp.bfloat16
MESH_ID = pl.DeviceIdType.MESH


MIX_CHUNKS = ((0, 5), (5, 10))
UP_CHUNKS = ((0, 5), (5, 9))


def dot(a, w):
    return lax.dot_general(a, w, (((1,), (0,)), ((), ())), preferred_element_type=F32)


def exchange_kernel(
    entries, cols, latents, w1_hbm, w2, gain, shift, bias1_hbm, m0, md, edge, w2v,
    deep, acat, w1_raw, w2_raw, w1, gain_v, shift_v, bias1, gather, raw, rest, total,
    in_sem, w_sem, gsend, grecv, rawsend, rawrecv, rowsend, colsend, trecv, hsend, hrecv, ready,
):
    y = lax.axis_index("view_0")
    x = lax.axis_index("view_1")
    c = lax.axis_index("view_2")
    ny = lax.axis_size("view_0")
    nx = lax.axis_size("view_1")
    nc = lax.axis_size("view_2")
    rows = latents.shape[0]
    columns = latents.shape[1]
    halo = (deep.shape[0] - rows) // 2
    step = ny * (rows // cols) // H_LAT
    slot = x * nc + c
    members = nx * nc
    everyone = ny * members
    hub = 1
    me = y * members + slot
    is_hub = me == hub
    not_hub = jnp.logical_not(is_hub)
    is_root = me == 0
    fed_by_root = (y == 0) & (c == 0) & (x != 0)
    fed_by_hub = (y == 0) & (c != 0) & (x != 0)
    has_previous = y >= step
    has_next = y < ny - step

    load = pltpu.make_async_copy(latents, deep.at[pl.ds(halo, rows)], in_sem)
    load.start()
    affine = [
        pltpu.make_async_copy(gain, gain_v, w_sem.at[2]),
        pltpu.make_async_copy(shift, shift_v, w_sem.at[3]),
        pltpu.make_async_copy(bias1_hbm, bias1, w_sem.at[4]),
    ]
    weights = [
        pltpu.make_async_copy(w1_hbm, w1_raw, w_sem.at[0]),
        pltpu.make_async_copy(w2, w2_raw, w_sem.at[1]),
    ]

    def turn_weights():
        for copy, source, target in zip(weights, (w1_raw, w2_raw), (w1, w2v)):
            copy.wait()

            def body(t, carry):
                target[t] = source[t].T
                return carry

            lax.fori_loop(0, source.shape[0], body, 0)


    def member(row, p):
        return {"view_0": row, "view_1": p // nc, "view_2": lax.rem(p, nc)}

    barrier = pltpu.get_barrier_semaphore()

    def greet(device):
        pl.semaphore_signal(barrier, inc=1, device_id=device, device_id_type=MESH_ID)

    @pl.when(is_hub)
    def _():
        def body(p, carry):
            q = lax.rem(hub + p, everyone)
            greet(member(q // members, lax.rem(q, members)))
            return carry

        lax.fori_loop(1, everyone, body, 0)

    @pl.when(has_previous)
    def _():
        greet(member(lax.rem(y + ny - step, ny), slot))

    @pl.when(fed_by_root)
    def _():
        greet(member(0, 0))

    load.wait()
    for copy in affine + weights:
        copy.start()

    sums = jnp.zeros((8, columns), F32)
    squares = jnp.zeros((8, columns), F32)
    for i in range(0, rows, 64):
        v = deep[pl.ds(halo + i, 64), :].astype(F32)
        q = v * v
        for j in range(0, 64, 8):
            sums = sums + v[j : j + 8]
            squares = squares + q[j : j + 8]
    sub = lax.broadcasted_iota(jnp.int32, (8, columns), 0)
    both = jnp.where(
        sub == 0, jnp.sum(sums, axis=0, keepdims=True), jnp.sum(squares, axis=0, keepdims=True)
    )
    lane = lax.broadcasted_iota(jnp.int32, (8, 128), 1)
    sub1 = lax.broadcasted_iota(jnp.int32, (8, 128), 0)
    packed = jnp.zeros((8, 128), F32)
    for t in range(columns // 128):
        tile = both[:, t * 128 : (t + 1) * 128]
        for d in (8, 4, 2, 1):
            tile = tile + pltpu.roll(tile, 128 - d, 1)
        s_part = pltpu.roll(tile, t, 1) if t else tile
        q_part = pltpu.roll(tile, t + 4, 1)
        packed = jnp.where((lax.rem(lane, 16) == t) & (sub1 == 0), s_part, packed)
        packed = jnp.where((lax.rem(lane, 16) == t + 4) & (sub1 == 1), q_part, packed)
    mine = jnp.sum(packed, axis=0, keepdims=True)
    gather[pl.ds(me, 1), :] = mine

    pl.semaphore_wait(barrier, jnp.where(is_hub, 0, 1) + jnp.where(has_next, 1, 0) + jnp.where(is_root, nx - 1, 0))

    def remote(src, dst, send, recv, device):
        return pltpu.make_async_remote_copy(
            src_ref=src, dst_ref=dst, send_sem=send, recv_sem=recv, device_id=device, device_id_type=MESH_ID
        )

    def to_row(buf, p):
        return remote(buf, buf, rowsend.at[p], trecv, member(0, p))

    def to_second(p):
        return remote(total, total, rowsend.at[members + p], trecv, member(1, p))

    def raw_to(p):
        return remote(raw, raw, rawsend.at[p], rawrecv, member(0, p))

    def to_column(k, column, first):
        return remote(total, total, colsend.at[first + k], trecv, member(k, column))

    line = gather.at[pl.ds(me, 1)]
    to_hub = remote(line, line, gsend, grecv, member(0, hub))
    far = sorted(range(1, nx), key=lambda k: -min(k, nx - k))
    fed = [k * nc for k in far]
    sent_total = [k * nc + 1 for k in far]
    second = [k * nc for k in far + [0]]
    following = member(lax.rem(y + step, ny), slot)
    to_next = remote(
        deep.at[pl.ds(rows, halo)], deep.at[pl.ds(0, halo)], hsend.at[0], hrecv.at[0], following
    )
    to_previous = remote(
        deep.at[pl.ds(halo, halo)], deep.at[pl.ds(halo + rows, halo)], hsend.at[1], hrecv.at[1],
        member(lax.rem(y + ny - step, ny), slot),
    )

    @pl.when(is_root)
    def _():
        raw[...] = mine
        raw_to(hub).start()
        for p in fed:
            raw_to(p).start()

    @pl.when(not_hub & jnp.logical_not(is_root))
    def _():
        to_hub.start()

    @pl.when(has_next)
    def _():
        pl.semaphore_signal(ready, inc=1, device_id=following, device_id_type=MESH_ID)
        to_next.start()

    turn_weights()

    @pl.when(has_previous)
    def _():
        pl.semaphore_wait(ready, 1)
        to_previous.start()

    @pl.when(not_hub & jnp.logical_not(is_root))
    def _():
        to_hub.wait_send()

    @pl.when(is_hub)
    def _():
        arrivals = gather.at[pl.ds(hub + 1, everyone - hub - 1)]
        pltpu.make_async_copy(arrivals, arrivals, grecv).wait()
        row = lax.broadcasted_iota(jnp.int32, gather.shape, 0)
        rest[...] = jnp.sum(jnp.where(row == 0, 0.0, gather[...]), axis=0, keepdims=True)
        for p in fed:
            to_row(rest, p).start()
        raw_to(hub).wait_recv()
        total[...] = rest[...] + raw[...]
        for p in sent_total:
            to_row(total, p).start()
        to_row(rest, 0).start()
        for p in second:
            to_second(p).start()

    @pl.when(is_root | fed_by_root)
    def _():
        to_row(rest, 0).wait_recv()

        @pl.when(fed_by_root)
        def _():
            raw_to(hub).wait_recv()

        total[...] = rest[...] + raw[...]

    @pl.when(fed_by_hub | (y != 0))
    def _():
        to_row(total, 0).wait_recv()

    forwards = (y == 0) & (x != 0)
    forwards_twice = (y == 0) & (x == nx - 1)

    def forward(act):
        @pl.when(forwards)
        def _():
            for k in range(2, ny):
                act(to_column(k, slot, 0))

        @pl.when(forwards & (c != 0))
        def _():
            act(to_column(1, slot, 0))

        @pl.when(forwards_twice)
        def _():
            for k in range(2, ny):
                act(to_column(k, c, ny))

        @pl.when(forwards_twice & (c != 0))
        def _():
            act(to_column(1, c, ny))

    forward(lambda copy: copy.start())

    @pl.when(has_next)
    def _():
        to_previous.wait_recv()

    @pl.when(has_previous)
    def _():
        to_next.wait_recv()

    for copy in affine:
        copy.wait()
    st = jnp.broadcast_to(total[...], (8, 128))
    base = lane - lax.rem(lane, 16)
    means, rstds = [], []
    for t in range(columns // 128):
        s = jnp.take_along_axis(st, base + t, axis=1)
        q = jnp.take_along_axis(st, base + (t + 4), axis=1)
        mean = s / entries
        var = q / entries - mean * mean
        means.append(mean)
        rstds.append(lax.rsqrt(var + EPSILON))
    mean = jnp.concatenate(means, axis=1)[0:1]
    rstd = jnp.concatenate(rstds, axis=1)[0:1]
    scale = rstd * gain_v[...]
    offset = shift_v[...] - mean * scale
    half_scale = 0.5 * scale
    half_offset = 0.5 * offset

    tall = deep.shape[0] // cols

    def activate(i):
        h = deep[i * cols : (i + 1) * cols, :].astype(F32) * half_scale + half_offset
        a = h * jnp.tanh(h) + h
        if i < 2:
            a = jnp.where(has_previous, a, 0.0)
        if i >= tall - 2:
            a = jnp.where(has_next, a, 0.0)
        rows = slice(i * cols, (i + 1) * cols)
        acat[rows, 0:columns] = shifted_down(a, 0.0).astype(BF16)
        acat[rows, columns : 2 * columns] = a.astype(BF16)
        acat[rows, 2 * columns :] = shifted_up(a, 0.0).astype(BF16)

    mid = tall - 2

    def mix(lo, hi):
        acc = None
        for r in range(3):
            for s in range(3):
                lhs = acat[(lo + r) * cols : (hi + r) * cols, s * columns : (s + 1) * columns]
                term = dot(lhs, w1[3 * r + s])
                acc = term if acc is None else acc + term
        for p in range(lo, hi):
            i = p - lo
            v = acc[i * cols : (i + 1) * cols] + deep[(p + 1) * cols : (p + 2) * cols, :].astype(F32) + bias1[...]
            if p == 0:
                v = jnp.where(has_previous, v, 0.0)
            if p == mid - 1:
                v = jnp.where(has_next, v, 0.0)
            rows = slice(p * cols, (p + 1) * cols)
            m0[rows, :] = v.astype(BF16)
            md[rows, :] = shifted_down(v, 0.0).astype(BF16)
            edge[p : p + 1, :] = v[cols - 1 : cols]

    done = 0
    for lo, hi in MIX_CHUNKS:
        for i in range(done, hi + 2):
            activate(i)
        done = hi + 2
        mix(lo, hi)

    @pl.when(has_next)
    def _():
        to_next.wait_send()

    @pl.when(has_previous)
    def _():
        to_previous.wait_send()

    @pl.when(is_hub)
    def _():
        for p in fed:
            to_row(rest, p).wait_send()
        for p in sent_total:
            to_row(total, p).wait_send()
        to_row(rest, 0).wait_send()
        for p in second:
            to_second(p).wait_send()

    @pl.when(is_root)
    def _():
        for p in [hub] + fed:
            raw_to(p).wait_send()

    forward(lambda copy: copy.wait_send())


def shifted_down(v, first):
    row = lax.broadcasted_iota(jnp.int32, v.shape, 0)
    return jnp.where(row == 0, first, pltpu.roll(v, 1, 0))


def shifted_up(v, last):
    n = v.shape[0]
    row = lax.broadcasted_iota(jnp.int32, v.shape, 0)
    return jnp.where(row == n - 1, last, pltpu.roll(v, n - 1, 0))


def upsample_kernel(
    cols, m0, md, edge, bias2, w2, out,
    keep_s, keep_x, z, obuf, out_sem,
):
    channels = m0.shape[1]
    slab_rows = m0.shape[0] // cols - 2

    def edge_rows(first, count):
        pad = jnp.zeros((16 - count, channels), F32)
        return jnp.concatenate([edge[first : first + count, :], pad], axis=0).astype(BF16)

    zero16 = jnp.zeros((16, channels), BF16)
    corners = slab_rows + 1

    def block(buf, first, count):
        return buf[first * cols : (first + count) * cols, :]

    def with_edge(buf, first, count, e):
        return jnp.concatenate([block(buf, first, count), e], axis=0)

    def send_rows(y_lo, y_hi, sem):
        copy = pltpu.make_async_copy(
            obuf.at[pl.ds(y_lo, y_hi - y_lo)], out.at[pl.ds(y_lo, y_hi - y_lo)], out_sem.at[sem]
        )
        copy.start()
        return copy

    def upsample(lo, hi):
        n = hi - lo
        nb = min(hi, slab_rows) - lo
        bb = dot(block(m0, lo + 1, nb), w2[4])
        bs = dot(with_edge(md, lo + 1, nb, edge_rows(lo + 1, nb)), w2[3])
        bs = bs + dot(with_edge(m0, lo + 1, nb, zero16), w2[5])
        sb = dot(block(m0, lo, n), w2[1]) + dot(block(m0, lo + 1, n), w2[7])
        ss = dot(with_edge(md, lo, n, edge_rows(lo, n)), w2[0])
        ss = ss + dot(with_edge(m0, lo, n, zero16), w2[2])
        ss = ss + dot(with_edge(md, lo + 1, n, edge_rows(lo + 1, n)), w2[6])
        ss = ss + dot(with_edge(m0, lo + 1, n, zero16), w2[8])

        return n, nb, bb, bs, sb, ss

    def combine(lo, hi, n_out, n, nb, bb, bs, sb, ss):
        sent = []
        for i in range(lo, hi):
            k = i - lo
            s_main = ss[k * cols : (k + 1) * cols]
            s_edge = ss[n * cols + k : n * cols + k + 1]
            c_main = sb[k * cols : (k + 1) * cols] + bias2[...]
            for yy in (2 * i - 1, 2 * i):
                if not 0 <= yy < 2 * slab_rows:
                    continue
                b = yy // 2
                if b < lo:
                    u = s_main + keep_s[0:cols, :]
                    u_edge = s_edge + keep_x[0:1, :]
                    w = c_main + keep_s[cols : 2 * cols, :]
                else:
                    kb = b - lo
                    u = s_main + bs[kb * cols : (kb + 1) * cols]
                    u_edge = s_edge + bs[nb * cols + kb : nb * cols + kb + 1]
                    w = c_main + bb[kb * cols : (kb + 1) * cols]
                zi = yy % 4
                even = u + w
                odd = shifted_up(u, u_edge) + w
                for t in range(channels // 128):
                    lanes = slice(t * 128, (t + 1) * 128)
                    z[zi, t, pl.ds(0, cols, stride=2), :] = even[:, lanes]
                    z[zi, t, pl.ds(1, cols, stride=2), :] = odd[:, lanes]
                    obuf[yy, :, lanes] = z[zi, t].astype(BF16)
            if hi == corners:
                sent.append(send_rows(max(2 * i - 1, 0), min(2 * i + 1, 2 * slab_rows), n_out + k))
        if hi < corners:
            kb = nb - 1
            keep_s[0:cols, :] = bs[kb * cols : (kb + 1) * cols]
            keep_s[cols : 2 * cols, :] = bb[kb * cols : (kb + 1) * cols]
            keep_x[0:1, :] = bs[nb * cols + kb : nb * cols + kb + 1]
        return sent

    copies = []
    (a_lo, a_hi), (b_lo, b_hi) = UP_CHUNKS
    first = upsample(a_lo, a_hi)
    second = upsample(b_lo, b_hi)
    combine(a_lo, a_hi, 0, *first)
    copies.append([send_rows(max(2 * a_lo - 1, 0), 2 * a_hi - 1, 0)])
    copies.append(combine(b_lo, b_hi, 1, *second))
    for group in copies:
        for copy in group:
            copy.wait()


def in_hbm(array):
    return pltpu.with_memory_space_constraint(array, pltpu.HBM)


def exchange(flat, w1, w2, gain, shift, bias1, cols, ny, members, entries):
    rows, channels = flat.shape
    hbm = pl.BlockSpec(memory_space=pltpu.HBM)
    vmem = pl.BlockSpec(memory_space=pltpu.VMEM)
    dma = pltpu.SemaphoreType.DMA
    return pl.pallas_call(
        functools.partial(exchange_kernel, entries, cols),
        out_shape=(
            pltpu.VMEM((rows + 2 * cols, channels), BF16),
            pltpu.VMEM((rows + 2 * cols, channels), BF16),
            pltpu.VMEM((24, channels), F32),
            pltpu.VMEM(w2.shape, BF16),
        ),
        in_specs=[hbm] * 6,
        out_specs=(vmem,) * 4,
        scratch_shapes=[
            pltpu.VMEM((rows + 4 * cols, channels), BF16),
            pltpu.VMEM((rows + 4 * cols, 3 * channels), BF16),
            pltpu.VMEM(w1.shape, BF16),
            pltpu.VMEM(w2.shape, BF16),
            pltpu.VMEM(w1.shape, BF16),
            pltpu.VMEM((1, channels), F32),
            pltpu.VMEM((1, channels), F32),
            pltpu.VMEM((1, channels), F32),
            pltpu.VMEM((ny * members, 128), F32),
            pltpu.VMEM((1, 128), F32),
            pltpu.VMEM((1, 128), F32),
            pltpu.VMEM((1, 128), F32),
            dma,
            dma((5,)),
            dma,
            dma,
            dma((members,)),
            dma,
            dma((2 * members,)),
            dma((2 * ny,)),
            dma,
            dma((2,)),
            dma((2,)),
            pltpu.SemaphoreType.REGULAR,
        ],
        compiler_params=pltpu.CompilerParams(
            collective_id=0, has_side_effects=True, vmem_limit_bytes=36 * 2**20
        ),
        cost_estimate=pl.CostEstimate(flops=3 * 10**9, bytes_accessed=10 * 10**6, transcendentals=0),
        name="exchange",
    )(in_hbm(flat), in_hbm(w1), in_hbm(w2), in_hbm(gain), in_hbm(shift), in_hbm(bias1))


def upsample(m0, md, edge, bias2, w2, cols):
    tall_rows, channels = m0.shape
    slab_rows = tall_rows // cols - 2
    vmem = pl.BlockSpec(memory_space=pltpu.VMEM)
    return pl.pallas_call(
        functools.partial(upsample_kernel, cols),
        out_shape=jax.ShapeDtypeStruct((2 * slab_rows, 2 * cols, channels), BF16),
        in_specs=[vmem] * 5,
        out_specs=pl.BlockSpec(memory_space=pl.ANY),
        scratch_shapes=[
            pltpu.VMEM((2 * cols, channels), F32),
            pltpu.VMEM((8, channels), F32),
            pltpu.VMEM((4, channels // 128, 2 * cols, 128), F32),
            pltpu.VMEM((2 * slab_rows, 2 * cols, channels), BF16),
            pltpu.SemaphoreType.DMA((16,)),
        ],
        compiler_params=pltpu.CompilerParams(vmem_limit_bytes=32 * 2**20),
        cost_estimate=pl.CostEstimate(flops=3 * 10**9, bytes_accessed=4 * 10**6, transcendentals=0),
        name="upsample",
    )(m0, md, edge, bias2, w2)


def per_device(latents, norm_gain, norm_shift, w_first, bias_first, w_second, bias_second):
    slab_rows, cols, channels = latents.shape
    ny = lax.axis_size("view_0")
    members = lax.axis_size("view_1") * lax.axis_size("view_2")
    entries = float(slab_rows * cols * (channels // GROUPS) * ny * members)
    w1 = jnp.transpose(w_first, (1, 2, 0, 3)).reshape(9, channels, channels)
    w2 = jnp.transpose(w_second, (1, 2, 0, 3)).reshape(9, channels, channels)
    flat = latents.reshape(slab_rows * cols, channels)
    row = lambda v: v.reshape(1, channels)
    m0, md, edge, w2 = exchange(
        flat, w1, w2, row(norm_gain), row(norm_shift), row(bias_first), cols, ny, members, entries
    )
    return upsample(m0, md, edge, row(bias_second), w2, cols)


def solution(mesh):
    torus = Mesh(mesh.devices.reshape(mesh.shape["scene"], 8, 8, 2), SCENE_VIEW)
    in_specs = (P(SCENE_VIEW, None, None), P(), P(), P(), P(), P(), P())
    out_specs = P(SCENE_VIEW, None, None)
    return jax.shard_map(per_device, mesh=torus, in_specs=in_specs, out_specs=out_specs, check_vma=False)
```

```python
import functools

import jax
import jax.numpy as jnp
from jax import lax
from jax.experimental import pallas as pl
from jax.experimental.pallas import tpu as pltpu
from jax.sharding import Mesh
from jax.sharding import PartitionSpec as P

GROUPS = 32
H_LAT = 32
AXES = ("view_0", "view_1", "view_2")
SCENE_VIEW = ("scene",) + AXES
EPSILON = 1e-06
F32 = jnp.float32
BF16 = jnp.bfloat16
MESH_ID = pl.DeviceIdType.MESH


MIX_CHUNKS = ((0, 5), (5, 10))
UP_CHUNKS = ((0, 5), (5, 9))


def dot(a, w):
    return lax.dot_general(a, w, (((1,), (0,)), ((), ())), preferred_element_type=F32)


def exchange_kernel(
    entries, cols, latents, w1_hbm, w2, gain, shift, bias1_hbm, m0, md, edge, w2v,
    deep, acat, w1_raw, w2_raw, w1, gain_v, shift_v, bias1, gather, raw, rest, total,
    in_sem, w_sem, gsend, grecv, rawsend, rawrecv, rowsend, colsend, trecv, hsend, hrecv, ready,
):
    y = lax.axis_index("view_0")
    x = lax.axis_index("view_1")
    c = lax.axis_index("view_2")
    ny = lax.axis_size("view_0")
    nx = lax.axis_size("view_1")
    nc = lax.axis_size("view_2")
    rows = latents.shape[0]
    columns = latents.shape[1]
    halo = (deep.shape[0] - rows) // 2
    step = ny * (rows // cols) // H_LAT
    slot = x * nc + c
    members = nx * nc
    everyone = ny * members
    hub = 1
    me = y * members + slot
    is_hub = me == hub
    not_hub = jnp.logical_not(is_hub)
    is_root = me == 0
    fed_by_root = (y == 0) & (c == 0) & (x != 0)
    fed_by_hub = (y == 0) & (c != 0) & (x != 0)
    has_previous = y >= step
    has_next = y < ny - step

    load = pltpu.make_async_copy(latents, deep.at[pl.ds(halo, rows)], in_sem)
    load.start()
    affine = [
        pltpu.make_async_copy(gain, gain_v, w_sem.at[2]),
        pltpu.make_async_copy(shift, shift_v, w_sem.at[3]),
        pltpu.make_async_copy(bias1_hbm, bias1, w_sem.at[4]),
    ]
    weights = [
        pltpu.make_async_copy(w1_hbm, w1_raw, w_sem.at[0]),
        pltpu.make_async_copy(w2, w2_raw, w_sem.at[1]),
    ]

    def turn_weights():
        for copy, source, target in zip(weights, (w1_raw, w2_raw), (w1, w2v)):
            copy.wait()

            def body(t, carry):
                target[t] = source[t].T
                return carry

            lax.fori_loop(0, source.shape[0], body, 0)


    def member(row, p):
        return {"view_0": row, "view_1": p // nc, "view_2": lax.rem(p, nc)}

    barrier = pltpu.get_barrier_semaphore()

    def greet(device):
        pl.semaphore_signal(barrier, inc=1, device_id=device, device_id_type=MESH_ID)

    @pl.when(is_hub)
    def _():
        def body(p, carry):
            q = lax.rem(hub + p, everyone)
            greet(member(q // members, lax.rem(q, members)))
            return carry

        lax.fori_loop(1, everyone, body, 0)

    @pl.when(has_previous)
    def _():
        greet(member(lax.rem(y + ny - step, ny), slot))

    @pl.when(fed_by_root)
    def _():
        greet(member(0, 0))

    load.wait()
    for copy in affine + weights:
        copy.start()

    sums = jnp.zeros((8, columns), F32)
    squares = jnp.zeros((8, columns), F32)
    for i in range(0, rows, 64):
        v = deep[pl.ds(halo + i, 64), :].astype(F32)
        q = v * v
        for j in range(0, 64, 8):
            sums = sums + v[j : j + 8]
            squares = squares + q[j : j + 8]
    sub = lax.broadcasted_iota(jnp.int32, (8, columns), 0)
    both = jnp.where(
        sub == 0, jnp.sum(sums, axis=0, keepdims=True), jnp.sum(squares, axis=0, keepdims=True)
    )
    lane = lax.broadcasted_iota(jnp.int32, (8, 128), 1)
    sub1 = lax.broadcasted_iota(jnp.int32, (8, 128), 0)
    packed = jnp.zeros((8, 128), F32)
    for t in range(columns // 128):
        tile = both[:, t * 128 : (t + 1) * 128]
        for d in (8, 4, 2, 1):
            tile = tile + pltpu.roll(tile, 128 - d, 1)
        s_part = pltpu.roll(tile, t, 1) if t else tile
        q_part = pltpu.roll(tile, t + 4, 1)
        packed = jnp.where((lax.rem(lane, 16) == t) & (sub1 == 0), s_part, packed)
        packed = jnp.where((lax.rem(lane, 16) == t + 4) & (sub1 == 1), q_part, packed)
    mine = jnp.sum(packed, axis=0, keepdims=True)
    gather[pl.ds(me, 1), :] = mine

    pl.semaphore_wait(barrier, jnp.where(is_hub, 0, 1) + jnp.where(has_next, 1, 0) + jnp.where(is_root, nx - 1, 0))

    def remote(src, dst, send, recv, device):
        return pltpu.make_async_remote_copy(
            src_ref=src, dst_ref=dst, send_sem=send, recv_sem=recv, device_id=device, device_id_type=MESH_ID
        )

    def to_row(buf, p):
        return remote(buf, buf, rowsend.at[p], trecv, member(0, p))

    def to_second(p):
        return remote(total, total, rowsend.at[members + p], trecv, member(1, p))

    def raw_to(p):
        return remote(raw, raw, rawsend.at[p], rawrecv, member(0, p))

    def to_column(k, column, first):
        return remote(total, total, colsend.at[first + k], trecv, member(k, column))

    line = gather.at[pl.ds(me, 1)]
    to_hub = remote(line, line, gsend, grecv, member(0, hub))
    far = sorted(range(1, nx), key=lambda k: -min(k, nx - k))
    fed = [k * nc for k in far]
    sent_total = [k * nc + 1 for k in far]
    second = [k * nc for k in far + [0]]
    following = member(lax.rem(y + step, ny), slot)
    to_next = remote(
        deep.at[pl.ds(rows, halo)], deep.at[pl.ds(0, halo)], hsend.at[0], hrecv.at[0], following
    )
    to_previous = remote(
        deep.at[pl.ds(halo, halo)], deep.at[pl.ds(halo + rows, halo)], hsend.at[1], hrecv.at[1],
        member(lax.rem(y + ny - step, ny), slot),
    )

    @pl.when(is_root)
    def _():
        raw[...] = mine
        raw_to(hub).start()
        for p in fed:
            raw_to(p).start()

    @pl.when(not_hub & jnp.logical_not(is_root))
    def _():
        to_hub.start()

    @pl.when(has_next)
    def _():
        pl.semaphore_signal(ready, inc=1, device_id=following, device_id_type=MESH_ID)
        to_next.start()

    turn_weights()

    @pl.when(has_previous)
    def _():
        pl.semaphore_wait(ready, 1)
        to_previous.start()

    @pl.when(not_hub & jnp.logical_not(is_root))
    def _():
        to_hub.wait_send()

    @pl.when(is_hub)
    def _():
        arrivals = gather.at[pl.ds(hub + 1, everyone - hub - 1)]
        pltpu.make_async_copy(arrivals, arrivals, grecv).wait()
        row = lax.broadcasted_iota(jnp.int32, gather.shape, 0)
        rest[...] = jnp.sum(jnp.where(row == 0, 0.0, gather[...]), axis=0, keepdims=True)
        for p in fed:
            to_row(rest, p).start()
        raw_to(hub).wait_recv()
        total[...] = rest[...] + raw[...]
        for p in sent_total:
            to_row(total, p).start()
        to_row(rest, 0).start()
        for p in second:
            to_second(p).start()

    @pl.when(is_root | fed_by_root)
    def _():
        to_row(rest, 0).wait_recv()

        @pl.when(fed_by_root)
        def _():
            raw_to(hub).wait_recv()

        total[...] = rest[...] + raw[...]

    @pl.when(fed_by_hub | (y != 0))
    def _():
        to_row(total, 0).wait_recv()

    forwards = (y == 0) & jnp.logical_not(is_root)

    def forward(act):
        @pl.when(forwards)
        def _():
            for k in range(2, ny):
                act(to_column(k, slot, 0))

        @pl.when(forwards & (c != 0))
        def _():
            act(to_column(1, slot, 0))

        @pl.when(is_hub)
        def _():
            for k in range(2, ny):
                act(to_column(k, 0, ny))

    forward(lambda copy: copy.start())

    @pl.when(has_next)
    def _():
        to_previous.wait_recv()

    @pl.when(has_previous)
    def _():
        to_next.wait_recv()

    for copy in affine:
        copy.wait()
    st = jnp.broadcast_to(total[...], (8, 128))
    base = lane - lax.rem(lane, 16)
    means, rstds = [], []
    for t in range(columns // 128):
        s = jnp.take_along_axis(st, base + t, axis=1)
        q = jnp.take_along_axis(st, base + (t + 4), axis=1)
        mean = s / entries
        var = q / entries - mean * mean
        means.append(mean)
        rstds.append(lax.rsqrt(var + EPSILON))
    mean = jnp.concatenate(means, axis=1)[0:1]
    rstd = jnp.concatenate(rstds, axis=1)[0:1]
    scale = rstd * gain_v[...]
    offset = shift_v[...] - mean * scale
    half_scale = 0.5 * scale
    half_offset = 0.5 * offset

    tall = deep.shape[0] // cols

    def activate(i):
        h = deep[i * cols : (i + 1) * cols, :].astype(F32) * half_scale + half_offset
        a = h * jnp.tanh(h) + h
        if i < 2:
            a = jnp.where(has_previous, a, 0.0)
        if i >= tall - 2:
            a = jnp.where(has_next, a, 0.0)
        rows = slice(i * cols, (i + 1) * cols)
        acat[rows, 0:columns] = shifted_down(a, 0.0).astype(BF16)
        acat[rows, columns : 2 * columns] = a.astype(BF16)
        acat[rows, 2 * columns :] = shifted_up(a, 0.0).astype(BF16)

    mid = tall - 2

    def mix(lo, hi):
        acc = None
        for r in range(3):
            for s in range(3):
                lhs = acat[(lo + r) * cols : (hi + r) * cols, s * columns : (s + 1) * columns]
                term = dot(lhs, w1[3 * r + s])
                acc = term if acc is None else acc + term
        for p in range(lo, hi):
            i = p - lo
            v = acc[i * cols : (i + 1) * cols] + deep[(p + 1) * cols : (p + 2) * cols, :].astype(F32) + bias1[...]
            if p == 0:
                v = jnp.where(has_previous, v, 0.0)
            if p == mid - 1:
                v = jnp.where(has_next, v, 0.0)
            rows = slice(p * cols, (p + 1) * cols)
            m0[rows, :] = v.astype(BF16)
            md[rows, :] = shifted_down(v, 0.0).astype(BF16)
            edge[p : p + 1, :] = v[cols - 1 : cols]

    done = 0
    for lo, hi in MIX_CHUNKS:
        for i in range(done, hi + 2):
            activate(i)
        done = hi + 2
        mix(lo, hi)

    @pl.when(has_next)
    def _():
        to_next.wait_send()

    @pl.when(has_previous)
    def _():
        to_previous.wait_send()

    @pl.when(is_hub)
    def _():
        for p in fed:
            to_row(rest, p).wait_send()
        for p in sent_total:
            to_row(total, p).wait_send()
        to_row(rest, 0).wait_send()
        for p in second:
            to_second(p).wait_send()

    @pl.when(is_root)
    def _():
        for p in [hub] + fed:
            raw_to(p).wait_send()

    forward(lambda copy: copy.wait_send())


def shifted_down(v, first):
    row = lax.broadcasted_iota(jnp.int32, v.shape, 0)
    return jnp.where(row == 0, first, pltpu.roll(v, 1, 0))


def shifted_up(v, last):
    n = v.shape[0]
    row = lax.broadcasted_iota(jnp.int32, v.shape, 0)
    return jnp.where(row == n - 1, last, pltpu.roll(v, n - 1, 0))


def upsample_kernel(
    cols, m0, md, edge, bias2, w2, out,
    keep_s, keep_x, z, obuf, out_sem,
):
    channels = m0.shape[1]
    slab_rows = m0.shape[0] // cols - 2

    def edge_rows(first, count):
        pad = jnp.zeros((16 - count, channels), F32)
        return jnp.concatenate([edge[first : first + count, :], pad], axis=0).astype(BF16)

    zero16 = jnp.zeros((16, channels), BF16)
    corners = slab_rows + 1

    def block(buf, first, count):
        return buf[first * cols : (first + count) * cols, :]

    def with_edge(buf, first, count, e):
        return jnp.concatenate([block(buf, first, count), e], axis=0)

    def send_rows(y_lo, y_hi, sem):
        copy = pltpu.make_async_copy(
            obuf.at[pl.ds(y_lo, y_hi - y_lo)], out.at[pl.ds(y_lo, y_hi - y_lo)], out_sem.at[sem]
        )
        copy.start()
        return copy

    def upsample(lo, hi):
        n = hi - lo
        nb = min(hi, slab_rows) - lo
        bb = dot(block(m0, lo + 1, nb), w2[4])
        bs = dot(with_edge(md, lo + 1, nb, edge_rows(lo + 1, nb)), w2[3])
        bs = bs + dot(with_edge(m0, lo + 1, nb, zero16), w2[5])
        sb = dot(block(m0, lo, n), w2[1]) + dot(block(m0, lo + 1, n), w2[7])
        ss = dot(with_edge(md, lo, n, edge_rows(lo, n)), w2[0])
        ss = ss + dot(with_edge(m0, lo, n, zero16), w2[2])
        ss = ss + dot(with_edge(md, lo + 1, n, edge_rows(lo + 1, n)), w2[6])
        ss = ss + dot(with_edge(m0, lo + 1, n, zero16), w2[8])

        return n, nb, bb, bs, sb, ss

    def combine(lo, hi, n_out, n, nb, bb, bs, sb, ss):
        sent = []
        for i in range(lo, hi):
            k = i - lo
            s_main = ss[k * cols : (k + 1) * cols]
            s_edge = ss[n * cols + k : n * cols + k + 1]
            c_main = sb[k * cols : (k + 1) * cols] + bias2[...]
            for yy in (2 * i - 1, 2 * i):
                if not 0 <= yy < 2 * slab_rows:
                    continue
                b = yy // 2
                if b < lo:
                    u = s_main + keep_s[0:cols, :]
                    u_edge = s_edge + keep_x[0:1, :]
                    w = c_main + keep_s[cols : 2 * cols, :]
                else:
                    kb = b - lo
                    u = s_main + bs[kb * cols : (kb + 1) * cols]
                    u_edge = s_edge + bs[nb * cols + kb : nb * cols + kb + 1]
                    w = c_main + bb[kb * cols : (kb + 1) * cols]
                zi = yy % 4
                even = u + w
                odd = shifted_up(u, u_edge) + w
                for t in range(channels // 128):
                    lanes = slice(t * 128, (t + 1) * 128)
                    z[zi, t, pl.ds(0, cols, stride=2), :] = even[:, lanes]
                    z[zi, t, pl.ds(1, cols, stride=2), :] = odd[:, lanes]
                    obuf[yy, :, lanes] = z[zi, t].astype(BF16)
            if hi == corners:
                sent.append(send_rows(max(2 * i - 1, 0), min(2 * i + 1, 2 * slab_rows), n_out + k))
        if hi < corners:
            kb = nb - 1
            keep_s[0:cols, :] = bs[kb * cols : (kb + 1) * cols]
            keep_s[cols : 2 * cols, :] = bb[kb * cols : (kb + 1) * cols]
            keep_x[0:1, :] = bs[nb * cols + kb : nb * cols + kb + 1]
        return sent

    copies = []
    (a_lo, a_hi), (b_lo, b_hi) = UP_CHUNKS
    first = upsample(a_lo, a_hi)
    second = upsample(b_lo, b_hi)
    combine(a_lo, a_hi, 0, *first)
    copies.append([send_rows(max(2 * a_lo - 1, 0), 2 * a_hi - 1, 0)])
    copies.append(combine(b_lo, b_hi, 1, *second))
    for group in copies:
        for copy in group:
            copy.wait()


def in_hbm(array):
    return pltpu.with_memory_space_constraint(array, pltpu.HBM)


def exchange(flat, w1, w2, gain, shift, bias1, cols, ny, members, entries):
    rows, channels = flat.shape
    hbm = pl.BlockSpec(memory_space=pltpu.HBM)
    vmem = pl.BlockSpec(memory_space=pltpu.VMEM)
    dma = pltpu.SemaphoreType.DMA
    return pl.pallas_call(
        functools.partial(exchange_kernel, entries, cols),
        out_shape=(
            pltpu.VMEM((rows + 2 * cols, channels), BF16),
            pltpu.VMEM((rows + 2 * cols, channels), BF16),
            pltpu.VMEM((24, channels), F32),
            pltpu.VMEM(w2.shape, BF16),
        ),
        in_specs=[hbm] * 6,
        out_specs=(vmem,) * 4,
        scratch_shapes=[
            pltpu.VMEM((rows + 4 * cols, channels), BF16),
            pltpu.VMEM((rows + 4 * cols, 3 * channels), BF16),
            pltpu.VMEM(w1.shape, BF16),
            pltpu.VMEM(w2.shape, BF16),
            pltpu.VMEM(w1.shape, BF16),
            pltpu.VMEM((1, channels), F32),
            pltpu.VMEM((1, channels), F32),
            pltpu.VMEM((1, channels), F32),
            pltpu.VMEM((ny * members, 128), F32),
            pltpu.VMEM((1, 128), F32),
            pltpu.VMEM((1, 128), F32),
            pltpu.VMEM((1, 128), F32),
            dma,
            dma((5,)),
            dma,
            dma,
            dma((members,)),
            dma,
            dma((2 * members,)),
            dma((2 * ny,)),
            dma,
            dma((2,)),
            dma((2,)),
            pltpu.SemaphoreType.REGULAR,
        ],
        compiler_params=pltpu.CompilerParams(
            collective_id=0, has_side_effects=True, vmem_limit_bytes=36 * 2**20
        ),
        cost_estimate=pl.CostEstimate(flops=3 * 10**9, bytes_accessed=10 * 10**6, transcendentals=0),
        name="exchange",
    )(in_hbm(flat), in_hbm(w1), in_hbm(w2), in_hbm(gain), in_hbm(shift), in_hbm(bias1))


def upsample(m0, md, edge, bias2, w2, cols):
    tall_rows, channels = m0.shape
    slab_rows = tall_rows // cols - 2
    vmem = pl.BlockSpec(memory_space=pltpu.VMEM)
    return pl.pallas_call(
        functools.partial(upsample_kernel, cols),
        out_shape=jax.ShapeDtypeStruct((2 * slab_rows, 2 * cols, channels), BF16),
        in_specs=[vmem] * 5,
        out_specs=pl.BlockSpec(memory_space=pl.ANY),
        scratch_shapes=[
            pltpu.VMEM((2 * cols, channels), F32),
            pltpu.VMEM((8, channels), F32),
            pltpu.VMEM((4, channels // 128, 2 * cols, 128), F32),
            pltpu.VMEM((2 * slab_rows, 2 * cols, channels), BF16),
            pltpu.SemaphoreType.DMA((16,)),
        ],
        compiler_params=pltpu.CompilerParams(vmem_limit_bytes=32 * 2**20),
        cost_estimate=pl.CostEstimate(flops=3 * 10**9, bytes_accessed=4 * 10**6, transcendentals=0),
        name="upsample",
    )(m0, md, edge, bias2, w2)


def per_device(latents, norm_gain, norm_shift, w_first, bias_first, w_second, bias_second):
    slab_rows, cols, channels = latents.shape
    ny = lax.axis_size("view_0")
    members = lax.axis_size("view_1") * lax.axis_size("view_2")
    entries = float(slab_rows * cols * (channels // GROUPS) * ny * members)
    w1 = jnp.transpose(w_first, (1, 2, 0, 3)).reshape(9, channels, channels)
    w2 = jnp.transpose(w_second, (1, 2, 0, 3)).reshape(9, channels, channels)
    flat = latents.reshape(slab_rows * cols, channels)
    row = lambda v: v.reshape(1, channels)
    m0, md, edge, w2 = exchange(
        flat, w1, w2, row(norm_gain), row(norm_shift), row(bias_first), cols, ny, members, entries
    )
    return upsample(m0, md, edge, row(bias_second), w2, cols)


def solution(mesh):
    torus = Mesh(mesh.devices.reshape(mesh.shape["scene"], 8, 8, 2), SCENE_VIEW)
    in_specs = (P(SCENE_VIEW, None, None), P(), P(), P(), P(), P(), P())
    out_specs = P(SCENE_VIEW, None, None)
    return jax.shard_map(per_device, mesh=torus, in_specs=in_specs, out_specs=out_specs, check_vma=False)
```

```python
import functools

import jax
import jax.numpy as jnp
from jax import lax
from jax.experimental import pallas as pl
from jax.experimental.pallas import tpu as pltpu
from jax.sharding import Mesh
from jax.sharding import PartitionSpec as P

GROUPS = 32
H_LAT = 32
AXES = ("view_0", "view_1", "view_2")
SCENE_VIEW = ("scene",) + AXES
EPSILON = 1e-06
F32 = jnp.float32
BF16 = jnp.bfloat16
MESH_ID = pl.DeviceIdType.MESH


MIX_CHUNKS = ((0, 5), (5, 10))
UP_CHUNKS = ((0, 5), (5, 9))


def dot(a, w):
    return lax.dot_general(a, w, (((1,), (0,)), ((), ())), preferred_element_type=F32)


def exchange_kernel(
    entries, cols, latents, w1_hbm, w2, gain, shift, bias1_hbm, m0, md, edge, w2v,
    deep, acat, w1_raw, w2_raw, w1, gain_v, shift_v, bias1, gather, raw, rest, total,
    in_sem, w_sem, gsend, grecv, rawsend, rawrecv, rowsend, colsend, trecv, hsend, hrecv, ready,
):
    y = lax.axis_index("view_0")
    x = lax.axis_index("view_1")
    c = lax.axis_index("view_2")
    ny = lax.axis_size("view_0")
    nx = lax.axis_size("view_1")
    nc = lax.axis_size("view_2")
    rows = latents.shape[0]
    columns = latents.shape[1]
    halo = (deep.shape[0] - rows) // 2
    step = ny * (rows // cols) // H_LAT
    slot = x * nc + c
    members = nx * nc
    everyone = ny * members
    hub = 1
    me = y * members + slot
    is_hub = me == hub
    not_hub = jnp.logical_not(is_hub)
    is_root = me == 0
    fed_by_root = (y == 0) & (c == 0) & (x != 0)
    fed_by_hub = (y == 0) & (c != 0) & (x != 0)
    has_previous = y >= step
    has_next = y < ny - step

    load = pltpu.make_async_copy(latents, deep.at[pl.ds(halo, rows)], in_sem)
    load.start()
    affine = [
        pltpu.make_async_copy(gain, gain_v, w_sem.at[2]),
        pltpu.make_async_copy(shift, shift_v, w_sem.at[3]),
        pltpu.make_async_copy(bias1_hbm, bias1, w_sem.at[4]),
    ]
    weights = [
        pltpu.make_async_copy(w1_hbm, w1_raw, w_sem.at[0]),
        pltpu.make_async_copy(w2, w2_raw, w_sem.at[1]),
    ]

    def turn_weights():
        for copy, source, target in zip(weights, (w1_raw, w2_raw), (w1, w2v)):
            copy.wait()

            def body(t, carry):
                target[t] = source[t].T
                return carry

            lax.fori_loop(0, source.shape[0], body, 0)


    def member(row, p):
        return {"view_0": row, "view_1": p // nc, "view_2": lax.rem(p, nc)}

    barrier = pltpu.get_barrier_semaphore()

    def greet(device):
        pl.semaphore_signal(barrier, inc=1, device_id=device, device_id_type=MESH_ID)

    @pl.when(is_hub)
    def _():
        def body(p, carry):
            q = lax.rem(hub + p, everyone)
            greet(member(q // members, lax.rem(q, members)))
            return carry

        lax.fori_loop(1, everyone, body, 0)

    @pl.when(has_previous)
    def _():
        greet(member(lax.rem(y + ny - step, ny), slot))

    @pl.when(fed_by_root)
    def _():
        greet(member(0, 0))

    load.wait()
    for copy in affine + weights:
        copy.start()

    sums = jnp.zeros((8, columns), F32)
    squares = jnp.zeros((8, columns), F32)
    for i in range(0, rows, 64):
        v = deep[pl.ds(halo + i, 64), :].astype(F32)
        q = v * v
        for j in range(0, 64, 8):
            sums = sums + v[j : j + 8]
            squares = squares + q[j : j + 8]
    sub = lax.broadcasted_iota(jnp.int32, (8, columns), 0)
    both = jnp.where(
        sub == 0, jnp.sum(sums, axis=0, keepdims=True), jnp.sum(squares, axis=0, keepdims=True)
    )
    lane = lax.broadcasted_iota(jnp.int32, (8, 128), 1)
    sub1 = lax.broadcasted_iota(jnp.int32, (8, 128), 0)
    packed = jnp.zeros((8, 128), F32)
    for t in range(columns // 128):
        tile = both[:, t * 128 : (t + 1) * 128]
        for d in (8, 4, 2, 1):
            tile = tile + pltpu.roll(tile, 128 - d, 1)
        s_part = pltpu.roll(tile, t, 1) if t else tile
        q_part = pltpu.roll(tile, t + 4, 1)
        packed = jnp.where((lax.rem(lane, 16) == t) & (sub1 == 0), s_part, packed)
        packed = jnp.where((lax.rem(lane, 16) == t + 4) & (sub1 == 1), q_part, packed)
    mine = jnp.sum(packed, axis=0, keepdims=True)
    gather[pl.ds(me, 1), :] = mine

    pl.semaphore_wait(barrier, jnp.where(is_hub, 0, 1) + jnp.where(has_next, 1, 0) + jnp.where(is_root, nx - 1, 0))

    def remote(src, dst, send, recv, device):
        return pltpu.make_async_remote_copy(
            src_ref=src, dst_ref=dst, send_sem=send, recv_sem=recv, device_id=device, device_id_type=MESH_ID
        )

    def to_row(buf, p):
        return remote(buf, buf, rowsend.at[p], trecv, member(0, p))

    def raw_to(p):
        return remote(raw, raw, rawsend.at[p], rawrecv, member(0, p))

    def to_column(k, column, first):
        return remote(total, total, colsend.at[first + k], trecv, member(k, column))

    line = gather.at[pl.ds(me, 1)]
    to_hub = remote(line, line, gsend, grecv, member(0, hub))
    near = sorted(range(1, nx), key=lambda k: min(k, nx - k))
    fed = [k * nc for k in near]
    sent_total = [k * nc + 1 for k in near]
    following = member(lax.rem(y + step, ny), slot)
    to_next = remote(
        deep.at[pl.ds(rows, halo)], deep.at[pl.ds(0, halo)], hsend.at[0], hrecv.at[0], following
    )
    to_previous = remote(
        deep.at[pl.ds(halo, halo)], deep.at[pl.ds(halo + rows, halo)], hsend.at[1], hrecv.at[1],
        member(lax.rem(y + ny - step, ny), slot),
    )

    @pl.when(is_root)
    def _():
        raw[...] = mine
        raw_to(hub).start()
        for p in fed:
            raw_to(p).start()

    @pl.when(not_hub & jnp.logical_not(is_root))
    def _():
        to_hub.start()

    @pl.when(has_next)
    def _():
        pl.semaphore_signal(ready, inc=1, device_id=following, device_id_type=MESH_ID)
        to_next.start()

    turn_weights()

    @pl.when(has_previous)
    def _():
        pl.semaphore_wait(ready, 1)
        to_previous.start()

    @pl.when(not_hub & jnp.logical_not(is_root))
    def _():
        to_hub.wait_send()

    @pl.when(is_hub)
    def _():
        arrivals = gather.at[pl.ds(hub + 1, everyone - hub - 1)]
        pltpu.make_async_copy(arrivals, arrivals, grecv).wait()
        row = lax.broadcasted_iota(jnp.int32, gather.shape, 0)
        rest[...] = jnp.sum(jnp.where(row == 0, 0.0, gather[...]), axis=0, keepdims=True)
        for p in fed:
            to_row(rest, p).start()
        raw_to(hub).wait_recv()
        total[...] = rest[...] + raw[...]
        for p in sent_total:
            to_row(total, p).start()
        to_row(rest, 0).start()

    @pl.when(is_root | fed_by_root)
    def _():
        to_row(rest, 0).wait_recv()

        @pl.when(fed_by_root)
        def _():
            raw_to(hub).wait_recv()

        total[...] = rest[...] + raw[...]

    @pl.when(fed_by_hub | (y != 0))
    def _():
        to_row(total, 0).wait_recv()

    forwards = (y == 0) & jnp.logical_not(is_root)

    def forward(act):
        @pl.when(forwards)
        def _():
            for k in range(1, ny):
                act(to_column(k, slot, 0))

        @pl.when(is_hub)
        def _():
            for k in range(1, ny):
                act(to_column(k, 0, ny))

    forward(lambda copy: copy.start())

    @pl.when(has_next)
    def _():
        to_previous.wait_recv()

    @pl.when(has_previous)
    def _():
        to_next.wait_recv()

    for copy in affine:
        copy.wait()
    st = jnp.broadcast_to(total[...], (8, 128))
    base = lane - lax.rem(lane, 16)
    means, rstds = [], []
    for t in range(columns // 128):
        s = jnp.take_along_axis(st, base + t, axis=1)
        q = jnp.take_along_axis(st, base + (t + 4), axis=1)
        mean = s / entries
        var = q / entries - mean * mean
        means.append(mean)
        rstds.append(lax.rsqrt(var + EPSILON))
    mean = jnp.concatenate(means, axis=1)[0:1]
    rstd = jnp.concatenate(rstds, axis=1)[0:1]
    scale = rstd * gain_v[...]
    offset = shift_v[...] - mean * scale
    half_scale = 0.5 * scale
    half_offset = 0.5 * offset

    tall = deep.shape[0] // cols

    def activate(i):
        h = deep[i * cols : (i + 1) * cols, :].astype(F32) * half_scale + half_offset
        a = h * jnp.tanh(h) + h
        if i < 2:
            a = jnp.where(has_previous, a, 0.0)
        if i >= tall - 2:
            a = jnp.where(has_next, a, 0.0)
        rows = slice(i * cols, (i + 1) * cols)
        acat[rows, 0:columns] = shifted_down(a, 0.0).astype(BF16)
        acat[rows, columns : 2 * columns] = a.astype(BF16)
        acat[rows, 2 * columns :] = shifted_up(a, 0.0).astype(BF16)

    mid = tall - 2

    def mix(lo, hi):
        acc = None
        for r in range(3):
            for s in range(3):
                lhs = acat[(lo + r) * cols : (hi + r) * cols, s * columns : (s + 1) * columns]
                term = dot(lhs, w1[3 * r + s])
                acc = term if acc is None else acc + term
        for p in range(lo, hi):
            i = p - lo
            v = acc[i * cols : (i + 1) * cols] + deep[(p + 1) * cols : (p + 2) * cols, :].astype(F32) + bias1[...]
            if p == 0:
                v = jnp.where(has_previous, v, 0.0)
            if p == mid - 1:
                v = jnp.where(has_next, v, 0.0)
            rows = slice(p * cols, (p + 1) * cols)
            m0[rows, :] = v.astype(BF16)
            md[rows, :] = shifted_down(v, 0.0).astype(BF16)
            edge[p : p + 1, :] = v[cols - 1 : cols]

    done = 0
    for lo, hi in MIX_CHUNKS:
        for i in range(done, hi + 2):
            activate(i)
        done = hi + 2
        mix(lo, hi)

    @pl.when(has_next)
    def _():
        to_next.wait_send()

    @pl.when(has_previous)
    def _():
        to_previous.wait_send()

    @pl.when(is_hub)
    def _():
        for p in fed:
            to_row(rest, p).wait_send()
        for p in sent_total:
            to_row(total, p).wait_send()
        to_row(rest, 0).wait_send()

    @pl.when(is_root)
    def _():
        for p in [hub] + fed:
            raw_to(p).wait_send()

    forward(lambda copy: copy.wait_send())


def shifted_down(v, first):
    row = lax.broadcasted_iota(jnp.int32, v.shape, 0)
    return jnp.where(row == 0, first, pltpu.roll(v, 1, 0))


def shifted_up(v, last):
    n = v.shape[0]
    row = lax.broadcasted_iota(jnp.int32, v.shape, 0)
    return jnp.where(row == n - 1, last, pltpu.roll(v, n - 1, 0))


def upsample_kernel(
    cols, m0, md, edge, bias2, w2, out,
    keep_s, keep_x, z, obuf, out_sem,
):
    channels = m0.shape[1]
    slab_rows = m0.shape[0] // cols - 2

    def edge_rows(first, count):
        pad = jnp.zeros((16 - count, channels), F32)
        return jnp.concatenate([edge[first : first + count, :], pad], axis=0).astype(BF16)

    zero16 = jnp.zeros((16, channels), BF16)
    corners = slab_rows + 1

    def block(buf, first, count):
        return buf[first * cols : (first + count) * cols, :]

    def with_edge(buf, first, count, e):
        return jnp.concatenate([block(buf, first, count), e], axis=0)

    def send_rows(y_lo, y_hi, sem):
        copy = pltpu.make_async_copy(
            obuf.at[pl.ds(y_lo, y_hi - y_lo)], out.at[pl.ds(y_lo, y_hi - y_lo)], out_sem.at[sem]
        )
        copy.start()
        return copy

    def upsample(lo, hi):
        n = hi - lo
        nb = min(hi, slab_rows) - lo
        bb = dot(block(m0, lo + 1, nb), w2[4])
        bs = dot(with_edge(md, lo + 1, nb, edge_rows(lo + 1, nb)), w2[3])
        bs = bs + dot(with_edge(m0, lo + 1, nb, zero16), w2[5])
        sb = dot(block(m0, lo, n), w2[1]) + dot(block(m0, lo + 1, n), w2[7])
        ss = dot(with_edge(md, lo, n, edge_rows(lo, n)), w2[0])
        ss = ss + dot(with_edge(m0, lo, n, zero16), w2[2])
        ss = ss + dot(with_edge(md, lo + 1, n, edge_rows(lo + 1, n)), w2[6])
        ss = ss + dot(with_edge(m0, lo + 1, n, zero16), w2[8])

        return n, nb, bb, bs, sb, ss

    def combine(lo, hi, n_out, n, nb, bb, bs, sb, ss):
        sent = []
        for i in range(lo, hi):
            k = i - lo
            s_main = ss[k * cols : (k + 1) * cols]
            s_edge = ss[n * cols + k : n * cols + k + 1]
            c_main = sb[k * cols : (k + 1) * cols] + bias2[...]
            for yy in (2 * i - 1, 2 * i):
                if not 0 <= yy < 2 * slab_rows:
                    continue
                b = yy // 2
                if b < lo:
                    u = s_main + keep_s[0:cols, :]
                    u_edge = s_edge + keep_x[0:1, :]
                    w = c_main + keep_s[cols : 2 * cols, :]
                else:
                    kb = b - lo
                    u = s_main + bs[kb * cols : (kb + 1) * cols]
                    u_edge = s_edge + bs[nb * cols + kb : nb * cols + kb + 1]
                    w = c_main + bb[kb * cols : (kb + 1) * cols]
                zi = yy % 4
                even = u + w
                odd = shifted_up(u, u_edge) + w
                for t in range(channels // 128):
                    lanes = slice(t * 128, (t + 1) * 128)
                    z[zi, t, pl.ds(0, cols, stride=2), :] = even[:, lanes]
                    z[zi, t, pl.ds(1, cols, stride=2), :] = odd[:, lanes]
                    obuf[yy, :, lanes] = z[zi, t].astype(BF16)
            if hi == corners:
                sent.append(send_rows(max(2 * i - 1, 0), min(2 * i + 1, 2 * slab_rows), n_out + k))
        if hi < corners:
            kb = nb - 1
            keep_s[0:cols, :] = bs[kb * cols : (kb + 1) * cols]
            keep_s[cols : 2 * cols, :] = bb[kb * cols : (kb + 1) * cols]
            keep_x[0:1, :] = bs[nb * cols + kb : nb * cols + kb + 1]
        return sent

    copies = []
    (a_lo, a_hi), (b_lo, b_hi) = UP_CHUNKS
    first = upsample(a_lo, a_hi)
    second = upsample(b_lo, b_hi)
    combine(a_lo, a_hi, 0, *first)
    copies.append([send_rows(max(2 * a_lo - 1, 0), 2 * a_hi - 1, 0)])
    copies.append(combine(b_lo, b_hi, 1, *second))
    for group in copies:
        for copy in group:
            copy.wait()


def in_hbm(array):
    return pltpu.with_memory_space_constraint(array, pltpu.HBM)


def exchange(flat, w1, w2, gain, shift, bias1, cols, ny, members, entries):
    rows, channels = flat.shape
    hbm = pl.BlockSpec(memory_space=pltpu.HBM)
    vmem = pl.BlockSpec(memory_space=pltpu.VMEM)
    dma = pltpu.SemaphoreType.DMA
    return pl.pallas_call(
        functools.partial(exchange_kernel, entries, cols),
        out_shape=(
            pltpu.VMEM((rows + 2 * cols, channels), BF16),
            pltpu.VMEM((rows + 2 * cols, channels), BF16),
            pltpu.VMEM((24, channels), F32),
            pltpu.VMEM(w2.shape, BF16),
        ),
        in_specs=[hbm] * 6,
        out_specs=(vmem,) * 4,
        scratch_shapes=[
            pltpu.VMEM((rows + 4 * cols, channels), BF16),
            pltpu.VMEM((rows + 4 * cols, 3 * channels), BF16),
            pltpu.VMEM(w1.shape, BF16),
            pltpu.VMEM(w2.shape, BF16),
            pltpu.VMEM(w1.shape, BF16),
            pltpu.VMEM((1, channels), F32),
            pltpu.VMEM((1, channels), F32),
            pltpu.VMEM((1, channels), F32),
            pltpu.VMEM((ny * members, 128), F32),
            pltpu.VMEM((1, 128), F32),
            pltpu.VMEM((1, 128), F32),
            pltpu.VMEM((1, 128), F32),
            dma,
            dma((5,)),
            dma,
            dma,
            dma((members,)),
            dma,
            dma((members,)),
            dma((2 * ny,)),
            dma,
            dma((2,)),
            dma((2,)),
            pltpu.SemaphoreType.REGULAR,
        ],
        compiler_params=pltpu.CompilerParams(
            collective_id=0, has_side_effects=True, vmem_limit_bytes=36 * 2**20
        ),
        cost_estimate=pl.CostEstimate(flops=3 * 10**9, bytes_accessed=10 * 10**6, transcendentals=0),
        name="exchange",
    )(in_hbm(flat), in_hbm(w1), in_hbm(w2), in_hbm(gain), in_hbm(shift), in_hbm(bias1))


def upsample(m0, md, edge, bias2, w2, cols):
    tall_rows, channels = m0.shape
    slab_rows = tall_rows // cols - 2
    vmem = pl.BlockSpec(memory_space=pltpu.VMEM)
    return pl.pallas_call(
        functools.partial(upsample_kernel, cols),
        out_shape=jax.ShapeDtypeStruct((2 * slab_rows, 2 * cols, channels), BF16),
        in_specs=[vmem] * 5,
        out_specs=pl.BlockSpec(memory_space=pl.ANY),
        scratch_shapes=[
            pltpu.VMEM((2 * cols, channels), F32),
            pltpu.VMEM((8, channels), F32),
            pltpu.VMEM((4, channels // 128, 2 * cols, 128), F32),
            pltpu.VMEM((2 * slab_rows, 2 * cols, channels), BF16),
            pltpu.SemaphoreType.DMA((16,)),
        ],
        compiler_params=pltpu.CompilerParams(vmem_limit_bytes=32 * 2**20),
        cost_estimate=pl.CostEstimate(flops=3 * 10**9, bytes_accessed=4 * 10**6, transcendentals=0),
        name="upsample",
    )(m0, md, edge, bias2, w2)


def per_device(latents, norm_gain, norm_shift, w_first, bias_first, w_second, bias_second):
    slab_rows, cols, channels = latents.shape
    ny = lax.axis_size("view_0")
    members = lax.axis_size("view_1") * lax.axis_size("view_2")
    entries = float(slab_rows * cols * (channels // GROUPS) * ny * members)
    w1 = jnp.transpose(w_first, (1, 2, 0, 3)).reshape(9, channels, channels)
    w2 = jnp.transpose(w_second, (1, 2, 0, 3)).reshape(9, channels, channels)
    flat = latents.reshape(slab_rows * cols, channels)
    row = lambda v: v.reshape(1, channels)
    m0, md, edge, w2 = exchange(
        flat, w1, w2, row(norm_gain), row(norm_shift), row(bias_first), cols, ny, members, entries
    )
    return upsample(m0, md, edge, row(bias_second), w2, cols)


def solution(mesh):
    torus = Mesh(mesh.devices.reshape(mesh.shape["scene"], 8, 8, 2), SCENE_VIEW)
    in_specs = (P(SCENE_VIEW, None, None), P(), P(), P(), P(), P(), P())
    out_specs = P(SCENE_VIEW, None, None)
    return jax.shard_map(per_device, mesh=torus, in_specs=in_specs, out_specs=out_specs, check_vma=False)
```
